16 devices in a mesh: fsdp: 16 (over z, y, x, core).
Axes of the slice: x: 2, y: 2, z: 2, core: 2. Of those that a mesh axis runs over, the one named last changes fastest.
Arguments:
- patches: bfloat16 [1024, 196, 768], P('fsdp')
- keep: int32 [1024, 49], P('fsdp')
- w_patch: float32 [768, 1024], P(None, 'fsdp')
- b_patch: float32 [1024], P('fsdp')
- pos_table: float32 [197, 1024], P(None, 'fsdp')
- cls_tok: float32 [1024], P('fsdp')
- lnp_g: float32 [1024], P('fsdp')
- lnp_b: float32 [1024], P('fsdp')
- ln1_g: float32 [1024], P('fsdp')
- ln1_b: float32 [1024], P('fsdp')
- w_qkv: float32 [1024, 3, 16, 64], P('fsdp')
- b_qkv: float32 [3072], P('fsdp')
- w_out: float32 [1024, 1024], P('fsdp')
- b_out: float32 [1024], P('fsdp')
- ln2_g: float32 [1024], P('fsdp')
- ln2_b: float32 [1024], P('fsdp')
- w_fc: float32 [1024, 4096], P('fsdp')
- b_fc: float32 [4096], P('fsdp')
- w_proj: float32 [4096, 1024], P('fsdp')
- b_proj: float32 [1024], P('fsdp')
- grad_h1: bfloat16 [1024, 50, 1024], P('fsdp')
Outputs:
- output 1: bfloat16 [1024, 50, 1024], P('fsdp')
- output 2: float32 [768, 1024], P(None, 'fsdp')
- output 3: float32 [1024], P('fsdp')
- output 4: float32 [197, 1024], P(None, 'fsdp')
- output 5: float32 [1024], P('fsdp')
- output 6: float32 [1024], P('fsdp')
- output 7: float32 [1024], P('fsdp')
- output 8: float32 [1024], P('fsdp')
- output 9: float32 [1024], P('fsdp')
- output 10: float32 [1024, 3, 16, 64], P('fsdp')
- output 11: float32 [3072], P('fsdp')
- output 12: float32 [1024, 1024], P('fsdp')
- output 13: float32 [1024], P('fsdp')
- output 14: float32 [1024], P('fsdp')
- output 15: float32 [1024], P('fsdp')
- output 16: float32 [1024, 4096], P('fsdp')
- output 17: float32 [4096], P('fsdp')
- output 18: float32 [4096, 1024], P('fsdp')
- output 19: float32 [1024], P('fsdp')
All inputs are finite; a program needn't handle non-finite values.
Results may differ from the reference program's by a relative error of at most 0.02.
Values are sent between devices in bfloat16 or wider.
A program may use at most 1 GiB of HBM per device.

```python
import jax
import jax.numpy as jnp
from jax import lax

MODEL_WIDTH = 1024
NUM_HEADS = 16
MLP_WIDTH = 4096
NUM_PATCHES = 196
PATCH_PIXELS = 768
NUM_KEEP = 49
BATCH_SIZE = 1024
BLOCK_IMAGES = 64
TOKENS = NUM_KEEP + 1
HEAD_DIM = MODEL_WIDTH // NUM_HEADS
LN_EPS = 1e-5
INV_SQRT2 = 0.7071067811865476
INV_SQRT_2PI = 0.3989422804014327
PARAM_NAMES = ('w_patch', 'b_patch', 'pos_table', 'cls_tok', 'lnp_g', 'lnp_b', 'ln1_g', 'ln1_b', 'w_qkv', 'b_qkv', 'w_out', 'b_out', 'ln2_g', 'ln2_b', 'w_fc', 'b_fc', 'w_proj', 'b_proj')
VECTOR_NAMES = ('b_patch', 'cls_tok', 'lnp_g', 'lnp_b', 'ln1_g', 'ln1_b', 'b_qkv', 'b_out', 'ln2_g', 'ln2_b', 'b_fc', 'b_proj')


def setup_inputs(seed: int = 0) -> dict:
    key_list = jax.random.split(jax.random.key(seed), 21)
    d_model = MODEL_WIDTH
    mlp_width = MLP_WIDTH

    def draw_normal(index, shape, scale):
        return jax.random.normal(key_list[index], shape, jnp.float32) * scale

    def gain_vec(index):
        return 1.0 + draw_normal(index, (d_model,), 0.2)

    row_keys = jax.random.split(key_list[1], BATCH_SIZE)
    perm_rows = jax.vmap(lambda row_key: jax.random.permutation(row_key, NUM_PATCHES))(row_keys)
    return {
        'patches': draw_normal(0, (BATCH_SIZE, NUM_PATCHES, PATCH_PIXELS), 1.0).astype(jnp.bfloat16),
        'keep': perm_rows[:, :NUM_KEEP].astype(jnp.int32),
        'w_patch': draw_normal(2, (PATCH_PIXELS, d_model), PATCH_PIXELS ** -0.5),
        'b_patch': draw_normal(3, (d_model,), 0.3),
        'pos_table': draw_normal(4, (NUM_PATCHES + 1, d_model), 0.5),
        'cls_tok': draw_normal(5, (d_model,), 1.0),
        'lnp_g': gain_vec(6),
        'lnp_b': draw_normal(7, (d_model,), 0.2),
        'ln1_g': gain_vec(8),
        'ln1_b': draw_normal(9, (d_model,), 0.2),
        'w_qkv': draw_normal(10, (d_model, 3, NUM_HEADS, HEAD_DIM), d_model ** -0.5),
        'b_qkv': draw_normal(11, (3 * d_model,), 0.3),
        'w_out': draw_normal(12, (d_model, d_model), d_model ** -0.5),
        'b_out': draw_normal(13, (d_model,), 0.3),
        'ln2_g': gain_vec(14),
        'ln2_b': draw_normal(15, (d_model,), 0.2),
        'w_fc': draw_normal(16, (d_model, mlp_width), d_model ** -0.5),
        'b_fc': draw_normal(17, (mlp_width,), 0.3),
        'w_proj': draw_normal(18, (mlp_width, d_model), mlp_width ** -0.5),
        'b_proj': draw_normal(19, (d_model,), 0.3),
        'grad_h1': draw_normal(20, (BATCH_SIZE, TOKENS, d_model), (BATCH_SIZE * TOKENS) ** -0.5).astype(jnp.bfloat16),
    }


def product(einsum_form, left_op, right_op):
    return jnp.einsum(einsum_form, left_op.astype(jnp.float32), right_op.astype(jnp.float32))


def norm_forward(x_in, gain_f, shift_f):
    centered = x_in - jnp.mean(x_in, axis=-1, keepdims=True)
    inv_std = lax.rsqrt(jnp.mean(centered * centered, axis=-1, keepdims=True) + LN_EPS)
    x_hat = centered * inv_std
    return x_hat * gain_f + shift_f, x_hat, inv_std


def norm_backward(d_norm, x_hat, inv_std, gain_f):
    d_hat = d_norm * gain_f
    d_in = inv_std * (d_hat - jnp.mean(d_hat, axis=-1, keepdims=True) - x_hat * jnp.mean(d_hat * x_hat, axis=-1, keepdims=True))
    return d_in, jnp.sum(d_norm * x_hat, axis=(0, 1)), jnp.sum(d_norm, axis=(0, 1))


def gelu_slope(pre_act):
    return 0.5 * (1.0 + lax.erf(pre_act * INV_SQRT2)) + pre_act * jnp.exp(-0.5 * pre_act * pre_act) * INV_SQRT_2PI


def forward(full_w, patches, keep):
    n_img = patches.shape[0]
    d_model = full_w['w_out'].shape[0]
    n_heads, head_dim = full_w['w_qkv'].shape[2], full_w['w_qkv'].shape[3]
    logit_scale = head_dim ** -0.5
    as_f32 = {name: full_w[name].astype(jnp.float32) for name in VECTOR_NAMES}
    kept_rows = jnp.take_along_axis(patches, keep[:, :, None], axis=1)
    embed_rows = product('bkq,qw->bkw', kept_rows, full_w['w_patch']) + as_f32['b_patch'] + full_w['pos_table'][1 + keep].astype(jnp.float32)
    head_row = as_f32['cls_tok'] + full_w['pos_table'][0].astype(jnp.float32)
    x_zero = jnp.concatenate([jnp.broadcast_to(head_row, (n_img, 1, d_model)), embed_rows], axis=1)
    h_zero, hat_p, inv_p = norm_forward(x_zero, as_f32['lnp_g'], as_f32['lnp_b'])
    y_one, hat_1, inv_1 = norm_forward(h_zero, as_f32['ln1_g'], as_f32['ln1_b'])
    a_in = y_one.astype(jnp.bfloat16)
    qkv_all = (product('btw,wchd->btchd', a_in, full_w['w_qkv']) + as_f32['b_qkv'].reshape(3, n_heads, head_dim)).astype(jnp.bfloat16)
    q_heads, k_heads, v_heads = qkv_all[:, :, 0], qkv_all[:, :, 1], qkv_all[:, :, 2]
    attn_prob = jax.nn.softmax(product('bqhd,bkhd->bhqk', q_heads, k_heads) * logit_scale, axis=-1)
    prob_b = attn_prob.astype(jnp.bfloat16)
    context = product('bhqk,bkhd->bqhd', prob_b, v_heads).astype(jnp.bfloat16)
    h_mid = h_zero + product('bqhd,hdw->bqw', context, full_w['w_out'].reshape(n_heads, head_dim, d_model)) + as_f32['b_out']
    y_two, hat_2, inv_2 = norm_forward(h_mid, as_f32['ln2_g'], as_f32['ln2_b'])
    c_in = y_two.astype(jnp.bfloat16)
    pre_act = product('btw,wf->btf', c_in, full_w['w_fc']) + as_f32['b_fc']
    gelu_out = jax.nn.gelu(pre_act, approximate=False).astype(jnp.bfloat16)
    h_one = (h_mid + product('btf,fw->btw', gelu_out, full_w['w_proj']) + as_f32['b_proj']).astype(jnp.bfloat16)
    saved = dict(keep=keep, kept_rows=kept_rows, hat_p=hat_p, inv_p=inv_p, hat_1=hat_1, inv_1=inv_1, a_in=a_in, q_heads=q_heads, k_heads=k_heads, v_heads=v_heads, attn_prob=attn_prob, prob_b=prob_b, context=context, hat_2=hat_2, inv_2=inv_2, c_in=c_in, pre_act=pre_act, gelu_out=gelu_out)
    return h_one, saved


def backward(weights, saved, grad_h1):
    d_model = weights['w_out'].shape[0]
    n_heads, head_dim = weights['w_qkv'].shape[2], weights['w_qkv'].shape[3]
    logit_scale = head_dim ** -0.5
    w_out3 = weights['w_out'].reshape(n_heads, head_dim, d_model)
    d_h = grad_h1.astype(jnp.float32)
    g_w_proj = product('btf,btw->fw', saved['gelu_out'], grad_h1)
    d_pre = product('btw,fw->btf', grad_h1, weights['w_proj']) * gelu_slope(saved['pre_act'])
    d_pre_b = d_pre.astype(jnp.bfloat16)
    g_w_fc = product('btw,btf->wf', saved['c_in'], d_pre_b)
    d_c = product('btf,wf->btw', d_pre_b, weights['w_fc'])
    d_norm2, g_ln2_g, g_ln2_b = norm_backward(d_c, saved['hat_2'], saved['inv_2'], weights['ln2_g'].astype(jnp.float32))
    d_mid = d_norm2 + d_h
    d_mid_b = d_mid.astype(jnp.bfloat16)
    g_w_out = product('bqhd,bqw->hdw', saved['context'], d_mid_b).reshape(d_model, d_model)
    d_ctx = product('bqw,hdw->bqhd', d_mid_b, w_out3).astype(jnp.bfloat16)
    g_v = product('bhqk,bqhd->bkhd', saved['prob_b'], d_ctx)
    d_prob = product('bqhd,bkhd->bhqk', d_ctx, saved['v_heads'])
    attn_prob = saved['attn_prob']
    d_logit = (attn_prob * (d_prob - jnp.sum(attn_prob * d_prob, axis=-1, keepdims=True)) * logit_scale).astype(jnp.bfloat16)
    g_q = product('bhqk,bkhd->bqhd', d_logit, saved['k_heads'])
    g_k = product('bhqk,bqhd->bkhd', d_logit, saved['q_heads'])
    d_qkv = jnp.stack([g_q, g_k, g_v], axis=2)
    d_qkv_b = d_qkv.astype(jnp.bfloat16)
    g_w_qkv = product('btw,btchd->wchd', saved['a_in'], d_qkv_b)
    d_a = product('btchd,wchd->btw', d_qkv_b, weights['w_qkv'])
    d_norm1, g_ln1_g, g_ln1_b = norm_backward(d_a, saved['hat_1'], saved['inv_1'], weights['ln1_g'].astype(jnp.float32))
    d_zero = d_norm1 + d_mid
    d_x, g_lnp_g, g_lnp_b = norm_backward(d_zero, saved['hat_p'], saved['inv_p'], weights['lnp_g'].astype(jnp.float32))
    d_head = jnp.sum(d_x[:, 0], axis=0)
    d_emb = d_x[:, 1:]
    d_emb_b = d_emb.astype(jnp.bfloat16)
    pos_rest = jax.ops.segment_sum(d_emb_b.astype(jnp.float32).reshape(-1, d_model), saved['keep'].reshape(-1), num_segments=NUM_PATCHES)
    g_pos = jnp.concatenate([d_head[None], pos_rest], axis=0)
    return dict(w_patch=product('bkq,bkw->qw', saved['kept_rows'], d_emb_b), b_patch=jnp.sum(d_emb, axis=(0, 1)), pos_table=g_pos, cls_tok=d_head, lnp_g=g_lnp_g, lnp_b=g_lnp_b, ln1_g=g_ln1_g, ln1_b=g_ln1_b, w_qkv=g_w_qkv, b_qkv=jnp.sum(d_qkv, axis=(0, 1)).reshape(-1), w_out=g_w_out, b_out=jnp.sum(d_mid, axis=(0, 1)), ln2_g=g_ln2_g, ln2_b=g_ln2_b, w_fc=g_w_fc, b_fc=jnp.sum(d_pre, axis=(0, 1)), w_proj=g_w_proj, b_proj=jnp.sum(d_h, axis=(0, 1)))


def reference(patches, keep, w_patch, b_patch, pos_table, cls_tok, lnp_g, lnp_b, ln1_g, ln1_b, w_qkv, b_qkv, w_out, b_out, ln2_g, ln2_b, w_fc, b_fc, w_proj, b_proj, grad_h1):
    masters = (w_patch, b_patch, pos_table, cls_tok, lnp_g, lnp_b, ln1_g, ln1_b, w_qkv, b_qkv, w_out, b_out, ln2_g, ln2_b, w_fc, b_fc, w_proj, b_proj)
    full_w = {name: value.astype(jnp.bfloat16) for name, value in zip(PARAM_NAMES, masters)}
    n_blocks = BATCH_SIZE // BLOCK_IMAGES

    def split_blocks(array_in):
        return array_in.reshape((n_blocks, BLOCK_IMAGES) + array_in.shape[1:])

    def scan_step(running, block_in):
        h_one, saved = forward(full_w, block_in[0], block_in[1])
        grad_map = backward(full_w, saved, block_in[2])
        return {name: running[name] + grad_map[name] for name in PARAM_NAMES}, h_one

    zero_grads = {name: jnp.zeros(value.shape, jnp.float32) for name, value in zip(PARAM_NAMES, masters)}
    totals, h_blocks = lax.scan(scan_step, zero_grads, (split_blocks(patches), split_blocks(keep), split_blocks(grad_h1)))
    h_out = h_blocks.reshape(BATCH_SIZE, TOKENS, MODEL_WIDTH)
    return (h_out, totals['w_patch'], totals['b_patch'], totals['pos_table'], totals['cls_tok'], totals['lnp_g'], totals['lnp_b'], totals['ln1_g'], totals['ln1_b'], totals['w_qkv'], totals['b_qkv'], totals['w_out'], totals['b_out'], totals['ln2_g'], totals['ln2_b'], totals['w_fc'], totals['b_fc'], totals['w_proj'], totals['b_proj'])
```

```python
import functools

import jax
import jax.numpy as jnp
from jax import lax
from jax.sharding import PartitionSpec as P
from jax.experimental import pallas as pl
from jax.experimental.pallas import tpu as pltpu


F32, BF16 = jnp.float32, jnp.bfloat16
LN_EPS = 1e-5
INV_SQRT2 = 0.7071067811865476
INV_SQRT_2PI = 0.3989422804014327
TOK = 50
ROWS = 200
GROUP = 8
VEC_ROW = 976
N_VEC = 10
WIN = 112
LOG2E = 1.4426950408889634
MASKED = -1e30
ALL_VMEM = 67043328


def dot(left, right):
    return jnp.dot(left, right, preferred_element_type=F32)


def dot_nt(left, right):
    return lax.dot_general(left, right, (((1,), (1,)), ((), ())), preferred_element_type=F32)


def dot_tn(left, right):
    return lax.dot_general(left, right, (((0,), (0,)), ((), ())), preferred_element_type=F32)


def held(shape):
    return pl.BlockSpec(shape, lambda *_: (0,) * len(shape), pipeline_mode=pl.Buffered(1))


def rows_spec(n_rows, width):
    return pl.BlockSpec((n_rows, width), lambda i, *_: (i, 0))


ANY = pl.BlockSpec(memory_space=pl.ANY)


def params(n_grid, vmem):
    return pltpu.CompilerParams(dimension_semantics=(pltpu.ARBITRARY,) * n_grid, vmem_limit_bytes=vmem)


def ordered(kernel, n_in, n_after):
    def body(*refs):
        return kernel(*refs[:n_in], *refs[n_in + n_after:])

    return body


def call(kernel, after, args, *, prefetch=None, grid, in_specs, out_specs, out_shape, scratch_shapes=(), cost_estimate, vmem=ALL_VMEM):
    n_pre = 0 if prefetch is None else 1
    return pl.pallas_call(
        ordered(kernel, n_pre + len(args), len(after)),
        grid_spec=pltpu.PrefetchScalarGridSpec(
            num_scalar_prefetch=n_pre, grid=grid, in_specs=list(in_specs) + [ANY] * len(after),
            out_specs=out_specs, scratch_shapes=list(scratch_shapes)),
        out_shape=out_shape, compiler_params=params(len(grid), vmem), cost_estimate=cost_estimate,
    )(*(() if prefetch is None else (prefetch,)), *args, *after)


def shaped(shape, dtype):
    return jax.ShapeDtypeStruct(shape, dtype)


def cost(flops, n_bytes, trans=0):
    return pl.CostEstimate(flops=int(flops), bytes_accessed=int(n_bytes), transcendentals=int(trans))


def normalize(x):
    centered = x - jnp.mean(x, axis=-1, keepdims=True)
    inv = lax.rsqrt(jnp.mean(centered * centered, axis=-1, keepdims=True) + LN_EPS)
    return centered * inv, inv


def norm_grad(d_out, x_hat, inv, gain):
    d_hat = d_out * gain
    return inv * (d_hat - jnp.mean(d_hat, axis=-1, keepdims=True) - x_hat * jnp.mean(d_hat * x_hat, axis=-1, keepdims=True))


def image_of(row):
    return (row >= TOK).astype(jnp.int32) + (row >= 2 * TOK).astype(jnp.int32) + (row >= 3 * TOK).astype(jnp.int32)


def pack_kernel(wt_ref, pt_ref, *refs):
    vec_refs, out_ref, rows_ref, pos_ref = refs[:N_VEC + 2], refs[-3], refs[-2], refs[-1]
    n_pix, n_pos = wt_ref.shape[1], pt_ref.shape[1]
    out_ref[:, :n_pix] = wt_ref[...].astype(BF16)
    out_ref[:, n_pix:n_pix + 128] = pt_ref[:, :128].astype(BF16)
    rows_ref[...] = jnp.zeros_like(rows_ref)
    pos_ref[...] = jnp.zeros_like(pos_ref)
    pos_ref[:, :n_pos - 128] = pt_ref[:, 128:]
    at = VEC_ROW % 128
    for ref in vec_refs:
        for j in range(ref.shape[1] // 64):
            rows_ref[at:at + 1, :64] = ref[:, j * 64:(j + 1) * 64]
            at += 1
    out_ref[:, n_pix + 128:] = (pos_ref[...] + rows_ref[...].T[:64]).astype(BF16)


def pack_small(wt, pt, vecs):
    args = [wt, pt] + vecs
    return call(pack_kernel, (), args, grid=(1,), in_specs=[held(x.shape) for x in args],
                out_specs=pl.BlockSpec((64, 1024), lambda *_: (0, 0)), out_shape=shaped((64, 1024), BF16),
                scratch_shapes=[pltpu.VMEM((128, 128), F32), pltpu.VMEM((64, 128), F32)],
                cost_estimate=cost(1e6, 1e6))


def gather_kernel(keep_ref, patches_ref, g_ref, zo_ref, gi_ref, pad_ref):
    n_patch, _, n_pix = patches_ref.shape
    n_rows = GROUP * TOK
    pad_ref[...] = jnp.zeros_like(pad_ref)
    pad_ref[:, :TOK - 1] = keep_ref[...].astype(F32)
    image = lax.broadcasted_iota(jnp.int32, pad_ref.shape, 0)
    lane = lax.broadcasted_iota(jnp.int32, pad_ref.shape, 1)
    spread = jnp.zeros(pad_ref.shape, F32)
    for b in range(GROUP):
        spread = jnp.where(image == b, pltpu.roll(pad_ref[...], TOK * b + 1, 1), spread)
    own = (lane > TOK * image) & (lane < TOK * image + TOK)
    source = jnp.sum(jnp.where(own, spread * GROUP + image.astype(F32), 0.0), axis=0, keepdims=True)
    token = jnp.sum(jnp.where(own, spread + 1.0, 0.0), axis=0, keepdims=True)
    kept = jnp.sum(jnp.where(own, 1.0, 0.0), axis=0, keepdims=True)
    source = jnp.where(kept > 0.0, source, -1.0)
    cols = jnp.where(image == 0, source, token).T
    source, token = cols[:n_rows, 0:1].astype(jnp.int32), cols[:n_rows, 1:2].astype(jnp.int32)
    pick = (lax.broadcasted_iota(jnp.int32, (n_rows, GROUP * n_patch), 1) == source).astype(F32).astype(BF16)
    zo_ref[:, :n_pix] = dot(pick, patches_ref.reshape(GROUP * n_patch, n_pix)[...]).astype(BF16)
    wide = zo_ref.shape[1] - n_pix
    zo_ref[:, n_pix:] = (lax.broadcasted_iota(jnp.int32, (n_rows, wide), 1) == token).astype(F32).astype(BF16)
    row = lax.broadcasted_iota(jnp.int32, (n_rows, n_rows), 0)
    col = lax.broadcasted_iota(jnp.int32, (n_rows, n_rows), 1)
    move = (row == (col & (GROUP - 1)) * TOK + (col >> 3)).astype(F32).astype(BF16)
    gi_ref[...] = dot(move, g_ref.reshape(n_rows, g_ref.shape[2])[...]).astype(BF16)


def gather_rows(keep, patches_t, g_t, width):
    n_patch, n_img, n_pix = patches_t.shape
    d = g_t.shape[2]
    n_tok = n_img * TOK
    three = lambda s: pl.BlockSpec((s[0], GROUP, s[2]), lambda i: (0, i, 0))
    return call(gather_kernel, (), (keep, patches_t, g_t), grid=(n_img // GROUP,),
                in_specs=[pl.BlockSpec((GROUP, TOK - 1), lambda i: (i, 0)), three(patches_t.shape), three(g_t.shape)],
                out_specs=[rows_spec(GROUP * TOK, width), rows_spec(GROUP * TOK, d)],
                out_shape=[shaped((n_tok, width), BF16), shaped((n_tok, d), BF16)],
                scratch_shapes=[pltpu.VMEM((GROUP, 512), F32)],
                cost_estimate=cost(2 * n_tok * n_patch * n_pix * GROUP, patches_t.size * 2 + n_tok * (width + 2 * d) * 2))


def embed_kernel(zo_ref, wt_ref, x0_ref, a_ref, vec_ref, bq_ref, bf_ref):
    @pl.when(pl.program_id(0) == 0)
    def _():
        base = VEC_ROW // 128 * 128
        rows = wt_ref[:, base:base + 128].astype(F32).T
        vec_ref[...] = rows[VEC_ROW - base:VEC_ROW - base + 32]
        at = N_VEC
        for ref in (bq_ref, bf_ref):
            n = ref.shape[1] // vec_ref.shape[1]
            chunk = lambda q: vec_ref[at + q % n:at + q % n + 1, q // n * 64:(q // n + 1) * 64]
            for tile in range(ref.shape[1] // 128):
                ref[:, tile * 128:(tile + 1) * 128] = jnp.concatenate([chunk(2 * tile), chunk(2 * tile + 1)], axis=1)
            at += n

    row = lax.broadcasted_iota(jnp.int32, (ROWS, 1), 0)
    is_cls = row == TOK * image_of(row)
    x0 = dot_nt(zo_ref[...], wt_ref[...]) + jnp.where(is_cls, vec_ref[1:2, :], vec_ref[0:1, :])
    x0_ref[...] = x0
    hat, _ = normalize(x0)
    h0 = hat * vec_ref[2:3, :] + vec_ref[3:4, :]
    hat1, _ = normalize(h0)
    a_ref[...] = (hat1 * vec_ref[4:5, :] + vec_ref[5:6, :]).astype(BF16)


def embed(zo, wt, d_mlp):
    n_tok, width = zo.shape
    d = wt.shape[0]
    whole = lambda s: pl.BlockSpec(s, lambda i: (0, 0))
    return call(embed_kernel, (), (zo, wt), grid=(n_tok // ROWS,),
                in_specs=[rows_spec(ROWS, width), held(wt.shape)],
                out_specs=[rows_spec(ROWS, d), rows_spec(ROWS, d), whole((32, d)), whole((1, 3 * d)), whole((1, d_mlp))],
                out_shape=[shaped((n_tok, d), F32), shaped((n_tok, d), BF16), shaped((32, d), F32), shaped((1, 3 * d), F32), shaped((1, d_mlp), F32)],
                cost_estimate=cost(2 * n_tok * width * d, n_tok * (width * 2 + d * 6)))


def window_mask(start):
    key = lax.broadcasted_iota(jnp.int32, (WIN, 2 * WIN), 0)
    qry = lax.broadcasted_iota(jnp.int32, (WIN, 2 * WIN), 1)
    qry = jnp.where(qry >= WIN, qry - WIN, qry)
    return jnp.where(image_of(key + start) == image_of(qry + start), 0.0, MASKED)


STARTS = (0, ROWS - WIN)
FWD_PAIRS = 8
BWD_PAIRS = 8


def split_heads(x):
    first = lax.broadcasted_iota(jnp.int32, x.shape, 1) < 64
    zero = jnp.zeros_like(x)
    return jnp.concatenate([jnp.where(first, x, zero), jnp.where(first, zero, x)], axis=0)


def join_heads(x):
    first = lax.broadcasted_iota(jnp.int32, (WIN, x.shape[1]), 1) < 64
    return jnp.where(first, x[:WIN], x[WIN:])


def join_windows(lo, hi):
    row8 = lax.broadcasted_iota(jnp.int32, (8, lo.shape[1]), 0)
    edge = jnp.where(row8 < 2 * TOK - 96, lo[96:104], hi[8:16])
    return jnp.concatenate([lo[:96], edge, hi[16:]], axis=0)


def attend_kernel(scale, a_ref, w_ref, b_ref, qkv_ref, o_ref, mask_ref):
    d = o_ref.shape[1]

    @pl.when(pl.program_id(0) == 0)
    def _():
        for i, start in enumerate(STARTS):
            mask_ref[i] = window_mask(start)

    a = a_ref[...]
    for j in range(0, 3 * d, 512):
        qkv_ref[:, j:j + 512] = (dot(a, w_ref[:, j:j + 512]) + b_ref[:, j:j + 512]).astype(BF16)

    def head_group(step, carry):
        lanes = [[pl.ds(pl.multiple_of((step * FWD_PAIRS + g) * 128 + part * d, 128), 128) for part in range(3)] for g in range(FWD_PAIRS)]
        units = [(g, i) for g in range(FWD_PAIRS) for i in range(2)]
        read = lambda part, g, i: qkv_ref[STARTS[i]:STARTS[i] + WIN, lanes[g][part]]
        s = [dot_nt(read(1, g, i), split_heads(read(0, g, i))) * scale + mask_ref[i] for g, i in units]
        e = [jnp.exp(x - jnp.max(x, axis=0, keepdims=True)) for x in s]
        p = [(x * (1.0 / jnp.sum(x, axis=0, keepdims=True))).astype(BF16) for x in e]
        o = [join_heads(dot_tn(x, read(2, g, i))) for x, (g, i) in zip(p, units)]
        for g in range(FWD_PAIRS):
            o_ref[:, lanes[g][0]] = join_windows(o[2 * g], o[2 * g + 1]).astype(BF16)
        return carry

    lax.fori_loop(0, d // (128 * FWD_PAIRS), head_group, 0)


def attend(a, w_qkv, b_qkv, scale):
    n_tok, d = a.shape
    return call(functools.partial(attend_kernel, scale), (), (a, w_qkv, b_qkv), grid=(n_tok // ROWS,),
                in_specs=[rows_spec(ROWS, d), held(w_qkv.shape), held(b_qkv.shape)],
                out_specs=[rows_spec(ROWS, 3 * d), rows_spec(ROWS, d)],
                out_shape=[shaped((n_tok, 3 * d), BF16), shaped((n_tok, d), BF16)],
                scratch_shapes=[pltpu.VMEM((2, WIN, 2 * WIN), F32)],
                cost_estimate=cost(2 * n_tok * d * 3 * d * 1.8, n_tok * d * 10))


def attend_grad_kernel(scale, qkv_ref, dctx_ref, dqkv_ref, bsum_ref, mask_ref):
    d = dctx_ref.shape[1]

    @pl.when(pl.program_id(0) == 0)
    def _():
        for i, start in enumerate(STARTS):
            mask_ref[i] = window_mask(start)
        bsum_ref[...] = jnp.zeros_like(bsum_ref)

    def head_group(step, carry):
        lanes = [[pl.ds(pl.multiple_of((step * BWD_PAIRS + g) * 128 + part * d, 128), 128) for part in range(3)] for g in range(BWD_PAIRS)]
        units = [(g, i) for g in range(BWD_PAIRS) for i in range(2)]
        read = lambda part, g, i: qkv_ref[STARTS[i]:STARTS[i] + WIN, lanes[g][part]]
        q2 = [split_heads(read(0, g, i)) for g, i in units]
        do2 = [split_heads(dctx_ref[STARTS[i]:STARTS[i] + WIN, lanes[g][0]]) for g, i in units]
        s = [dot_nt(read(1, g, i), q) * scale + mask_ref[i] for q, (g, i) in zip(q2, units)]
        dp = [dot_nt(read(2, g, i), do) for do, (g, i) in zip(do2, units)]
        e = [jnp.exp(x - jnp.max(x, axis=0, keepdims=True)) for x in s]
        p = [x * (1.0 / jnp.sum(x, axis=0, keepdims=True)) for x in e]
        dv = [dot(x.astype(BF16), do) for x, do in zip(p, do2)]
        ds = [(x * (y - jnp.sum(x * y, axis=0, keepdims=True)) * scale).astype(BF16) for x, y in zip(p, dp)]
        dk = [dot(x, q) for x, q in zip(ds, q2)]
        dq = [join_heads(dot_tn(x, read(1, g, i))) for x, (g, i) in zip(ds, units)]
        for g in range(BWD_PAIRS):
            for part, grad in enumerate((dq, dk, dv)):
                both = join_windows(grad[2 * g], grad[2 * g + 1])
                dqkv_ref[:, lanes[g][part]] = both.astype(BF16)
                bsum_ref[:, lanes[g][part]] += jnp.sum(both, axis=0, keepdims=True)
        return carry

    lax.fori_loop(0, d // (128 * BWD_PAIRS), head_group, 0)


def attend_grad(qkv, d_ctx, scale, after):
    n_tok, d = d_ctx.shape
    return call(functools.partial(attend_grad_kernel, scale), after, (qkv, d_ctx), grid=(n_tok // ROWS,),
                in_specs=[rows_spec(ROWS, 3 * d), rows_spec(ROWS, d)],
                out_specs=[rows_spec(ROWS, 3 * d), pl.BlockSpec((1, 3 * d), lambda i: (0, 0))],
                out_shape=[shaped((n_tok, 3 * d), BF16), shaped((1, 3 * d), F32)],
                scratch_shapes=[pltpu.VMEM((2, WIN, 2 * WIN), F32)],
                cost_estimate=cost(31e9 * n_tok / 3200, n_tok * d * 14))


def mlp_up_kernel(o_ref, x0_ref, wo_ref, wf_ref, vec_ref, bf_ref, m_ref, c_ref, act_ref, slope_ref):
    hat, _ = normalize(x0_ref[...])
    m = hat * vec_ref[2:3, :] + vec_ref[3:4, :] + dot(o_ref[...], wo_ref[...]) + vec_ref[6:7, :]
    m_ref[...] = m
    hat2, _ = normalize(m)
    c = (hat2 * vec_ref[7:8, :] + vec_ref[8:9, :]).astype(BF16)
    c_ref[...] = c
    step = 1024
    n_mlp = wf_ref.shape[1]

    def finish(at, u):
        w = u * INV_SQRT2
        cdf = 0.5 + 0.5 * lax.erf(w)
        act_ref[:, at:at + step] = (u * cdf).astype(BF16)
        slope_ref[:, at:at + step] = cdf + u * (jnp.exp2((w * w) * (-LOG2E)) * INV_SQRT_2PI)

    held_u = None
    for at in range(0, n_mlp, step):
        u = dot(c, wf_ref[:, at:at + step]) + bf_ref[:, at:at + step]
        if held_u is not None:
            finish(*held_u)
        held_u = (at, u)
    finish(*held_u)


def mlp_up(o, x0, w_out, w_fc, vecs, b_fc):
    n_tok, d = o.shape
    f = w_fc.shape[1]
    return call(mlp_up_kernel, (), (o, x0, w_out, w_fc, vecs, b_fc), grid=(n_tok // ROWS,),
                in_specs=[rows_spec(ROWS, d), rows_spec(ROWS, d), held(w_out.shape), held(w_fc.shape), held(vecs.shape), held(b_fc.shape)],
                out_specs=[rows_spec(ROWS, d), rows_spec(ROWS, d), rows_spec(ROWS, f), rows_spec(ROWS, f)],
                out_shape=[shaped((n_tok, d), F32), shaped((n_tok, d), BF16), shaped((n_tok, f), BF16), shaped((n_tok, f), F32)],
                cost_estimate=cost(2 * n_tok * d * (d + f) * 1.5, n_tok * (d * 12 + f * 6), 2 * n_tok * f))


def mlp_down_kernel(act_ref, m_ref, w_ref, vec_ref, h1_ref):
    n_rows = GROUP * TOK
    h1 = (m_ref[...] + dot(act_ref[...], w_ref[...]) + vec_ref[9:10, :]).astype(BF16)
    row = lax.broadcasted_iota(jnp.int32, (n_rows, n_rows), 0)
    col = lax.broadcasted_iota(jnp.int32, (n_rows, n_rows), 1)
    move = (col == (row & (GROUP - 1)) * TOK + (row >> 3)).astype(F32).astype(BF16)
    h1_ref.reshape(n_rows, h1_ref.shape[2])[...] = dot(move, h1).astype(BF16)


def mlp_down(act, m, w_proj, vecs, after):
    n_tok, f = act.shape
    d = m.shape[1]
    return call(mlp_down_kernel, after, (act, m, w_proj, vecs), grid=(n_tok // GROWS,),
                in_specs=[rows_spec(GROWS, f), rows_spec(GROWS, d), held(w_proj.shape), held(vecs.shape)],
                out_specs=pl.BlockSpec((TOK, GROUP, d), lambda i: (0, i, 0)),
                out_shape=shaped((TOK, n_tok // TOK, d), BF16),
                cost_estimate=cost(2.2 * n_tok * d * f, n_tok * (d * 6 + f * 2)))


GROWS = 400


def mlp_grad_kernel(g_ref, slope_ref, m_ref, wp_ref, wf_ref, wo_ref, vec_ref,
                    dpre_ref, dmid_ref, dmidb_ref, dctx_ref, vsum_ref, bfc_ref):
    @pl.when(pl.program_id(0) == 0)
    def _():
        vsum_ref[...] = jnp.zeros_like(vsum_ref)
        bfc_ref[...] = jnp.zeros_like(bfc_ref)

    g = g_ref[...]
    step = 512
    d_c = None
    held_d = None
    for at in range(0, wp_ref.shape[0], step):
        d_act = dot_nt(g, wp_ref[at:at + step, :])
        if held_d is not None:
            part = dot_nt(held_d[1], wf_ref[:, held_d[0]:held_d[0] + step])
            d_c = part if d_c is None else d_c + part
        d_pre = d_act * slope_ref[:, at:at + step]
        bfc_ref[:, at:at + step] += jnp.sum(d_pre, axis=0, keepdims=True)
        d_pre_b = d_pre.astype(BF16)
        dpre_ref[:, at:at + step] = d_pre_b
        held_d = (at, d_pre_b)
    d_c = d_c + dot_nt(held_d[1], wf_ref[:, held_d[0]:held_d[0] + step])
    hat2, inv2 = normalize(m_ref[...])
    g_f = g.astype(F32)
    d_mid = norm_grad(d_c, hat2, inv2, vec_ref[7:8, :]) + g_f
    dmid_ref[...] = d_mid
    d_mid_b = d_mid.astype(BF16)
    dmidb_ref[...] = d_mid_b
    dctx_ref[...] = dot_nt(d_mid_b, wo_ref[...]).astype(BF16)
    vsum_ref[0:1, :] += jnp.sum(d_mid, axis=0, keepdims=True)
    vsum_ref[1:2, :] += jnp.sum(d_c * hat2, axis=0, keepdims=True)
    vsum_ref[2:3, :] += jnp.sum(d_c, axis=0, keepdims=True)
    vsum_ref[3:4, :] += jnp.sum(g_f, axis=0, keepdims=True)


def mlp_grad(g, slope, m, w_proj, w_fc, w_out, vecs, after):
    n_tok, d = g.shape
    f = slope.shape[1]
    whole = lambda s: pl.BlockSpec(s, lambda i: (0, 0))
    return call(mlp_grad_kernel, after, (g, slope, m, w_proj, w_fc, w_out, vecs), grid=(n_tok // GROWS,),
                in_specs=[rows_spec(GROWS, d), rows_spec(GROWS, f), rows_spec(GROWS, d),
                          held(w_proj.shape), held(w_fc.shape), held(w_out.shape), held(vecs.shape)],
                out_specs=[rows_spec(GROWS, f), rows_spec(GROWS, d), rows_spec(GROWS, d), rows_spec(GROWS, d), whole((8, d)), whole((1, f))],
                out_shape=[shaped((n_tok, f), BF16), shaped((n_tok, d), F32), shaped((n_tok, d), BF16), shaped((n_tok, d), BF16),
                           shaped((8, d), F32), shaped((1, f), F32)],
                cost_estimate=cost(2 * n_tok * d * (2 * f + d), n_tok * (d * 14 + f * 6)))


def embed_grad_kernel(dqkv_ref, dmid_ref, x0_ref, w_ref, vec_ref, demb_ref, vsum_ref):
    @pl.when(pl.program_id(0) == 0)
    def _():
        vsum_ref[...] = jnp.zeros_like(vsum_ref)

    d_a = dot_nt(dqkv_ref[...], w_ref[...])
    hat_p, inv_p = normalize(x0_ref[...])
    hat1, inv1 = normalize(hat_p * vec_ref[2:3, :] + vec_ref[3:4, :])
    d_zero = norm_grad(d_a, hat1, inv1, vec_ref[4:5, :]) + dmid_ref[...]
    d_x = norm_grad(d_zero, hat_p, inv_p, vec_ref[2:3, :])
    demb_ref[...] = d_x.astype(BF16)
    row = lax.broadcasted_iota(jnp.int32, (ROWS, 1), 0)
    d_cls = jnp.sum(jnp.where(row == TOK * image_of(row), d_x, 0.0), axis=0, keepdims=True)
    vsum_ref[0:1, :] += jnp.sum(jnp.where(row == TOK * image_of(row), 0.0, d_x), axis=0, keepdims=True)
    vsum_ref[1:2, :] += d_cls
    vsum_ref[2:3, :] += jnp.sum(d_zero * hat_p, axis=0, keepdims=True)
    vsum_ref[3:4, :] += jnp.sum(d_zero, axis=0, keepdims=True)
    vsum_ref[4:5, :] += jnp.sum(d_a * hat1, axis=0, keepdims=True)
    vsum_ref[5:6, :] += jnp.sum(d_a, axis=0, keepdims=True)


def embed_grad(dqkv, d_mid, x0, w_qkv, vecs, after):
    n_tok, d = d_mid.shape
    return call(embed_grad_kernel, after, (dqkv, d_mid, x0, w_qkv, vecs), grid=(n_tok // ROWS,),
                in_specs=[rows_spec(ROWS, 3 * d), rows_spec(ROWS, d), rows_spec(ROWS, d), held(w_qkv.shape), held(vecs.shape)],
                out_specs=[rows_spec(ROWS, d), pl.BlockSpec((8, d), lambda i: (0, 0))],
                out_shape=[shaped((n_tok, d), BF16), shaped((8, d), F32)],
                cost_estimate=cost(2.5 * n_tok * d * 3 * d, n_tok * d * 16))


def tail_kernel(se_ref, sm_ref, sq_ref, sf_ref, out_ref, rows_ref):
    d = se_ref.shape[1]
    rows_ref[...] = jnp.zeros_like(rows_ref)
    at = VEC_ROW % 128
    rows_ref[at:at + 6, :] = se_ref[:6, :]
    rows_ref[at + 6:at + N_VEC, :] = sm_ref[:4, :]
    at += N_VEC
    for ref in (sq_ref, sf_ref):
        n = ref.shape[1] // d
        for r in range(n):
            for j in range(d // 128):
                chunk = lambda q: ref[:, (n * q + r) * 64:(n * q + r + 1) * 64]
                rows_ref[at + r:at + r + 1, j * 128:(j + 1) * 128] = jnp.concatenate([chunk(2 * j), chunk(2 * j + 1)], axis=1)
        at += n
    for j in range(d // 128):
        cols = rows_ref[:, j * 128:(j + 1) * 128].T
        out_ref[0, j * 64:(j + 1) * 64] = cols[:64]
        out_ref[1, j * 64:(j + 1) * 64] = cols[64:]


def vector_tail(sums_e, sums_m, sum_qkv, sum_fc):
    args = (sums_e, sums_m, sum_qkv, sum_fc)
    d = sums_e.shape[1]
    return call(tail_kernel, (), args, grid=(1,), in_specs=[held(x.shape) for x in args],
                out_specs=pl.BlockSpec((2, d // 2, 128), lambda i: (0, 0, 0)), out_shape=shaped((2, d // 2, 128), F32),
                scratch_shapes=[pltpu.VMEM((128, d), F32)], cost_estimate=cost(1e6, 1e6))


LINKS = ('core', 'x', 'y', 'z')
GRID = ('z', 'y', 'x')
ORDERS = (('x', 'y', 'z'), ('y', 'z', 'x'), ('z', 'x', 'y'))


def bit(me, link):
    return (me >> LINKS.index(link)) & 1


def transposed_halves(a_ref, at_ref):
    for j in range(a_ref.shape[1] // 128):
        t = a_ref[:, j * 128:(j + 1) * 128].T
        at_ref[0, j * 64:(j + 1) * 64, :] = t[:64]
        at_ref[1, j * 64:(j + 1) * 64, :] = t[64:]


def cols_sent_kernel(has_tail, me_ref, a_ref, b_ref, *refs):
    tail_ref = refs[0] if has_tail else None
    out_ref, at_ref = refs[-2:]

    @pl.when(pl.program_id(0) == 0)
    def _():
        transposed_halves(a_ref, at_ref)

    other = 1 - bit(me_ref[0], 'core')
    out_ref[...] = dot(at_ref[other], b_ref[...])
    if has_tail:
        @pl.when(pl.program_id(0) == pl.num_programs(0) - 1)
        def _():
            out_ref[:, -128:] += tail_ref[other]


def cols_sent(me, a, b, tile, after, tail=None):
    k, m = a.shape
    n = b.shape[1]
    args = [a, b] + ([] if tail is None else [tail])
    in_specs = [held(a.shape), pl.BlockSpec((k, tile), lambda j, s: (0, j))] + ([] if tail is None else [held(tail.shape)])
    return call(functools.partial(cols_sent_kernel, tail is not None), after, args, prefetch=me, grid=(n // tile,), in_specs=in_specs,
                out_specs=pl.BlockSpec((m // 2, tile), lambda j, s: (0, j)), out_shape=shaped((m // 2, n), F32),
                scratch_shapes=[pltpu.VMEM((2, m // 2, k), BF16)],
                cost_estimate=cost(k * m * n, k * (m + n) * 2 + m * n * 2))


def half_copies(me, order, buf, send, keep, columns, sem):
    at = GRID.index(order[0])
    mine = bit(me, order[0])
    half = lambda index: buf.at[(slice(None),) * at + (index,)]
    return [pltpu.make_async_copy(half(1 - mine), send.at[:, :, :, columns], sem.at[0]),
            pltpu.make_async_copy(half(mine), keep.at[:, :, :, columns], sem.at[1])]


def cols_kept_kernel(orders, edges, tile, has_tail, me_ref, a_ref, b_ref, base_ref, *refs):
    tail_ref = refs[0] if has_tail else None
    outs, (at_ref, buf_ref, sems) = refs[has_tail:-3], refs[-3:]
    step, last = pl.program_id(0), pl.num_programs(0) - 1
    slot = step % 2

    @pl.when(step == 0)
    def _():
        transposed_halves(a_ref, at_ref)

    def landed(at):
        for copy in half_copies(me_ref[0], orders[0], buf_ref.at[at], outs[0], outs[1], pl.ds(0, tile), sems.at[at]):
            copy.wait()

    @pl.when(step >= 2)
    def _():
        landed(slot)

    mine = bit(me_ref[0], 'core')
    total = dot(at_ref[mine], b_ref[...]) + base_ref[...]
    buf_ref[slot] = total.reshape(2, 2, 2, -1, tile)
    if has_tail:
        @pl.when(step == last)
        def _():
            buf_ref[slot, :, :, :, :, tile - 128:] += tail_ref[mine].reshape(2, 2, 2, -1, 128)
    for c, order in enumerate(orders):
        lo, hi = edges[c] // tile, edges[c + 1] // tile

        @pl.when((step >= lo) & (step < hi))
        def _():
            columns = pl.ds(pl.multiple_of((step - lo) * tile, tile), tile)
            for copy in half_copies(me_ref[0], order, buf_ref.at[slot], outs[2 * c], outs[2 * c + 1], columns, sems.at[slot]):
                copy.start()

    @pl.when(step == last)
    def _():
        landed(1 - slot)
        landed(slot)


def cols_kept(me, a, b, base, tile, orders, edges, after, tail=None):
    k, m = a.shape
    n = b.shape[1]
    r = m // 16
    args = [a, b, base] + ([] if tail is None else [tail])
    in_specs = [held(a.shape), pl.BlockSpec((k, tile), lambda j, s: (0, j)), pl.BlockSpec((m // 2, tile), lambda j, s: (0, j))]
    in_specs += [] if tail is None else [held(tail.shape)]
    shapes = [shaped((2, 2, r, hi - lo), F32) for lo, hi in zip(edges, edges[1:]) for _ in range(2)]
    return call(functools.partial(cols_kept_kernel, orders, edges, tile, tail is not None), after, args, prefetch=me, grid=(n // tile,),
                in_specs=in_specs, out_specs=[ANY] * len(shapes), out_shape=shapes,
                scratch_shapes=[pltpu.VMEM((2, m // 2, k), BF16), pltpu.VMEM((2, 2, 2, 2, r, tile), F32), pltpu.SemaphoreType.DMA((2, 2))],
                cost_estimate=cost(k * m * n, k * (m + n) * 2 + m * n * 4))


def rows_sent_kernel(me_ref, a_ref, b_ref, out_ref):
    out_ref[...] = dot_tn(a_ref[...], b_ref[...])


def rows_sent(me, a, b, after):
    k, m = a.shape
    n = b.shape[1]
    r = m // 16
    return call(rows_sent_kernel, after, (a, b), prefetch=me, grid=(8,),
                in_specs=[pl.BlockSpec((k, r), lambda j, s: (0, 2 * j + 1 - bit(s[0], 'core'))), held(b.shape)],
                out_specs=pl.BlockSpec((r, n), lambda j, s: (j, 0)), out_shape=shaped((m // 2, n), F32),
                cost_estimate=cost(k * m * n, k * (m + n) * 2 + m * n * 2))


def rows_kept_kernel(orders, edges, me_ref, a_ref, b_ref, base_ref, *refs):
    outs, (buf_ref, sems) = refs[:-2], refs[-2:]
    step, last = pl.program_id(0), pl.num_programs(0) - 1
    slot = step % 2

    def copies(c, at, chip, wanted):
        rest = [(chip >> (LINKS.index(link) - 1)) & 1 for link in GRID if link != orders[c][0]]
        source = buf_ref.at[at, :, pl.ds(edges[c], edges[c + 1] - edges[c])]
        return pltpu.make_async_copy(source, outs[2 * c + wanted].at[rest[0], rest[1]], sems.at[at, c])

    def landed(at):
        for c in range(len(orders)):
            copies(c, at, 0, 0).wait()

    @pl.when(step >= 2)
    def _():
        landed(slot)

    buf_ref[slot] = dot_tn(a_ref[...], b_ref[...]) + base_ref[...]
    for c, order in enumerate(orders):
        same = ((step >> (LINKS.index(order[0]) - 1)) & 1) == bit(me_ref[0], order[0])
        for wanted in range(2):
            @pl.when(same if wanted else jnp.logical_not(same))
            def _():
                copies(c, slot, step, wanted).start()

    @pl.when(step == last)
    def _():
        landed(1 - slot)
        landed(slot)


def rows_kept(me, a, b, base, orders, edges, after):
    k, m = a.shape
    n = b.shape[1]
    r = m // 16
    shapes = [shaped((2, 2, r, hi - lo), F32) for lo, hi in zip(edges, edges[1:]) for _ in range(2)]
    return call(functools.partial(rows_kept_kernel, orders, edges), after, (a, b, base), prefetch=me, grid=(8,),
                in_specs=[pl.BlockSpec((k, r), lambda j, s: (0, 2 * j + bit(s[0], 'core'))), held(b.shape), pl.BlockSpec((r, n), lambda j, s: (j, 0))],
                out_specs=[ANY] * len(shapes), out_shape=shapes,
                scratch_shapes=[pltpu.VMEM((2, r, n), F32), pltpu.SemaphoreType.DMA((2, len(orders)))],
                cost_estimate=cost(k * m * n, k * (m + n) * 2 + m * n * 4))


def add_pairs_kernel(me_ref, *refs):
    n = len(refs) // 3
    for i in range(n):
        refs[2 * n + i][...] = refs[2 * i][...] + refs[2 * i + 1][...]


def next_halves(me, items, level, after):
    args, in_specs, shapes, out_specs = [], [], [], []
    for order, kept, received in items:
        links = [link for link in GRID if link not in order[:level]]
        at = links.index(order[level])
        r, n = kept.shape[-2:]
        for keep in range(2):
            def index(i, s, keep=keep, at=at, n_links=len(links), link=order[level]):
                mine = bit(s[0], link)
                lead = [i] * n_links
                lead[at] = mine if keep else 1 - mine
                return tuple(lead) + (0, 0)

            args += [kept, received]
            in_specs += [pl.BlockSpec((None,) * len(links) + (r, n), index)] * 2
            if len(links) == 2:
                shapes.append(shaped((2, r, n), F32))
                out_specs.append(pl.BlockSpec((None, r, n), lambda i, s: (i, 0, 0)))
            else:
                shapes.append(shaped((r, n), F32))
                out_specs.append(pl.BlockSpec((r, n), lambda i, s: (0, 0)))
    total = sum(kept.size for _, kept, _ in items)
    outs = call(add_pairs_kernel, after, args, prefetch=me, grid=(2 if level == 1 else 1,), in_specs=in_specs, out_specs=out_specs,
                out_shape=shapes, cost_estimate=cost(total * 40, total * 12))
    return list(zip(outs[::2], outs[1::2]))


def join_kernel(groups, *refs):
    n = sum(groups)
    at = 0
    for out_ref, count in zip(refs[2 * n:], groups):
        lo = 0
        for _ in range(count):
            kept, received = refs[2 * at], refs[2 * at + 1]
            out_ref[:, lo:lo + kept.shape[1]] = kept[...] + received[...]
            lo += kept.shape[1]
            at += 1


def join(groups, after):
    args = [x for group in groups for pair in group for x in pair]
    r = args[0].shape[0]
    shapes = [shaped((r, sum(pair[0].shape[1] for pair in group)), F32) for group in groups]
    total = sum(x.size for x in args)
    return call(functools.partial(join_kernel, [len(group) for group in groups]), after, args, grid=(1,),
                in_specs=[held(x.shape) for x in args], out_specs=[pl.BlockSpec(s.shape, lambda i: (0, 0)) for s in shapes],
                out_shape=shapes, cost_estimate=cost(total * 20, total * 6))


def finish_kernel(n_pairs, n_pix, n_pos, *refs):
    outs, full_ref = refs[2 * n_pairs:-1], refs[-1]
    lo = 0
    for i in range(n_pairs):
        n = refs[2 * i].shape[1]
        full_ref[:, lo:lo + n] = refs[2 * i][...] + refs[2 * i + 1][...]
        lo += n
    outs[0][...] = full_ref[:, :n_pix]
    pos_ref = outs[1]
    pos_ref[:, :128] = full_ref[:, n_pix:n_pix + 128]
    pos_ref[:, 128:] = full_ref[:, n_pix + 128:n_pix + n_pos]
    pos_ref[:, 0:1] = full_ref[:, VEC_ROW + 1:VEC_ROW + 2]
    base = VEC_ROW // 128 * 128
    rows = full_ref[:, base:base + 128].T
    at = VEC_ROW - base
    for ref in outs[2:]:
        n = ref.shape[1] // 64
        if n == 1:
            ref[...] = rows[at:at + 1]
        else:
            ref[...] = jnp.concatenate([rows[at + j:at + j + 1] for j in range(n)], axis=1)
        at += n


def finish(pairs, n_pix, n_pos, widths, after):
    args = [x for pair in pairs for x in pair]
    shapes = [shaped((64, n_pix), F32), shaped((64, n_pos), F32)] + [shaped((1, w), F32) for w in widths]
    return call(functools.partial(finish_kernel, len(pairs), n_pix, n_pos), after, args, grid=(1,), in_specs=[held(x.shape) for x in args],
                out_specs=[pl.BlockSpec(s.shape, lambda i: (0, 0)) for s in shapes], out_shape=shapes,
                scratch_shapes=[pltpu.VMEM((64, 1024), F32)], cost_estimate=cost(1e6, 1e6))


MESH_AXIS = 'fsdp'
PARAM_NAMES = ('w_patch', 'b_patch', 'pos_table', 'cls_tok', 'lnp_g', 'lnp_b', 'ln1_g', 'ln1_b', 'w_qkv', 'b_qkv', 'w_out', 'b_out', 'ln2_g', 'ln2_b', 'w_fc', 'b_fc', 'w_proj', 'b_proj')
PACKED = tuple(PARAM_NAMES[i] for i in (1, 3, 4, 5, 6, 7, 11, 12, 13, 17, 9, 15))
LAST_SPLIT = PARAM_NAMES[0:3:2]


def solution(mesh):
    n_dev = mesh.shape[MESH_AXIS]

    def across(value, link):
        return lax.ppermute(value, MESH_AXIS, [(i, i ^ (1 << LINKS.index(link))) for i in range(n_dev)])

    def compute(patches, keep, *rest):
        shard = dict(zip(PARAM_NAMES, rest[:-1]))
        _, _, d = rest[-1].shape
        d_mlp = shard['w_fc'].shape[1]
        n_pix, n_pos = shard['w_patch'].shape[0], shard['pos_table'].shape[0]
        scale = shard['w_qkv'].shape[3] ** -0.5
        me = lax.axis_index(MESH_AXIS).reshape(1)

        pack = pack_small(shard['w_patch'].T, shard['pos_table'].T, [shard[name][None] for name in PACKED])

        def whole(value):
            return lax.all_gather(value, MESH_AXIS, tiled=True)

        wt = whole(pack)
        w_qkv = whole(shard['w_qkv'].astype(BF16).reshape(-1, 3 * d))
        w_out, w_fc, w_proj = (whole(shard[name].astype(BF16)) for name in ('w_out', 'w_fc', 'w_proj'))

        zo, g = gather_rows(keep, patches.transpose(1, 0, 2), rest[-1].transpose(1, 0, 2), d)
        x0, a, vecs, b_qkv, b_fc = embed(zo, wt, d_mlp)
        qkv, ctx = attend(a, w_qkv, b_qkv, scale)
        m, c, act, slope = mlp_up(ctx, x0, w_out, w_fc, vecs, b_fc)

        def cut(outs, orders):
            return [(order, outs[2 * i + 1], across(outs[2 * i], order[0])) for i, order in enumerate(orders)]

        def halve(items, level, after):
            halves = next_halves(me, items, level, after)
            return [(order, kept, across(sent, order[level])) for (order, _, _), (sent, kept) in zip(items, halves)]

        def ends(items):
            return [(kept, received) for _, kept, received in items]

        proj_sent = rows_sent(me, act, g, ())
        h1 = mlp_down(act, m, w_proj, vecs, (proj_sent,))
        outs = rows_kept(me, act, g, across(proj_sent, 'core'), ORDERS, (0, 384, 768, d), (h1,))
        proj = cut(outs, ORDERS)
        d_pre, d_mid, d_mid_b, d_ctx, sums_m, sum_fc = mlp_grad(g, slope, m, w_proj, w_fc, w_out, vecs, (outs[1],))
        fc_sent = cols_sent(me, c, d_pre, 512, ())
        proj = halve(proj, 1, (fc_sent,))
        out_sent = cols_sent(me, ctx, d_mid_b, 256, (proj[0][1],))
        outs = cols_kept(me, c, d_pre, across(fc_sent, 'core'), 256, ORDERS, (0, 1280, 2560, d_mlp), (out_sent,))
        fc = cut(outs, ORDERS)
        proj = halve(proj, 2, (outs[1],))
        outs = cols_kept(me, ctx, d_mid_b, across(out_sent, 'core'), 256, ORDERS[2:], (0, d), (proj[0][1],))
        out = cut(outs, ORDERS[2:])
        d_qkv, sum_qkv = attend_grad(qkv, d_ctx, scale, (outs[1],))
        g_proj, = join([ends(proj)], (sum_qkv,))
        qkv_sent = cols_sent(me, a, d_qkv, 512, (g_proj,))
        fc = halve(fc, 1, (qkv_sent,))
        outs = cols_kept(me, a, d_qkv, across(qkv_sent, 'core'), 256, ORDERS, (0, 1280, 2816, 3 * d), (fc[0][1],))
        qkv = cut(outs, ORDERS) + out
        d_emb, sums_e = embed_grad(d_qkv, d_mid, x0, w_qkv, vecs, (outs[1],))
        fc = halve(fc, 2, (sums_e,))
        tail = vector_tail(sums_e, sums_m, sum_qkv, sum_fc)
        small_sent = cols_sent(me, d_emb, zo, 128, (fc[0][1],), tail)
        qkv = halve(qkv, 1, (small_sent,))
        outs = cols_kept(me, d_emb, zo, across(small_sent, 'core'), 128, ORDERS, (0, 384, 768, d), (qkv[0][1],), tail)
        small = cut(outs, ORDERS)
        g_fc, = join([ends(fc)], (outs[1],))
        qkv = halve(qkv, 2, (g_fc,))
        small = halve(small, 1, (qkv[0][1],))
        g_qkv, g_out = join([ends(qkv)[:3], ends(qkv)[3:]], (small[0][1],))
        small = halve(small, 2, (g_out,))
        done = finish(ends(small), n_pix, n_pos, [shard[name].shape[0] for name in PACKED], (g_out,))

        grads = dict(w_patch=done[0].T, pos_table=done[1].T, w_qkv=g_qkv.reshape(shard['w_qkv'].shape), w_out=g_out, w_fc=g_fc, w_proj=g_proj.reshape(shard['w_proj'].shape))
        grads.update({name: value.reshape(-1) for name, value in zip(PACKED, done[2:])})
        return (h1.transpose(1, 0, 2),) + tuple(grads[name] for name in PARAM_NAMES)

    batch_spec = P(MESH_AXIS)
    param_specs = tuple(P(None, MESH_AXIS) if name in LAST_SPLIT else P(MESH_AXIS) for name in PARAM_NAMES)
    return jax.shard_map(compute, mesh=mesh, in_specs=(batch_spec, batch_spec) + param_specs + (batch_spec,), out_specs=(batch_spec,) + param_specs, check_vma=False)
```

```python
import functools

import jax
import jax.numpy as jnp
from jax import lax
from jax.sharding import PartitionSpec as P
from jax.experimental import pallas as pl
from jax.experimental.pallas import tpu as pltpu


F32, BF16 = jnp.float32, jnp.bfloat16
LN_EPS = 1e-5
INV_SQRT2 = 0.7071067811865476
INV_SQRT_2PI = 0.3989422804014327
TOK = 50
ROWS = 200
GROWS = 400
GROUP = 8
VEC_ROW = 976
N_VEC = 10
WIN = 112
LOG2E = 1.4426950408889634
MASKED = -1e30
ALL_VMEM = 67043328


def dot(left, right):
    return jnp.dot(left, right, preferred_element_type=F32)


def dot_nt(left, right):
    return lax.dot_general(left, right, (((1,), (1,)), ((), ())), preferred_element_type=F32)


def dot_tn(left, right):
    return lax.dot_general(left, right, (((0,), (0,)), ((), ())), preferred_element_type=F32)


def held(shape):
    return pl.BlockSpec(shape, lambda *_: (0,) * len(shape), pipeline_mode=pl.Buffered(1))


def held_cols(n_rows, n_cols, at):
    return pl.BlockSpec((n_rows, n_cols), lambda *_: (0, at // n_cols), pipeline_mode=pl.Buffered(1))


def rows_spec(n_rows, width):
    return pl.BlockSpec((n_rows, width), lambda i, *_: (i, 0))


ANY = pl.BlockSpec(memory_space=pl.ANY)


def params(n_grid, vmem):
    return pltpu.CompilerParams(dimension_semantics=(pltpu.ARBITRARY,) * n_grid, vmem_limit_bytes=vmem)


def ordered(kernel, n_in, n_after):
    def body(*refs):
        return kernel(*refs[:n_in], *refs[n_in + n_after:])

    return body


def call(kernel, after, args, *, prefetch=None, grid, in_specs, out_specs, out_shape, scratch_shapes=(), cost_estimate, vmem=ALL_VMEM):
    n_pre = 0 if prefetch is None else 1
    return pl.pallas_call(
        ordered(kernel, n_pre + len(args), len(after)),
        grid_spec=pltpu.PrefetchScalarGridSpec(
            num_scalar_prefetch=n_pre, grid=grid, in_specs=list(in_specs) + [ANY] * len(after),
            out_specs=out_specs, scratch_shapes=list(scratch_shapes)),
        out_shape=out_shape, compiler_params=params(len(grid), vmem), cost_estimate=cost_estimate,
    )(*(() if prefetch is None else (prefetch,)), *args, *after)


def shaped(shape, dtype):
    return jax.ShapeDtypeStruct(shape, dtype)


def cost(flops, n_bytes, trans=0):
    return pl.CostEstimate(flops=int(flops), bytes_accessed=int(n_bytes), transcendentals=int(trans))


def normalize(x):
    centered = x - jnp.mean(x, axis=-1, keepdims=True)
    inv = lax.rsqrt(jnp.mean(centered * centered, axis=-1, keepdims=True) + LN_EPS)
    return centered * inv, inv


def norm_grad(d_out, x_hat, inv, gain):
    d_hat = d_out * gain
    return inv * (d_hat - jnp.mean(d_hat, axis=-1, keepdims=True) - x_hat * jnp.mean(d_hat * x_hat, axis=-1, keepdims=True))


def image_of(row, n_img=4):
    return sum((row >= j * TOK).astype(jnp.int32) for j in range(1, n_img))


def is_class(n_rows):
    row = lax.broadcasted_iota(jnp.int32, (n_rows, 1), 0)
    return row == TOK * image_of(row, n_rows // TOK)


def this_block(n_rows, width, n):
    return pl.BlockSpec((n_rows, width), lambda i: (jnp.minimum(i, n - 1), 0))


def last_block(n_rows, width):
    return pl.BlockSpec((n_rows, width), lambda i: (jnp.maximum(i - 1, 0), 0))


def pack_kernel(wq_ref, wt_ref, pt_ref, *refs):
    vec_refs, whole_ref, rows_ref, pos_ref = refs[:N_VEC + 2], refs[-3], refs[-2], refs[-1]
    n_pix, n_pos, n_qkv = wt_ref.shape[1], pt_ref.shape[1], wq_ref.shape[1]
    whole_ref[:, :n_qkv] = wq_ref[...]
    out_ref = whole_ref.at[:, n_qkv:]
    out_ref[:, :n_pix] = wt_ref[...].astype(BF16)
    out_ref[:, n_pix:n_pix + 128] = pt_ref[:, :128].astype(BF16)
    rows_ref[...] = jnp.zeros_like(rows_ref)
    pos_ref[...] = jnp.zeros_like(pos_ref)
    pos_ref[:, :n_pos - 128] = pt_ref[:, 128:]
    at = VEC_ROW % 128
    for ref in vec_refs:
        for j in range(ref.shape[1] // 64):
            rows_ref[at:at + 1, :64] = ref[:, j * 64:(j + 1) * 64]
            at += 1
    out_ref[:, n_pix + 128:] = (pos_ref[...] + rows_ref[...].T[:64]).astype(BF16)


def pack_small(wq, wt, pt, vecs):
    args = [wq, wt, pt] + vecs
    width = wq.shape[1] + 1024
    return call(pack_kernel, (), args, grid=(1,), in_specs=[held(x.shape) for x in args],
                out_specs=pl.BlockSpec((64, width), lambda *_: (0, 0)), out_shape=shaped((64, width), BF16),
                scratch_shapes=[pltpu.VMEM((128, 128), F32), pltpu.VMEM((64, 128), F32)],
                cost_estimate=cost(1e6, 1e6))


def gather_kernel(keep_ref, patches_ref, g_ref, zo_ref, gi_ref, pad_ref):
    n_patch, _, n_pix = patches_ref.shape
    n_rows = GROUP * TOK
    pad_ref[...] = jnp.zeros_like(pad_ref)
    pad_ref[:, :TOK - 1] = keep_ref[...].astype(F32)
    image = lax.broadcasted_iota(jnp.int32, pad_ref.shape, 0)
    lane = lax.broadcasted_iota(jnp.int32, pad_ref.shape, 1)
    spread = jnp.zeros(pad_ref.shape, F32)
    for b in range(GROUP):
        spread = jnp.where(image == b, pltpu.roll(pad_ref[...], TOK * b + 1, 1), spread)
    own = (lane > TOK * image) & (lane < TOK * image + TOK)
    source = jnp.sum(jnp.where(own, spread * GROUP + image.astype(F32), 0.0), axis=0, keepdims=True)
    token = jnp.sum(jnp.where(own, spread + 1.0, 0.0), axis=0, keepdims=True)
    kept = jnp.sum(jnp.where(own, 1.0, 0.0), axis=0, keepdims=True)
    source = jnp.where(kept > 0.0, source, -1.0)
    cols = jnp.where(image == 0, source, token).T
    source, token = cols[:n_rows, 0:1].astype(jnp.int32), cols[:n_rows, 1:2].astype(jnp.int32)
    pick = (lax.broadcasted_iota(jnp.int32, (n_rows, GROUP * n_patch), 1) == source).astype(F32).astype(BF16)
    zo_ref[:, :n_pix] = dot(pick, patches_ref.reshape(GROUP * n_patch, n_pix)[...]).astype(BF16)
    wide = zo_ref.shape[1] - n_pix
    zo_ref[:, n_pix:] = (lax.broadcasted_iota(jnp.int32, (n_rows, wide), 1) == token).astype(F32).astype(BF16)
    row = lax.broadcasted_iota(jnp.int32, (n_rows, n_rows), 0)
    col = lax.broadcasted_iota(jnp.int32, (n_rows, n_rows), 1)
    move = (row == (col & (GROUP - 1)) * TOK + (col >> 3)).astype(F32).astype(BF16)
    gi_ref[...] = dot(move, g_ref.reshape(n_rows, g_ref.shape[2])[...]).astype(BF16)


def gather_rows(keep, patches_t, g_t, width):
    n_patch, n_img, n_pix = patches_t.shape
    d = g_t.shape[2]
    n_tok = n_img * TOK
    three = lambda s: pl.BlockSpec((s[0], GROUP, s[2]), lambda i: (0, i, 0))
    return call(gather_kernel, (), (keep, patches_t, g_t), grid=(n_img // GROUP,),
                in_specs=[pl.BlockSpec((GROUP, TOK - 1), lambda i: (i, 0)), three(patches_t.shape), three(g_t.shape)],
                out_specs=[rows_spec(GROUP * TOK, width), rows_spec(GROUP * TOK, d)],
                out_shape=[shaped((n_tok, width), BF16), shaped((n_tok, d), BF16)],
                scratch_shapes=[pltpu.VMEM((GROUP, 512), F32)],
                cost_estimate=cost(2 * n_tok * n_patch * n_pix * GROUP, patches_t.size * 2 + n_tok * (width + 2 * d) * 2))


def embed_kernel(zo_ref, wt_ref, hat_ref, a_ref, stat_ref, vec_ref, bq_ref, bf_ref, next_ref, now_ref):
    @pl.when(pl.program_id(0) == 0)
    def _():
        base = VEC_ROW // 128 * 128
        rows = wt_ref[:, base:base + 128].astype(F32).T
        vec_ref[...] = rows[VEC_ROW - base:VEC_ROW - base + 32]
        at = N_VEC
        for ref in (bq_ref, bf_ref):
            n = ref.shape[1] // vec_ref.shape[1]
            chunk = lambda q: vec_ref[at + q % n:at + q % n + 1, q // n * 64:(q // n + 1) * 64]
            for tile in range(ref.shape[1] // 128):
                ref[:, tile * 128:(tile + 1) * 128] = jnp.concatenate([chunk(2 * tile), chunk(2 * tile + 1)], axis=1)
            at += n

    now_ref[...] = next_ref[...]
    next_ref[...] = dot_nt(zo_ref[...], wt_ref[...]) + jnp.where(is_class(zo_ref.shape[0]), vec_ref[1:2, :], vec_ref[0:1, :])
    hat, inv = normalize(now_ref[...])
    hat_ref[...] = hat
    h0 = hat * vec_ref[2:3, :] + vec_ref[3:4, :]
    mean1 = jnp.mean(h0, axis=-1, keepdims=True)
    centered = h0 - mean1
    inv1 = lax.rsqrt(jnp.mean(centered * centered, axis=-1, keepdims=True) + LN_EPS)
    a_ref[...] = (centered * inv1 * vec_ref[4:5, :] + vec_ref[5:6, :]).astype(BF16)
    lane = lax.broadcasted_iota(jnp.int32, stat_ref.shape, 1)
    stat_ref[...] = jnp.where(lane == 0, inv, jnp.where(lane == 1, inv1, mean1))


def embed(zo, first, d_mlp):
    n_tok, width = zo.shape
    d = first.shape[0]
    n = n_tok // GROWS
    whole = lambda s: pl.BlockSpec(s, lambda i: (0, 0))
    return call(embed_kernel, (), (zo, first), grid=(n + 1,),
                in_specs=[this_block(GROWS, width, n), held_cols(d, width, first.shape[1] - width)],
                out_specs=[last_block(GROWS, d), last_block(GROWS, d), last_block(GROWS, 128), whole((32, d)), whole((1, 3 * d)), whole((1, d_mlp))],
                out_shape=[shaped((n_tok, d), F32), shaped((n_tok, d), BF16), shaped((n_tok, 128), F32),
                           shaped((32, d), F32), shaped((1, 3 * d), F32), shaped((1, d_mlp), F32)],
                scratch_shapes=[pltpu.VMEM((GROWS, d), F32), pltpu.VMEM((GROWS, d), F32)],
                cost_estimate=cost(2 * n_tok * width * d, n_tok * (width * 2 + d * 6)))


def window_mask(start):
    key = lax.broadcasted_iota(jnp.int32, (WIN, 2 * WIN), 0)
    qry = lax.broadcasted_iota(jnp.int32, (WIN, 2 * WIN), 1)
    qry = jnp.where(qry >= WIN, qry - WIN, qry)
    return jnp.where(image_of(key + start) == image_of(qry + start), 0.0, MASKED)


STARTS = (0, ROWS - WIN)
FWD_PAIRS = 8
BWD_PAIRS = 8


def split_heads(x):
    first = lax.broadcasted_iota(jnp.int32, x.shape, 1) < 64
    zero = jnp.zeros_like(x)
    return jnp.concatenate([jnp.where(first, x, zero), jnp.where(first, zero, x)], axis=0)


def join_heads(x):
    first = lax.broadcasted_iota(jnp.int32, (WIN, x.shape[1]), 1) < 64
    return jnp.where(first, x[:WIN], x[WIN:])


def join_windows(lo, hi):
    row8 = lax.broadcasted_iota(jnp.int32, (8, lo.shape[1]), 0)
    edge = jnp.where(row8 < 2 * TOK - 96, lo[96:104], hi[8:16])
    return jnp.concatenate([lo[:96], edge, hi[16:]], axis=0)


def attend_kernel(scale, a_ref, w_ref, b_ref, qkv_ref, o_ref, mask_ref):
    d = o_ref.shape[1]

    @pl.when(pl.program_id(0) == 0)
    def _():
        for i, start in enumerate(STARTS):
            mask_ref[i] = window_mask(start)

    a = a_ref[...]
    for j in range(0, 3 * d, 512):
        qkv_ref[:, j:j + 512] = (dot(a, w_ref[:, j:j + 512]) + b_ref[:, j:j + 512]).astype(BF16)

    def head_group(step, carry):
        lanes = [[pl.ds(pl.multiple_of((step * FWD_PAIRS + g) * 128 + part * d, 128), 128) for part in range(3)] for g in range(FWD_PAIRS)]
        units = [(g, i) for g in range(FWD_PAIRS) for i in range(2)]
        read = lambda part, g, i: qkv_ref[STARTS[i]:STARTS[i] + WIN, lanes[g][part]]
        s = [dot_nt(read(1, g, i), split_heads(read(0, g, i))) * scale + mask_ref[i] for g, i in units]
        e = [jnp.exp(x - jnp.max(x, axis=0, keepdims=True)) for x in s]
        p = [(x * (1.0 / jnp.sum(x, axis=0, keepdims=True))).astype(BF16) for x in e]
        o = [join_heads(dot_tn(x, read(2, g, i))) for x, (g, i) in zip(p, units)]
        for g in range(FWD_PAIRS):
            o_ref[:, lanes[g][0]] = join_windows(o[2 * g], o[2 * g + 1]).astype(BF16)
        return carry

    lax.fori_loop(0, d // (128 * FWD_PAIRS), head_group, 0)


def attend(a, w_qkv, b_qkv, scale):
    n_tok, d = a.shape
    return call(functools.partial(attend_kernel, scale), (), (a, w_qkv, b_qkv), grid=(n_tok // ROWS,),
                in_specs=[rows_spec(ROWS, d), held_cols(d, 3 * d, 0), held(b_qkv.shape)],
                out_specs=[rows_spec(ROWS, 3 * d), rows_spec(ROWS, d)],
                out_shape=[shaped((n_tok, 3 * d), BF16), shaped((n_tok, d), BF16)],
                scratch_shapes=[pltpu.VMEM((2, WIN, 2 * WIN), F32)],
                cost_estimate=cost(2 * n_tok * d * 3 * d * 1.8, n_tok * d * 10))


def attend_grad_kernel(scale, qkv_ref, dctx_ref, dqkv_ref, bsum_ref, mask_ref):
    d = dctx_ref.shape[1]

    @pl.when(pl.program_id(0) == 0)
    def _():
        for i, start in enumerate(STARTS):
            mask_ref[i] = window_mask(start)
        bsum_ref[...] = jnp.zeros_like(bsum_ref)

    def head_group(step, carry):
        lanes = [[pl.ds(pl.multiple_of((step * BWD_PAIRS + g) * 128 + part * d, 128), 128) for part in range(3)] for g in range(BWD_PAIRS)]
        units = [(g, i) for g in range(BWD_PAIRS) for i in range(2)]
        read = lambda part, g, i: qkv_ref[STARTS[i]:STARTS[i] + WIN, lanes[g][part]]
        q2 = [split_heads(read(0, g, i)) for g, i in units]
        do2 = [split_heads(dctx_ref[STARTS[i]:STARTS[i] + WIN, lanes[g][0]]) for g, i in units]
        s = [dot_nt(read(1, g, i), q) * scale + mask_ref[i] for q, (g, i) in zip(q2, units)]
        dp = [dot_nt(read(2, g, i), do) for do, (g, i) in zip(do2, units)]
        e = [jnp.exp(x - jnp.max(x, axis=0, keepdims=True)) for x in s]
        p = [x * (1.0 / jnp.sum(x, axis=0, keepdims=True)) for x in e]
        dv = [dot(x.astype(BF16), do) for x, do in zip(p, do2)]
        ds = [(x * (y - jnp.sum(x * y, axis=0, keepdims=True)) * scale).astype(BF16) for x, y in zip(p, dp)]
        dk = [dot(x, q) for x, q in zip(ds, q2)]
        dq = [join_heads(dot_tn(x, read(1, g, i))) for x, (g, i) in zip(ds, units)]
        for g in range(BWD_PAIRS):
            for part, grad in enumerate((dq, dk, dv)):
                both = join_windows(grad[2 * g], grad[2 * g + 1])
                dqkv_ref[:, lanes[g][part]] = both.astype(BF16)
                bsum_ref[:, lanes[g][part]] += jnp.sum(both, axis=0, keepdims=True)
        return carry

    lax.fori_loop(0, d // (128 * BWD_PAIRS), head_group, 0)


def attend_grad(qkv, d_ctx, scale, after):
    n_tok, d = d_ctx.shape
    return call(functools.partial(attend_grad_kernel, scale), after, (qkv, d_ctx), grid=(n_tok // ROWS,),
                in_specs=[rows_spec(ROWS, 3 * d), rows_spec(ROWS, d)],
                out_specs=[rows_spec(ROWS, 3 * d), pl.BlockSpec((1, 3 * d), lambda i: (0, 0))],
                out_shape=[shaped((n_tok, 3 * d), BF16), shaped((1, 3 * d), F32)],
                scratch_shapes=[pltpu.VMEM((2, WIN, 2 * WIN), F32)],
                cost_estimate=cost(31e9 * n_tok / 3200, n_tok * d * 14))


def mlp_up_kernel(o_ref, hat_ref, wo_ref, wf_ref, vec_ref, bf_ref, m_ref, c_ref, act_ref, pre_ref, next_ref, now_ref):
    now_ref[...] = next_ref[...]
    m = hat_ref[...] * vec_ref[2:3, :] + vec_ref[3:4, :] + dot(o_ref[...], wo_ref[...]) + vec_ref[6:7, :]
    m_ref[...] = m
    hat2, _ = normalize(m)
    next_c = (hat2 * vec_ref[7:8, :] + vec_ref[8:9, :]).astype(BF16)
    c_ref[...] = next_c
    c = now_ref[...]
    step = 512
    for at in range(0, wf_ref.shape[1], step):
        u = dot(c, wf_ref[:, at:at + step]) + bf_ref[:, at:at + step]
        pre_ref[:, at:at + step] = u
        act_ref[:, at:at + step] = (u * (0.5 + 0.5 * lax.erf(u * INV_SQRT2))).astype(BF16)
    next_ref[...] = next_c


def mlp_up(o, hat, w_fo, vecs, b_fc):
    n_tok, d = o.shape
    f = w_fo.shape[1] - d
    n = n_tok // ROWS
    return call(mlp_up_kernel, (), (o, hat, w_fo, w_fo, vecs, b_fc), grid=(n + 1,),
                in_specs=[this_block(ROWS, d, n), this_block(ROWS, d, n), held_cols(d, d, f), held_cols(d, f, 0), held(vecs.shape), held(b_fc.shape)],
                out_specs=[this_block(ROWS, d, n), this_block(ROWS, d, n), last_block(ROWS, f), last_block(ROWS, f)],
                out_shape=[shaped((n_tok, d), F32), shaped((n_tok, d), BF16), shaped((n_tok, f), BF16), shaped((n_tok, f), F32)],
                scratch_shapes=[pltpu.VMEM((ROWS, d), BF16), pltpu.VMEM((ROWS, d), BF16)],
                cost_estimate=cost(2 * n_tok * d * (d + f) * 1.5, n_tok * (d * 12 + f * 6), 2 * n_tok * f))


def mlp_down_kernel(act_ref, m_ref, w_ref, vec_ref, h1_ref):
    n_rows = GROUP * TOK
    h1 = (m_ref[...] + dot(act_ref[...], w_ref[...]) + vec_ref[9:10, :]).astype(BF16)
    row = lax.broadcasted_iota(jnp.int32, (n_rows, n_rows), 0)
    col = lax.broadcasted_iota(jnp.int32, (n_rows, n_rows), 1)
    move = (col == (row & (GROUP - 1)) * TOK + (row >> 3)).astype(F32).astype(BF16)
    h1_ref.reshape(n_rows, h1_ref.shape[2])[...] = dot(move, h1).astype(BF16)


def mlp_down(act, m, w_proj, vecs, after):
    n_tok, f = act.shape
    d = m.shape[1]
    return call(mlp_down_kernel, after, (act, m, w_proj, vecs), grid=(n_tok // GROWS,),
                in_specs=[rows_spec(GROWS, f), rows_spec(GROWS, d), held(w_proj.shape), held(vecs.shape)],
                out_specs=pl.BlockSpec((TOK, GROUP, d), lambda i: (0, i, 0)),
                out_shape=shaped((TOK, n_tok // TOK, d), BF16),
                cost_estimate=cost(2.2 * n_tok * d * f, n_tok * (d * 6 + f * 2)))


def mlp_grad_kernel(g_ref, pre_ref, m_ref, wp_ref, wf_ref, wo_ref, vec_ref,
                    dpre_ref, dmid_ref, dmidb_ref, dctx_ref, vsum_ref, bfc_ref):
    @pl.when(pl.program_id(0) == 0)
    def _():
        vsum_ref[...] = jnp.zeros_like(vsum_ref)
        bfc_ref[...] = jnp.zeros_like(bfc_ref)

    g = g_ref[...]
    step = 1024
    d_c = None
    acts, pres = dict(), dict()
    n_steps = wp_ref.shape[0] // step
    for j in range(n_steps + 2):
        if j < n_steps:
            acts[j] = dot_nt(g, wp_ref[j * step:(j + 1) * step, :])
        if 0 <= j - 1 < n_steps:
            cols = slice((j - 1) * step, j * step)
            u = pre_ref[:, cols]
            w = u * INV_SQRT2
            d_pre = acts.pop(j - 1) * (0.5 + 0.5 * lax.erf(w) + u * (jnp.exp2((w * w) * (-LOG2E)) * INV_SQRT_2PI))
            bfc_ref[:, cols] += jnp.sum(d_pre, axis=0, keepdims=True)
            pres[j - 1] = d_pre.astype(BF16)
            dpre_ref[:, cols] = pres[j - 1]
        if 0 <= j - 2:
            part = dot_nt(pres.pop(j - 2), wf_ref[:, (j - 2) * step:(j - 1) * step])
            d_c = part if d_c is None else d_c + part
    hat2, inv2 = normalize(m_ref[...])
    g_f = g.astype(F32)
    d_mid = norm_grad(d_c, hat2, inv2, vec_ref[7:8, :]) + g_f
    dmid_ref[...] = d_mid
    d_mid_b = d_mid.astype(BF16)
    dmidb_ref[...] = d_mid_b
    dctx_ref[...] = dot_nt(d_mid_b, wo_ref[...]).astype(BF16)
    vsum_ref[0:1, :] += jnp.sum(d_mid, axis=0, keepdims=True)
    vsum_ref[1:2, :] += jnp.sum(d_c * hat2, axis=0, keepdims=True)
    vsum_ref[2:3, :] += jnp.sum(d_c, axis=0, keepdims=True)
    vsum_ref[3:4, :] += jnp.sum(g_f, axis=0, keepdims=True)


def mlp_grad(g, pre, m, w_proj, w_fo, vecs, after):
    n_tok, d = g.shape
    f = pre.shape[1]
    whole = lambda s: pl.BlockSpec(s, lambda i: (0, 0))
    return call(mlp_grad_kernel, after, (g, pre, m, w_proj, w_fo, w_fo, vecs), grid=(n_tok // GROWS,),
                in_specs=[rows_spec(GROWS, d), rows_spec(GROWS, f), rows_spec(GROWS, d),
                          held(w_proj.shape), held_cols(d, f, 0), held_cols(d, d, f), held(vecs.shape)],
                out_specs=[rows_spec(GROWS, f), rows_spec(GROWS, d), rows_spec(GROWS, d), rows_spec(GROWS, d), whole((8, d)), whole((1, f))],
                out_shape=[shaped((n_tok, f), BF16), shaped((n_tok, d), F32), shaped((n_tok, d), BF16), shaped((n_tok, d), BF16),
                           shaped((8, d), F32), shaped((1, f), F32)],
                cost_estimate=cost(2 * n_tok * d * (2 * f + d), n_tok * (d * 14 + f * 6)))


def embed_grad_kernel(dqkv_ref, dmid_ref, hat_ref, stat_ref, w_ref, vec_ref, demb_ref, vsum_ref, next_ref, now_ref, dx_ref):
    step = pl.program_id(0)

    @pl.when(step == 0)
    def _():
        vsum_ref[...] = jnp.zeros_like(vsum_ref)

    now_ref[...] = next_ref[...]
    n_rows, d = now_ref.shape
    totals = None
    cuts = (0, 104, 208, 304, n_rows)
    for j, (lo, hi) in enumerate(zip(cuts, cuts[1:])):
        cols = slice(j * d // 4, (j + 1) * d // 4)
        next_ref[:, cols] = dot_nt(dqkv_ref[...], w_ref[cols, :])
        d_a, hat_p = now_ref[lo:hi, :], hat_ref[lo:hi, :]
        inv_p, inv1, mean1 = (stat_ref[lo:hi, k:k + 1] for k in range(3))
        hat1 = (hat_p * vec_ref[2:3, :] + vec_ref[3:4, :] - mean1) * inv1
        d_zero = norm_grad(d_a, hat1, inv1, vec_ref[4:5, :]) + dmid_ref[lo:hi, :]
        d_x = norm_grad(d_zero, hat_p, inv_p, vec_ref[2:3, :])
        demb_ref[lo:hi, :] = d_x.astype(BF16)
        dx_ref[lo:hi, :] = d_x
        parts = [jnp.sum(part, axis=0, keepdims=True) for part in (d_x, d_zero * hat_p, d_zero, d_a * hat1, d_a)]
        totals = parts if totals is None else [x + y for x, y in zip(totals, parts)]
    d_cls = sum(dx_ref[TOK * j:TOK * j + 1, :] for j in range(n_rows // TOK))
    for row, part in enumerate([totals[0] - d_cls, d_cls] + totals[1:]):
        vsum_ref[row:row + 1, :] += jnp.where(step > 0, part, 0.0)


def embed_grad(dqkv, d_mid, hat, stats, first, vecs, after):
    n_tok, d = d_mid.shape
    n = n_tok // GROWS
    return call(embed_grad_kernel, after, (dqkv, d_mid, hat, stats, first, vecs), grid=(n + 1,),
                in_specs=[this_block(GROWS, 3 * d, n), last_block(GROWS, d), last_block(GROWS, d), last_block(GROWS, 128), held_cols(d, 3 * d, 0), held(vecs.shape)],
                out_specs=[last_block(GROWS, d), pl.BlockSpec((8, d), lambda i: (0, 0))],
                out_shape=[shaped((n_tok, d), BF16), shaped((8, d), F32)],
                scratch_shapes=[pltpu.VMEM((GROWS, d), F32)] * 3,
                cost_estimate=cost(2.5 * n_tok * d * 3 * d, n_tok * d * 16))


def tail_kernel(se_ref, sm_ref, sq_ref, sf_ref, out_ref, rows_ref):
    d = se_ref.shape[1]
    rows_ref[...] = jnp.zeros_like(rows_ref)
    at = VEC_ROW % 128
    rows_ref[at:at + 6, :] = se_ref[:6, :]
    rows_ref[at + 6:at + N_VEC, :] = sm_ref[:4, :]
    at += N_VEC
    for ref in (sq_ref, sf_ref):
        n = ref.shape[1] // d
        for r in range(n):
            for j in range(d // 128):
                chunk = lambda q: ref[:, (n * q + r) * 64:(n * q + r + 1) * 64]
                rows_ref[at + r:at + r + 1, j * 128:(j + 1) * 128] = jnp.concatenate([chunk(2 * j), chunk(2 * j + 1)], axis=1)
        at += n
    for j in range(d // 128):
        cols = rows_ref[:, j * 128:(j + 1) * 128].T
        out_ref[0, j * 64:(j + 1) * 64] = cols[:64]
        out_ref[1, j * 64:(j + 1) * 64] = cols[64:]


def vector_tail(sums_e, sums_m, sum_qkv, sum_fc):
    args = (sums_e, sums_m, sum_qkv, sum_fc)
    d = sums_e.shape[1]
    return call(tail_kernel, (), args, grid=(1,), in_specs=[held(x.shape) for x in args],
                out_specs=pl.BlockSpec((2, d // 2, 128), lambda i: (0, 0, 0)), out_shape=shaped((2, d // 2, 128), F32),
                scratch_shapes=[pltpu.VMEM((128, d), F32)], cost_estimate=cost(1e6, 1e6))


LINKS = ('core', 'x', 'y', 'z')
GRID = ('z', 'y', 'x')
ORDERS = (('x', 'y', 'z'), ('y', 'z', 'x'), ('z', 'x', 'y'))


def bit(me, link):
    return (me >> LINKS.index(link)) & 1


def transposed_halves(a_ref, at_ref):
    for j in range(a_ref.shape[1] // 128):
        t = a_ref[:, j * 128:(j + 1) * 128].T
        at_ref[0, j * 64:(j + 1) * 64, :] = t[:64]
        at_ref[1, j * 64:(j + 1) * 64, :] = t[64:]


def cols_sent_kernel(has_tail, me_ref, a_ref, b_ref, *refs):
    tail_ref = refs[0] if has_tail else None
    out_ref, at_ref = refs[-2:]

    @pl.when(pl.program_id(0) == 0)
    def _():
        transposed_halves(a_ref, at_ref)

    other = 1 - bit(me_ref[0], 'core')
    out_ref[...] = dot(at_ref[other], b_ref[...])
    if has_tail:
        @pl.when(pl.program_id(0) == pl.num_programs(0) - 1)
        def _():
            out_ref[:, -128:] += tail_ref[other]


def cols_sent(me, a, b, tile, after, tail=None):
    k, m = a.shape
    n = b.shape[1]
    args = [a, b] + ([] if tail is None else [tail])
    in_specs = [held(a.shape), pl.BlockSpec((k, tile), lambda j, s: (0, j))] + ([] if tail is None else [held(tail.shape)])
    return call(functools.partial(cols_sent_kernel, tail is not None), after, args, prefetch=me, grid=(n // tile,), in_specs=in_specs,
                out_specs=pl.BlockSpec((m // 2, tile), lambda j, s: (0, j)), out_shape=shaped((m // 2, n), F32),
                scratch_shapes=[pltpu.VMEM((2, m // 2, k), BF16)],
                cost_estimate=cost(k * m * n, k * (m + n) * 2 + m * n * 2))


def half_copies(me, order, buf, send, keep, columns, sem):
    at = GRID.index(order[0])
    mine = bit(me, order[0])
    half = lambda index: buf.at[(slice(None),) * at + (index,)]
    return [pltpu.make_async_copy(half(1 - mine), send.at[:, :, :, columns], sem.at[0]),
            pltpu.make_async_copy(half(mine), keep.at[:, :, :, columns], sem.at[1])]


def cols_kept_kernel(orders, edges, tile, has_tail, me_ref, a_ref, b_ref, base_ref, *refs):
    tail_ref = refs[0] if has_tail else None
    outs, (at_ref, buf_ref, sems) = refs[has_tail:-3], refs[-3:]
    step, last = pl.program_id(0), pl.num_programs(0) - 1
    slot = step % 2

    @pl.when(step == 0)
    def _():
        transposed_halves(a_ref, at_ref)

    def landed(at):
        for copy in half_copies(me_ref[0], orders[0], buf_ref.at[at], outs[0], outs[1], pl.ds(0, tile), sems.at[at]):
            copy.wait()

    @pl.when(step >= 2)
    def _():
        landed(slot)

    mine = bit(me_ref[0], 'core')
    total = dot(at_ref[mine], b_ref[...]) + base_ref[...]
    buf_ref[slot] = total.reshape(2, 2, 2, -1, tile)
    if has_tail:
        @pl.when(step == last)
        def _():
            buf_ref[slot, :, :, :, :, tile - 128:] += tail_ref[mine].reshape(2, 2, 2, -1, 128)
    for c, order in enumerate(orders):
        lo, hi = edges[c] // tile, edges[c + 1] // tile

        @pl.when((step >= lo) & (step < hi))
        def _():
            columns = pl.ds(pl.multiple_of((step - lo) * tile, tile), tile)
            for copy in half_copies(me_ref[0], order, buf_ref.at[slot], outs[2 * c], outs[2 * c + 1], columns, sems.at[slot]):
                copy.start()

    @pl.when(step == last)
    def _():
        landed(1 - slot)
        landed(slot)


def cols_kept(me, a, b, base, tile, orders, edges, after, tail=None):
    k, m = a.shape
    n = b.shape[1]
    r = m // 16
    args = [a, b, base] + ([] if tail is None else [tail])
    in_specs = [held(a.shape), pl.BlockSpec((k, tile), lambda j, s: (0, j)), pl.BlockSpec((m // 2, tile), lambda j, s: (0, j))]
    in_specs += [] if tail is None else [held(tail.shape)]
    shapes = [shaped((2, 2, r, hi - lo), F32) for lo, hi in zip(edges, edges[1:]) for _ in range(2)]
    return call(functools.partial(cols_kept_kernel, orders, edges, tile, tail is not None), after, args, prefetch=me, grid=(n // tile,),
                in_specs=in_specs, out_specs=[ANY] * len(shapes), out_shape=shapes,
                scratch_shapes=[pltpu.VMEM((2, m // 2, k), BF16), pltpu.VMEM((2, 2, 2, 2, r, tile), F32), pltpu.SemaphoreType.DMA((2, 2))],
                cost_estimate=cost(k * m * n, k * (m + n) * 2 + m * n * 4))


def rows_sent_kernel(me_ref, a_ref, b_ref, out_ref):
    out_ref[...] = dot_tn(a_ref[...], b_ref[...])


def rows_sent(me, a, b, after):
    k, m = a.shape
    n = b.shape[1]
    r = m // 16
    return call(rows_sent_kernel, after, (a, b), prefetch=me, grid=(8,),
                in_specs=[pl.BlockSpec((k, r), lambda j, s: (0, 2 * j + 1 - bit(s[0], 'core'))), held(b.shape)],
                out_specs=pl.BlockSpec((r, n), lambda j, s: (j, 0)), out_shape=shaped((m // 2, n), F32),
                cost_estimate=cost(k * m * n, k * (m + n) * 2 + m * n * 2))


def rows_kept_kernel(orders, edges, me_ref, a_ref, b_ref, base_ref, *refs):
    outs, (buf_ref, sems) = refs[:-2], refs[-2:]
    step, last = pl.program_id(0), pl.num_programs(0) - 1
    slot = step % 2

    def copies(c, at, chip, wanted):
        rest = [(chip >> (LINKS.index(link) - 1)) & 1 for link in GRID if link != orders[c][0]]
        source = buf_ref.at[at, :, pl.ds(edges[c], edges[c + 1] - edges[c])]
        return pltpu.make_async_copy(source, outs[2 * c + wanted].at[rest[0], rest[1]], sems.at[at, c])

    def landed(at):
        for c in range(len(orders)):
            copies(c, at, 0, 0).wait()

    @pl.when(step >= 2)
    def _():
        landed(slot)

    buf_ref[slot] = dot_tn(a_ref[...], b_ref[...]) + base_ref[...]
    for c, order in enumerate(orders):
        same = ((step >> (LINKS.index(order[0]) - 1)) & 1) == bit(me_ref[0], order[0])
        for wanted in range(2):
            @pl.when(same if wanted else jnp.logical_not(same))
            def _():
                copies(c, slot, step, wanted).start()

    @pl.when(step == last)
    def _():
        landed(1 - slot)
        landed(slot)


def rows_kept(me, a, b, base, orders, edges, after):
    k, m = a.shape
    n = b.shape[1]
    r = m // 16
    shapes = [shaped((2, 2, r, hi - lo), F32) for lo, hi in zip(edges, edges[1:]) for _ in range(2)]
    return call(functools.partial(rows_kept_kernel, orders, edges), after, (a, b, base), prefetch=me, grid=(8,),
                in_specs=[pl.BlockSpec((k, r), lambda j, s: (0, 2 * j + bit(s[0], 'core'))), held(b.shape), pl.BlockSpec((r, n), lambda j, s: (j, 0))],
                out_specs=[ANY] * len(shapes), out_shape=shapes,
                scratch_shapes=[pltpu.VMEM((2, r, n), F32), pltpu.SemaphoreType.DMA((2, len(orders)))],
                cost_estimate=cost(k * m * n, k * (m + n) * 2 + m * n * 4))


def add_pairs_kernel(me_ref, *refs):
    n = len(refs) // 3
    for i in range(n):
        refs[2 * n + i][...] = refs[2 * i][...] + refs[2 * i + 1][...]


def next_halves(me, items, level, after):
    args, in_specs, shapes, out_specs = [], [], [], []
    for order, kept, received in items:
        links = [link for link in GRID if link not in order[:level]]
        at = links.index(order[level])
        r, n = kept.shape[-2:]
        for keep in range(2):
            def index(i, s, keep=keep, at=at, n_links=len(links), link=order[level]):
                mine = bit(s[0], link)
                lead = [i] * n_links
                lead[at] = mine if keep else 1 - mine
                return tuple(lead) + (0, 0)

            args += [kept, received]
            in_specs += [pl.BlockSpec((None,) * len(links) + (r, n), index)] * 2
            if len(links) == 2:
                shapes.append(shaped((2, r, n), F32))
                out_specs.append(pl.BlockSpec((None, r, n), lambda i, s: (i, 0, 0)))
            else:
                shapes.append(shaped((r, n), F32))
                out_specs.append(pl.BlockSpec((r, n), lambda i, s: (0, 0)))
    total = sum(kept.size for _, kept, _ in items)
    outs = call(add_pairs_kernel, after, args, prefetch=me, grid=(2 if level == 1 else 1,), in_specs=in_specs, out_specs=out_specs,
                out_shape=shapes, cost_estimate=cost(total * 40, total * 12))
    return list(zip(outs[::2], outs[1::2]))


def join_kernel(groups, *refs):
    n = sum(groups)
    at = 0
    for out_ref, count in zip(refs[2 * n:], groups):
        lo = 0
        for _ in range(count):
            kept, received = refs[2 * at], refs[2 * at + 1]
            out_ref[:, lo:lo + kept.shape[1]] = kept[...] + received[...]
            lo += kept.shape[1]
            at += 1


def join(groups, after):
    args = [x for group in groups for pair in group for x in pair]
    r = args[0].shape[0]
    shapes = [shaped((r, sum(pair[0].shape[1] for pair in group)), F32) for group in groups]
    total = sum(x.size for x in args)
    return call(functools.partial(join_kernel, [len(group) for group in groups]), after, args, grid=(1,),
                in_specs=[held(x.shape) for x in args], out_specs=[pl.BlockSpec(s.shape, lambda i: (0, 0)) for s in shapes],
                out_shape=shapes, cost_estimate=cost(total * 20, total * 6))


def finish_kernel(n_pairs, n_pix, n_pos, *refs):
    outs, full_ref = refs[2 * n_pairs:-1], refs[-1]
    lo = 0
    for i in range(n_pairs):
        n = refs[2 * i].shape[1]
        full_ref[:, lo:lo + n] = refs[2 * i][...] + refs[2 * i + 1][...]
        lo += n
    outs[0][...] = full_ref[:, :n_pix]
    pos_ref = outs[1]
    pos_ref[:, :128] = full_ref[:, n_pix:n_pix + 128]
    pos_ref[:, 128:] = full_ref[:, n_pix + 128:n_pix + n_pos]
    pos_ref[:, 0:1] = full_ref[:, VEC_ROW + 1:VEC_ROW + 2]
    base = VEC_ROW // 128 * 128
    rows = full_ref[:, base:base + 128].T
    at = VEC_ROW - base
    for ref in outs[2:]:
        n = ref.shape[1] // 64
        if n == 1:
            ref[...] = rows[at:at + 1]
        else:
            ref[...] = jnp.concatenate([rows[at + j:at + j + 1] for j in range(n)], axis=1)
        at += n


def finish(pairs, n_pix, n_pos, widths, after):
    args = [x for pair in pairs for x in pair]
    shapes = [shaped((64, n_pix), F32), shaped((64, n_pos), F32)] + [shaped((1, w), F32) for w in widths]
    return call(functools.partial(finish_kernel, len(pairs), n_pix, n_pos), after, args, grid=(1,), in_specs=[held(x.shape) for x in args],
                out_specs=[pl.BlockSpec(s.shape, lambda i: (0, 0)) for s in shapes], out_shape=shapes,
                scratch_shapes=[pltpu.VMEM((64, 1024), F32)], cost_estimate=cost(1e6, 1e6))


MESH_AXIS = 'fsdp'
PARAM_NAMES = ('w_patch', 'b_patch', 'pos_table', 'cls_tok', 'lnp_g', 'lnp_b', 'ln1_g', 'ln1_b', 'w_qkv', 'b_qkv', 'w_out', 'b_out', 'ln2_g', 'ln2_b', 'w_fc', 'b_fc', 'w_proj', 'b_proj')
PACKED = tuple(PARAM_NAMES[i] for i in (1, 3, 4, 5, 6, 7, 11, 12, 13, 17, 9, 15))
LAST_SPLIT = PARAM_NAMES[0:3:2]


def solution(mesh):
    n_dev = mesh.shape[MESH_AXIS]

    def across(value, link):
        return lax.ppermute(value, MESH_AXIS, [(i, i ^ (1 << LINKS.index(link))) for i in range(n_dev)])

    def compute(patches, keep, *rest):
        shard = dict(zip(PARAM_NAMES, rest[:-1]))
        _, _, d = rest[-1].shape
        d_mlp = shard['w_fc'].shape[1]
        n_pix, n_pos = shard['w_patch'].shape[0], shard['pos_table'].shape[0]
        scale = shard['w_qkv'].shape[3] ** -0.5
        me = lax.axis_index(MESH_AXIS).reshape(1)

        def whole(value):
            return lax.all_gather(value, MESH_AXIS, tiled=True)

        w_qkv = shard['w_qkv'].astype(BF16).reshape(-1, 3 * d)
        first = whole(pack_small(w_qkv, shard['w_patch'].T, shard['pos_table'].T, [shard[name][None] for name in PACKED]))
        w_fo = whole(jnp.concatenate([shard['w_fc'].astype(BF16), shard['w_out'].astype(BF16)], axis=1))
        w_proj = whole(shard['w_proj'].astype(BF16))

        zo, g = gather_rows(keep, patches.transpose(1, 0, 2), rest[-1].transpose(1, 0, 2), d)
        hat, a, stats, vecs, b_qkv, b_fc = embed(zo, first, d_mlp)
        qkv, ctx = attend(a, first, b_qkv, scale)
        m, c, act, pre = mlp_up(ctx, hat, w_fo, vecs, b_fc)

        def cut(outs, orders):
            return [(order, outs[2 * i + 1], across(outs[2 * i], order[0])) for i, order in enumerate(orders)]

        def halve(items, level, after):
            halves = next_halves(me, items, level, after)
            return [(order, kept, across(sent, order[level])) for (order, _, _), (sent, kept) in zip(items, halves)]

        def ends(items):
            return [(kept, received) for _, kept, received in items]

        one, two = ORDERS[:1], ORDERS[1:]
        proj_sent = rows_sent(me, act, g, ())
        h1 = mlp_down(act, m, w_proj, vecs, (proj_sent,))
        outs = rows_kept(me, act, g, across(proj_sent, 'core'), one, (0, d), (h1,))
        proj = cut(outs, one)
        d_pre, d_mid, d_mid_b, d_ctx, sums_m, sum_fc = mlp_grad(g, pre, m, w_proj, w_fo, vecs, (outs[1],))
        fc_sent = cols_sent(me, c, d_pre, 512, ())
        proj = halve(proj, 1, (fc_sent,))
        out_sent = cols_sent(me, ctx, d_mid_b, 256, (proj[0][1],))
        outs = cols_kept(me, c, d_pre, across(fc_sent, 'core'), 512, two, (0, 2048, d_mlp), (out_sent,))
        fc = cut(outs, two)
        proj = halve(proj, 2, (outs[1],))
        outs = cols_kept(me, ctx, d_mid_b, across(out_sent, 'core'), 512, ORDERS[2:], (0, d), (proj[0][1],))
        out = cut(outs, ORDERS[2:])
        d_qkv, sum_qkv = attend_grad(qkv, d_ctx, scale, (outs[1],))
        g_proj, = join([ends(proj)], (sum_qkv,))
        qkv_sent = cols_sent(me, a, d_qkv, 512, (g_proj,))
        fc = halve(fc, 1, (qkv_sent,))
        outs = cols_kept(me, a, d_qkv, across(qkv_sent, 'core'), 512, ORDERS, (0, 1024, 2048, 3 * d), (fc[0][1],))
        qkv = cut(outs, ORDERS) + out
        d_emb, sums_e = embed_grad(d_qkv, d_mid, hat, stats, first, vecs, (outs[1],))
        fc = halve(fc, 2, (sums_e,))
        tail = vector_tail(sums_e, sums_m, sum_qkv, sum_fc)
        small_sent = cols_sent(me, d_emb, zo, 512, (fc[0][1],), tail)
        qkv = halve(qkv, 1, (small_sent,))
        outs = cols_kept(me, d_emb, zo, across(small_sent, 'core'), 512, ORDERS[:2], (0, 512, d), (qkv[0][1],), tail)
        small = cut(outs, ORDERS[:2])
        g_fc, = join([ends(fc)], (outs[1],))
        qkv = halve(qkv, 2, (g_fc,))
        small = halve(small, 1, (qkv[0][1],))
        g_qkv, g_out = join([ends(qkv)[:3], ends(qkv)[3:]], (small[0][1],))
        small = halve(small, 2, (g_out,))
        done = finish(ends(small), n_pix, n_pos, [shard[name].shape[0] for name in PACKED], (g_out,))

        grads = dict(w_patch=done[0].T, pos_table=done[1].T, w_qkv=g_qkv.reshape(shard['w_qkv'].shape), w_out=g_out, w_fc=g_fc, w_proj=g_proj.reshape(shard['w_proj'].shape))
        grads.update({name: value.reshape(-1) for name, value in zip(PACKED, done[2:])})
        return (h1.transpose(1, 0, 2),) + tuple(grads[name] for name in PARAM_NAMES)

    batch_spec = P(MESH_AXIS)
    param_specs = tuple(P(None, MESH_AXIS) if name in LAST_SPLIT else P(MESH_AXIS) for name in PARAM_NAMES)
    return jax.shard_map(compute, mesh=mesh, in_specs=(batch_spec, batch_spec) + param_specs + (batch_spec,), out_specs=(batch_spec,) + param_specs, check_vma=False)
```

```python
import functools

import jax
import jax.numpy as jnp
from jax import lax
from jax.experimental import pallas as pl
from jax.experimental.pallas import tpu as pltpu
from jax.sharding import PartitionSpec as P


F32, BF16, I32 = jnp.float32, jnp.bfloat16, jnp.int32
LN_EPS = 1e-5
INV_SQRT2 = 0.7071067811865476
INV_SQRT_2PI = 0.3989422804014327
LOG2E = 1.4426950408889634
MASKED = -1e30
SUBLANES, LANES, HEAD = 8, 128, 64
TOK, FEW, MANY = 50, 4, 8
ROWS, GROWS = FEW * TOK, MANY * TOK
WIN = 112
STARTS = (0, ROWS - WIN)
EDGE = 96
PACK, VEC_ROW = 1024, 976
VEC_AT = VEC_ROW % LANES
N_VEC, VEC_ROWS = 10, 32
B_PATCH, CLS, LNP_G, LNP_B, LN1_G, LN1_B, B_OUT, LN2_G, LN2_B, B_PROJ = range(N_VEC)
STEP = 512
ALL_VMEM = 67043328
ANY = pl.BlockSpec(memory_space=pl.ANY)


def product(dims, left, right):
    return lax.dot_general(left, right, ((dims[:1], dims[1:]), ((), ())), preferred_element_type=F32)


dot = functools.partial(product, (1, 0))
dot_nt = functools.partial(product, (1, 1))
dot_tn = functools.partial(product, (0, 0))


def col_sum(x):
    return jnp.sum(x, axis=0, keepdims=True)


def col_max(x):
    return jnp.max(x, axis=0, keepdims=True)


def row_mean(x):
    return jnp.mean(x, axis=1, keepdims=True)


def row(ref, at):
    return ref[at:at + 1, :]


def iota(shape, axis):
    return lax.broadcasted_iota(I32, shape, axis)


def one_hot(test):
    return test.astype(F32).astype(BF16)


def origin(shape, *_):
    return (0,) * len(shape)


def held(shape):
    return pl.BlockSpec(shape, functools.partial(origin, shape), pipeline_mode=pl.Buffered(1))


def held_cols(n_rows, n_cols, at):
    return pl.BlockSpec((n_rows, n_cols), lambda *_: (0, at // n_cols), pipeline_mode=pl.Buffered(1))


def whole_out(shape):
    return pl.BlockSpec(shape, functools.partial(origin, shape))


def rows_spec(n_rows, width):
    return pl.BlockSpec((n_rows, width), lambda i, *_: (i, 0))


def this_block(n_rows, width, n):
    return pl.BlockSpec((n_rows, width), lambda i: (jnp.minimum(i, n - 1), 0))


def last_block(n_rows, width):
    return pl.BlockSpec((n_rows, width), lambda i: (jnp.maximum(i - 1, 0), 0))


def shaped(shape, dtype=F32):
    return jax.ShapeDtypeStruct(shape, dtype)


def call(kernel, after, args, *, prefetch=(), grid=(1,), in_specs, out_specs, out_shape, scratch_shapes=(), flops, n_bytes=0, partners=None):
    n_in, n_after = len(prefetch) + len(args), len(after)

    def body(*refs):
        return kernel(*refs[:n_in], *refs[n_in + n_after:])

    return pl.pallas_call(
        body,
        grid_spec=pltpu.PrefetchScalarGridSpec(
            num_scalar_prefetch=len(prefetch), grid=grid, in_specs=list(in_specs) + [ANY] * n_after,
            out_specs=out_specs, scratch_shapes=list(scratch_shapes)),
        out_shape=out_shape,
        compiler_params=pltpu.CompilerParams(
            dimension_semantics=(pltpu.ARBITRARY,) * len(grid), vmem_limit_bytes=ALL_VMEM,
            collective_id=partners, has_side_effects=partners is not None),
        cost_estimate=pl.CostEstimate(flops=int(flops), bytes_accessed=int(n_bytes), transcendentals=0),
    )(*prefetch, *args, *after)


def first_step():
    return pl.when(pl.program_id(0) == 0)


def clear(*refs):
    for ref in refs:
        ref[:] = jnp.zeros_like(ref)


def normalize(x):
    centered = x - row_mean(x)
    inv = lax.rsqrt(row_mean(centered * centered) + LN_EPS)
    return centered * inv, inv


def norm_grad(d_out, x_hat, inv, gain):
    d_hat = d_out * gain
    return inv * (d_hat - row_mean(d_hat) - x_hat * row_mean(d_hat * x_hat))


def image_of(at, n_img=FEW):
    return sum((at >= j * TOK).astype(I32) for j in range(1, n_img))


def is_class(n_rows):
    at = iota((n_rows, 1), 0)
    return at == TOK * image_of(at, n_rows // TOK)


def pack_kernel(wq_ref, wt_ref, pt_ref, *refs):
    *vec_refs, whole_ref, rows_ref, pos_ref = refs
    n_pix, n_pos, n_qkv = wt_ref.shape[1], pt_ref.shape[1], wq_ref.shape[1]
    whole_ref[:, :n_qkv] = wq_ref[:]
    out_ref = whole_ref.at[:, n_qkv:]
    out_ref[:, :n_pix] = wt_ref[:].astype(BF16)
    out_ref[:, n_pix:n_pix + LANES] = pt_ref[:, :LANES].astype(BF16)
    clear(rows_ref, pos_ref)
    pos_ref[:, :n_pos - LANES] = pt_ref[:, LANES:]
    at = VEC_AT
    for ref in vec_refs:
        for lo in range(0, ref.shape[1], HEAD):
            rows_ref[at:at + 1, :HEAD] = ref[:, lo:lo + HEAD]
            at += 1
    out_ref[:, n_pix + LANES:] = (pos_ref[:] + rows_ref[:].T[:HEAD]).astype(BF16)


def pack_small(wq, wt, pt, vecs):
    args = [wq, wt, pt] + vecs
    shape = (HEAD, wq.shape[1] + PACK)
    return call(pack_kernel, (), args, in_specs=[held(x.shape) for x in args], out_specs=whole_out(shape), out_shape=shaped(shape, BF16),
                scratch_shapes=[pltpu.VMEM((LANES, LANES), F32), pltpu.VMEM((HEAD, LANES), F32)], flops=PACK)


def pick_kernel(keep_ref, patches_ref, g_ref, zo_ref, gi_ref, pad_ref):
    n_patch, _, n_pix = patches_ref.shape
    clear(pad_ref)
    pad_ref[:, :TOK - 1] = keep_ref[:].astype(F32)
    image, lane = iota(pad_ref.shape, 0), iota(pad_ref.shape, 1)
    spread = pad_ref[:]
    for b in range(MANY):
        spread = jnp.where(image == b, pltpu.roll(pad_ref[:], TOK * b + 1, 1), spread)
    own = (lane > TOK * image) & (lane < TOK * image + TOK)
    token = col_sum(jnp.where(own, spread + 1.0, 0.0))
    source = col_sum(jnp.where(own, spread * MANY + image.astype(F32), 0.0))
    source = jnp.where(token > 0.0, source, -1.0)
    cols = jnp.where(image == 0, source, token).T[:GROWS].astype(I32)
    source, token = cols[:, :1], cols[:, 1:2]
    pick = one_hot(iota((GROWS, MANY * n_patch), 1) == source)
    zo_ref[:, :n_pix] = dot(pick, patches_ref.reshape(MANY * n_patch, n_pix)[:]).astype(BF16)
    zo_ref[:, n_pix:] = one_hot(iota((GROWS, PACK - n_pix), 1) == token)
    to, source = iota((GROWS, GROWS), 0), iota((GROWS, GROWS), 1)
    move = one_hot(to == lax.rem(source, MANY) * TOK + lax.div(source, MANY))
    gi_ref[:] = dot(move, g_ref.reshape(GROWS, g_ref.shape[2])[:]).astype(BF16)


def pick_rows(keep, patches_t, g_t):
    _, n_img, _ = patches_t.shape
    d = g_t.shape[2]
    n_tok = n_img * TOK
    by_image = lambda x: pl.BlockSpec((x.shape[0], MANY, x.shape[2]), lambda i: (0, i, 0))
    return call(pick_kernel, (), (keep, patches_t, g_t), grid=(n_img // MANY,),
                in_specs=[rows_spec(MANY, TOK - 1), by_image(patches_t), by_image(g_t)],
                out_specs=[rows_spec(GROWS, PACK), rows_spec(GROWS, d)], out_shape=[shaped((n_tok, PACK), BF16), shaped((n_tok, d), BF16)],
                scratch_shapes=[pltpu.VMEM((MANY, STEP), F32)], flops=STEP * patches_t.size)


def embed_kernel(zo_ref, wt_ref, hat_ref, a_ref, stat_ref, vec_ref, bq_ref, bf_ref, next_ref, now_ref):
    @first_step()
    def _():
        base = VEC_ROW - VEC_AT
        vec_ref[:] = wt_ref[:, base:base + LANES].astype(F32).T[VEC_AT:VEC_AT + VEC_ROWS]
        at = N_VEC
        for ref in (bq_ref, bf_ref):
            n = ref.shape[1] // vec_ref.shape[1]
            chunk = lambda q: row(vec_ref, at + q % n)[:, q // n * HEAD:(q // n + 1) * HEAD]
            for lo in range(0, ref.shape[1], LANES):
                ref[:, lo:lo + LANES] = jnp.concatenate([chunk(lo // HEAD), chunk(lo // HEAD + 1)], axis=1)
            at += n

    now_ref[:] = next_ref[:]
    next_ref[:] = dot_nt(zo_ref[:], wt_ref[:]) + jnp.where(is_class(GROWS), row(vec_ref, CLS), row(vec_ref, B_PATCH))
    hat, inv = normalize(now_ref[:])
    hat_ref[:] = hat
    h0 = hat * row(vec_ref, LNP_G) + row(vec_ref, LNP_B)
    mean1 = row_mean(h0)
    centered = h0 - mean1
    inv1 = lax.rsqrt(row_mean(centered * centered) + LN_EPS)
    a_ref[:] = (centered * inv1 * row(vec_ref, LN1_G) + row(vec_ref, LN1_B)).astype(BF16)
    lane = iota(stat_ref.shape, 1)
    stat_ref[:] = jnp.where(lane == 0, inv, jnp.where(lane == 1, inv1, mean1))


def embed(zo, first, d_mlp):
    n_tok = zo.shape[0]
    d, width = first.shape
    n = n_tok // GROWS
    outs = ((VEC_ROWS, d), (1, width - PACK), (1, d_mlp))
    return call(embed_kernel, (), (zo, first), grid=(n + 1,),
                in_specs=[this_block(GROWS, PACK, n), held_cols(d, PACK, width - PACK)],
                out_specs=[last_block(GROWS, d), last_block(GROWS, d), last_block(GROWS, LANES)] + [whole_out(s) for s in outs],
                out_shape=[shaped((n_tok, d)), shaped((n_tok, d), BF16), shaped((n_tok, LANES))] + [shaped(s) for s in outs],
                scratch_shapes=[pltpu.VMEM((GROWS, d), F32)] * 2, flops=2 * zo.size * d)


def window_mask(start):
    key, query = (iota((WIN, 2 * WIN), axis) for axis in (0, 1))
    return jnp.where(image_of(key + start) == image_of(lax.rem(query, WIN) + start), 0.0, MASKED)


def set_masks(mask_ref):
    for i, start in enumerate(STARTS):
        mask_ref[i] = window_mask(start)


def split_heads(x):
    first = iota(x.shape, 1) < HEAD
    zero = jnp.zeros_like(x)
    return jnp.concatenate([jnp.where(first, x, zero), jnp.where(first, zero, x)], axis=0)


def join_heads(x):
    return jnp.where(iota((WIN, LANES), 1) < HEAD, x[:WIN], x[WIN:])


def join_windows(lo, hi):
    at = EDGE + SUBLANES
    shift = STARTS[1]
    edge = jnp.where(iota((SUBLANES, LANES), 0) < 2 * TOK - EDGE, lo[EDGE:at], hi[EDGE - shift:at - shift])
    return jnp.concatenate([lo[:EDGE], edge, hi[at - shift:]], axis=0)


def weights_t(logits, mask, scale):
    masked = logits + mask
    e = jnp.exp2((masked - col_max(masked)) * (scale * LOG2E))
    return e * (1.0 / col_sum(e))


def lane_tile(at):
    return slice(at * LANES, (at + 1) * LANES)


def reader(ref):
    return lambda at, i: ref[STARTS[i]:STARTS[i] + WIN, lane_tile(at)]


def every_unit(n_tiles):
    return [(pair, i) for pair in range(n_tiles) for i in range(len(STARTS))]


def window_scratch():
    return pltpu.VMEM((len(STARTS), WIN, 2 * WIN), F32)


def attend_kernel(scale, a_ref, w_ref, b_ref, qkv_ref, o_ref, mask_ref):
    @first_step()
    def _():
        set_masks(mask_ref)

    n_tiles = o_ref.shape[1] // LANES
    a = a_ref[:]
    for lo in range(0, b_ref.shape[1], STEP):
        cols = slice(lo, lo + STEP)
        qkv_ref[:, cols] = (dot(a, w_ref[:, cols]) + b_ref[:, cols]).astype(BF16)
    read, units = reader(qkv_ref), every_unit(n_tiles)
    logits = [dot_nt(read(n_tiles + pair, i), split_heads(read(pair, i))) for pair, i in units]
    probs = [weights_t(x, mask_ref[i], scale).astype(BF16) for x, (_, i) in zip(logits, units)]
    outs = [join_heads(dot_tn(p, read(2 * n_tiles + pair, i))) for p, (pair, i) in zip(probs, units)]
    for lo, hi, (pair, _) in zip(outs[::2], outs[1::2], units[::2]):
        o_ref[:, lane_tile(pair)] = join_windows(lo, hi).astype(BF16)


def attend(a, first, b_qkv, scale):
    n_tok, d = a.shape
    width = b_qkv.shape[1]
    return call(functools.partial(attend_kernel, scale), (), (a, first, b_qkv), grid=(n_tok // ROWS,),
                in_specs=[rows_spec(ROWS, d), held_cols(d, width, 0), held(b_qkv.shape)],
                out_specs=[rows_spec(ROWS, width), rows_spec(ROWS, d)],
                out_shape=[shaped((n_tok, width), BF16), shaped((n_tok, d), BF16)],
                scratch_shapes=[window_scratch()], flops=4 * a.size * width)


def attend_grad_kernel(scale, qkv_ref, dctx_ref, dqkv_ref, bsum_ref, mask_ref):
    @first_step()
    def _():
        set_masks(mask_ref)
        clear(bsum_ref)

    n_tiles = dctx_ref.shape[1] // LANES
    read, read_grad, units = reader(qkv_ref), reader(dctx_ref), every_unit(n_tiles)
    q2 = [split_heads(read(pair, i)) for pair, i in units]
    do2 = [split_heads(read_grad(pair, i)) for pair, i in units]
    logits = [dot_nt(read(n_tiles + pair, i), q) for q, (pair, i) in zip(q2, units)]
    dp = [dot_nt(read(2 * n_tiles + pair, i), do) for do, (pair, i) in zip(do2, units)]
    logits = [x * scale + mask_ref[i] for x, (_, i) in zip(logits, units)]
    e = [jnp.exp2((x - col_max(x)) * LOG2E) for x in logits]
    p = [x * (1.0 / col_sum(x)) for x in e]
    dv = [dot(x.astype(BF16), do) for x, do in zip(p, do2)]
    ds = [(x * (y - col_sum(x * y)) * scale).astype(BF16) for x, y in zip(p, dp)]
    dk = [dot(x, q) for x, q in zip(ds, q2)]
    dq = [join_heads(dot_tn(x, read(n_tiles + pair, i))) for x, (pair, i) in zip(ds, units)]
    for at, (pair, _) in enumerate(units[::2]):
        for part, grads in enumerate((dq, dk, dv)):
            both = join_windows(grads[2 * at], grads[2 * at + 1])
            cols = lane_tile(part * n_tiles + pair)
            dqkv_ref[:, cols] = both.astype(BF16)
            bsum_ref[:, cols] += col_sum(both)


def attend_grad(qkv, d_ctx, scale, after):
    n_tok, width = qkv.shape
    return call(functools.partial(attend_grad_kernel, scale), after, (qkv, d_ctx), grid=(n_tok // ROWS,),
                in_specs=[rows_spec(ROWS, width), rows_spec(ROWS, d_ctx.shape[1])], out_specs=[rows_spec(ROWS, width), whole_out((1, width))],
                out_shape=[shaped((n_tok, width), BF16), shaped((1, width))],
                scratch_shapes=[window_scratch()], flops=3 * d_ctx.size * width)


def erf_cdf(u):
    return 0.5 + 0.5 * lax.erf(u * INV_SQRT2)


def mlp_up_kernel(o_ref, hat_ref, wo_ref, wf_ref, vec_ref, bf_ref, m_ref, c_ref, act_ref, pre_ref, next_ref, now_ref):
    now_ref[:] = next_ref[:]
    m = hat_ref[:] * row(vec_ref, LNP_G) + row(vec_ref, LNP_B) + dot(o_ref[:], wo_ref[:]) + row(vec_ref, B_OUT)
    m_ref[:] = m
    hat2, _ = normalize(m)
    next_c = (hat2 * row(vec_ref, LN2_G) + row(vec_ref, LN2_B)).astype(BF16)
    c_ref[:] = next_c
    c = now_ref[:]
    for lo in range(0, wf_ref.shape[1], STEP):
        cols = slice(lo, lo + STEP)
        u = dot(c, wf_ref[:, cols]) + bf_ref[:, cols]
        pre_ref[:, cols] = u
        act_ref[:, cols] = (u * erf_cdf(u)).astype(BF16)
    next_ref[:] = next_c


def mlp_up(o, hat, w_fo, vecs, b_fc):
    n_tok, d = o.shape
    f = b_fc.shape[1]
    n = n_tok // ROWS
    return call(mlp_up_kernel, (), (o, hat, w_fo, w_fo, vecs, b_fc), grid=(n + 1,),
                in_specs=[this_block(ROWS, d, n), this_block(ROWS, d, n), held_cols(d, d, f), held_cols(d, f, 0), held(vecs.shape), held(b_fc.shape)],
                out_specs=[this_block(ROWS, d, n), this_block(ROWS, d, n), last_block(ROWS, f), last_block(ROWS, f)],
                out_shape=[shaped((n_tok, d)), shaped((n_tok, d), BF16), shaped((n_tok, f), BF16), shaped((n_tok, f))],
                scratch_shapes=[pltpu.VMEM((ROWS, d), BF16)] * 2, flops=3 * o.size * f)


def mlp_down_kernel(act_ref, m_ref, w_ref, vec_ref, h1_ref):
    h1 = (m_ref[:] + dot(act_ref[:], w_ref[:]) + row(vec_ref, B_PROJ)).astype(BF16)
    to, source = iota((GROWS, GROWS), 0), iota((GROWS, GROWS), 1)
    move = one_hot(source == lax.rem(to, MANY) * TOK + lax.div(to, MANY))
    h1_ref.reshape(GROWS, h1_ref.shape[2])[:] = dot(move, h1).astype(BF16)


def mlp_down(act, m, w_proj, vecs, after):
    n_tok, f = act.shape
    d = m.shape[1]
    return call(mlp_down_kernel, after, (act, m, w_proj, vecs), grid=(n_tok // GROWS,),
                in_specs=[rows_spec(GROWS, f), rows_spec(GROWS, d), held(w_proj.shape), held(vecs.shape)],
                out_specs=pl.BlockSpec((TOK, MANY, d), lambda i: (0, i, 0)),
                out_shape=shaped((TOK, n_tok // TOK, d), BF16), flops=2 * m.size * f)


def mlp_grad_kernel(g_ref, pre_ref, m_ref, wp_ref, wf_ref, wo_ref, vec_ref, dpre_ref, dmid_ref, dmidb_ref, dctx_ref, vsum_ref, bfc_ref):
    @first_step()
    def _():
        clear(vsum_ref, bfc_ref)

    g = g_ref[:]
    step = 2 * STEP
    d_c = jnp.zeros(m_ref.shape, F32)
    cuts = [slice(lo, lo + step) for lo in range(0, wp_ref.shape[0], step)]
    acts, pres = dict(), dict()
    n = len(cuts)
    for tick in range(n + 2):
        if tick < n:
            acts[tick] = dot_nt(g, wp_ref[cuts[tick], :])
        if 0 <= tick - 1 < n:
            cols = cuts[tick - 1]
            u = pre_ref[:, cols]
            w = u * INV_SQRT2
            d_pre = acts.pop(tick - 1) * (0.5 + 0.5 * lax.erf(w) + u * (jnp.exp2((w * w) * (-LOG2E)) * INV_SQRT_2PI))
            bfc_ref[:, cols] += col_sum(d_pre)
            pres[tick - 1] = d_pre.astype(BF16)
            dpre_ref[:, cols] = pres[tick - 1]
        if tick >= 2:
            d_c = d_c + dot_nt(pres.pop(tick - 2), wf_ref[:, cuts[tick - 2]])
    hat2, inv2 = normalize(m_ref[:])
    g_f = g.astype(F32)
    d_mid = norm_grad(d_c, hat2, inv2, row(vec_ref, LN2_G)) + g_f
    dmid_ref[:] = d_mid
    d_mid_b = d_mid.astype(BF16)
    dmidb_ref[:] = d_mid_b
    dctx_ref[:] = dot_nt(d_mid_b, wo_ref[:]).astype(BF16)
    for at, part in enumerate((d_mid, d_c * hat2, d_c, g_f)):
        vsum_ref[at:at + 1, :] += col_sum(part)


def mlp_grad(g, pre, m, w_proj, w_fo, vecs, after):
    n_tok, d = g.shape
    f = pre.shape[1]
    wide, narrow = rows_spec(GROWS, f), rows_spec(GROWS, d)
    return call(mlp_grad_kernel, after, (g, pre, m, w_proj, w_fo, w_fo, vecs), grid=(n_tok // GROWS,),
                in_specs=[narrow, wide, narrow, held(w_proj.shape), held_cols(d, f, 0), held_cols(d, d, f), held(vecs.shape)],
                out_specs=[wide, narrow, narrow, narrow, whole_out((SUBLANES, d)), whole_out((1, f))],
                out_shape=[shaped((n_tok, f), BF16), shaped((n_tok, d)), shaped((n_tok, d), BF16), shaped((n_tok, d), BF16),
                           shaped((SUBLANES, d)), shaped((1, f))],
                flops=5 * g.size * f)


CUTS = (0, 104, 208, 304, GROWS)


def embed_grad_kernel(dqkv_ref, dmid_ref, hat_ref, stat_ref, w_ref, vec_ref, demb_ref, vsum_ref, next_ref, now_ref, dx_ref):
    step = pl.program_id(0)

    @first_step()
    def _():
        clear(vsum_ref)

    now_ref[:] = next_ref[:]
    width = now_ref.shape[1] // (len(CUTS) - 1)
    sums = []
    for j, (lo, hi) in enumerate(zip(CUTS, CUTS[1:])):
        cols, rows = slice(j * width, (j + 1) * width), slice(lo, hi)
        next_ref[:, cols] = dot_nt(dqkv_ref[:], w_ref[cols, :])
        d_a, hat_p = now_ref[rows, :], hat_ref[rows, :]
        inv_p, inv1, mean1 = (stat_ref[rows, k:k + 1] for k in range(3))
        hat1 = (hat_p * row(vec_ref, LNP_G) + row(vec_ref, LNP_B) - mean1) * inv1
        d_zero = norm_grad(d_a, hat1, inv1, row(vec_ref, LN1_G)) + dmid_ref[rows, :]
        d_x = norm_grad(d_zero, hat_p, inv_p, row(vec_ref, LNP_G))
        demb_ref[rows, :] = d_x.astype(BF16)
        dx_ref[rows, :] = d_x
        sums.append([col_sum(part) for part in (d_x, d_zero * hat_p, d_zero, d_a * hat1, d_a)])
    d_all, *others = (sum(parts) for parts in zip(*sums))
    d_cls = sum(row(dx_ref, at) for at in range(0, GROWS, TOK))
    for at, part in enumerate([d_all - d_cls, d_cls] + others):
        vsum_ref[at:at + 1, :] += jnp.where(step > 0, part, 0.0)


def embed_grad(dqkv, d_mid, hat, stats, first, vecs, after):
    n_tok, d = d_mid.shape
    width = dqkv.shape[1]
    n = n_tok // GROWS
    return call(embed_grad_kernel, after, (dqkv, d_mid, hat, stats, first, vecs), grid=(n + 1,),
                in_specs=[this_block(GROWS, width, n), last_block(GROWS, d), last_block(GROWS, d), last_block(GROWS, LANES),
                          held_cols(d, width, 0), held(vecs.shape)],
                out_specs=[last_block(GROWS, d), whole_out((SUBLANES, d))], out_shape=[shaped((n_tok, d), BF16), shaped((SUBLANES, d))],
                scratch_shapes=[pltpu.VMEM((GROWS, d), F32)] * 3, flops=3 * d_mid.size * width)


def tail_kernel(se_ref, sm_ref, sq_ref, sf_ref, out_ref, rows_ref):
    d = se_ref.shape[1]
    clear(rows_ref)
    at, cut = VEC_AT, VEC_AT + B_OUT
    rows_ref[at:cut, :] = se_ref[:B_OUT, :]
    at += N_VEC
    rows_ref[cut:at, :] = sm_ref[:N_VEC - B_OUT, :]
    for ref in (sq_ref, sf_ref):
        n = ref.shape[1] // d
        for r in range(n):
            chunk = lambda q: ref[:, (n * q + r) * HEAD:(n * q + r + 1) * HEAD]
            for j in range(d // LANES):
                rows_ref[at:at + 1, lane_tile(j)] = jnp.concatenate([chunk(2 * j), chunk(2 * j + 1)], axis=1)
            at += 1
    for j in range(d // LANES):
        out_ref[lane_tile(j)] = rows_ref[:, lane_tile(j)].T


def vector_tail(*args):
    d = args[0].shape[1]
    return call(tail_kernel, (), args, in_specs=[held(x.shape) for x in args], out_specs=whole_out((d, LANES)), out_shape=shaped((d, LANES)),
                scratch_shapes=[pltpu.VMEM((LANES, d), F32)], flops=d)


MESH_AXIS = 'fsdp'
LINKS = ('core', 'x', 'y', 'z')
GRID = LINKS[:0:-1]
CHIPS = 1 << len(GRID)
ORDERS = tuple(LINKS[k:] + LINKS[1:k] for k in range(1, len(LINKS)))


def bit(at, link):
    return lax.rem(lax.div(at, 1 << LINKS.index(link)), 2)


def wgrad_kernel(orders, edges, by_rows, has_tail, a_ref, b_ref, *refs):
    tail_ref = refs[0] if has_tail else None
    n_out = 2 * len(orders)
    outs, refs = refs[has_tail:has_tail + n_out], refs[has_tail + n_out:]
    made_ref, got_ref, own_ref, send_sem, got_sem, free_sem, out_sem = refs[:7]
    step, last = pl.program_id(0), pl.num_programs(0) - 1
    slot = lax.rem(step, 2)
    me = lax.axis_index(MESH_AXIS)
    mine = bit(me, 'core')
    partner = dict(device_id=(me + 1 - 2 * mine,), device_id_type=pl.DeviceIdType.MESH)

    def part(at, core):
        return made_ref.at[at, core] if by_rows else made_ref.at[at, :, core]

    def exchange(at):
        return pltpu.make_async_remote_copy(part(at, 1 - mine), got_ref.at[at], send_sem.at[at], got_sem.at[at], **partner)

    def copies(at, tile, order_index, wanted):
        link = orders[order_index][0]
        out = outs[2 * order_index + wanted]
        sem = out_sem.at[at, order_index if by_rows else wanted]
        if by_rows:
            rest = [bit(2 * tile, other) for other in GRID if other != link]
            lo, hi = edges[order_index:order_index + 2]
            return pltpu.make_async_copy(own_ref.at[at, :, pl.ds(lo, hi - lo)], out.at[rest[0], rest[1]], sem)
        width = own_ref.shape[-1]
        cols = pl.ds(pl.multiple_of((tile - edges[order_index] // width) * width, width), width)
        side = bit(me, link) if wanted else 1 - bit(me, link)
        return pltpu.make_async_copy(own_ref.at[(at,) + (slice(None),) * GRID.index(link) + (side,)], out.at[:, :, :, cols], sem)

    def stored(at):
        if by_rows:
            for index in range(len(orders)):
                copies(at, 0, index, 0).wait()
        else:
            for wanted in range(2):
                copies(at, 0, 0, wanted).wait()

    def finish(at, tile):
        exchange(at).wait_recv()

        @pl.when(tile >= 2)
        def _():
            stored(at)

        own_ref[at] = (part(at, mine)[:] + got_ref[at]).reshape(own_ref.shape[1:])

        @pl.when(tile + 2 <= last)
        def _():
            pl.semaphore_signal(free_sem.at[at], **partner)

        for index, order in enumerate(orders):
            if by_rows:
                same = bit(2 * tile, order[0]) == bit(me, order[0])
                for wanted, test in enumerate((jnp.logical_not(same), same)):
                    pl.when(test)(copies(at, tile, index, wanted).start)
            else:
                width = own_ref.shape[-1]

                @pl.when((tile >= edges[index] // width) & (tile < edges[index + 1] // width))
                def _():
                    for wanted in range(2):
                        copies(at, tile, index, wanted).start()

    @first_step()
    def _():
        barrier = pltpu.get_barrier_semaphore()
        pl.semaphore_signal(barrier, **partner)
        if not by_rows:
            for j in range(a_ref.shape[1] // LANES):
                refs[-1][lane_tile(j), :] = a_ref[:, lane_tile(j)].T
        pl.semaphore_wait(barrier, 1)

    @pl.when(step >= 2)
    def _():
        exchange(slot).wait_send()

    total = dot_tn(a_ref[:], b_ref[:]) if by_rows else dot(refs[-1][:], b_ref[:])
    made_ref[slot] = total.reshape(made_ref.shape[1:])
    if has_tail:
        @pl.when(step == last)
        def _():
            end = own_ref.shape[-1] - LANES
            made_ref[slot, :, :, :, end:] += tail_ref[:].reshape(made_ref.shape[1:4] + (LANES,))

    @pl.when(step >= 2)
    def _():
        pl.semaphore_wait(free_sem.at[slot], 1)

    exchange(slot).start()

    @pl.when(step >= 1)
    def _():
        finish(1 - slot, step - 1)

    @pl.when(step == last)
    def _():
        finish(slot, step)
        for at in range(2):
            exchange(at).wait_send()
            stored(at)


def wgrad(a, b, orders, edges, number, after, tile=STEP, by_rows=False, tail=()):
    k, m = a.shape
    n = b.shape[1]
    r = m // (2 * CHIPS)
    shapes = [shaped((2, 2, r, hi - lo)) for lo, hi in zip(edges, edges[1:]) for _ in range(2)]
    if by_rows:
        steps, block, own = CHIPS, (2, r, n), (r, n)
        in_specs = [pl.BlockSpec((k, 2 * r), lambda j: (0, j)), held(b.shape)]
        got, scratch = own, []
    else:
        steps, block, own = n // tile, (CHIPS, 2, r, tile), (2,) * len(GRID) + (r, tile)
        in_specs = [held(a.shape), pl.BlockSpec((k, tile), lambda j: (0, j))] + [held(x.shape) for x in tail]
        got, scratch = (CHIPS, r, tile), [pltpu.VMEM((m, k), BF16)]
    dma = pltpu.SemaphoreType.DMA
    return call(functools.partial(wgrad_kernel, orders, edges, by_rows, len(tail)), after, (a, b) + tuple(tail), grid=(steps,),
                in_specs=in_specs, out_specs=[ANY] * len(shapes), out_shape=shapes,
                scratch_shapes=[pltpu.VMEM((2,) + block, F32), pltpu.VMEM((2,) + got, F32), pltpu.VMEM((2,) + own, F32),
                                dma((2,)), dma((2,)), pltpu.SemaphoreType.REGULAR((2,)), dma((2, max(2, len(orders))))] + scratch,
                flops=2 * k * m * n, partners=number)


def add_kernel(*refs):
    _, *refs = refs
    n = len(refs) // 3
    for at in range(n):
        refs[2 * n + at][:] = refs[2 * at][:] + refs[2 * at + 1][:]


def halves(me, items, level, after):
    args, in_specs, shapes, out_specs = [], [], [], []
    for order, kept, received in items:
        links = [link for link in GRID if link not in order[:level]]
        at = links.index(order[level])
        r, n = kept.shape[-2:]
        rest = (2,) * (len(links) - 1)
        for keep in range(2):
            def index(i, s, keep=keep, at=at, count=len(links), link=order[level]):
                lead = [i] * count
                lead[at] = bit(s[0], link) if keep else 1 - bit(s[0], link)
                return (*lead, 0, 0)

            args += [kept, received]
            in_specs += [pl.BlockSpec((None,) * len(links) + (r, n), index)] * 2
            shapes.append(shaped(rest + (r, n)))
            out_specs.append(pl.BlockSpec((None,) * len(rest) + (r, n), lambda i, s, count=len(rest): (i,) * count + (0, 0)))
    outs = call(add_kernel, after, args, prefetch=(me,), grid=(len(GRID) - level,), in_specs=in_specs, out_specs=out_specs,
                out_shape=shapes, flops=STEP * sum(x.size for x in shapes))
    return list(zip(outs[::2], outs[1::2]))


def add_columns(out_ref, refs):
    lo = 0
    for kept, received in zip(refs[::2], refs[1::2]):
        hi = lo + kept.shape[1]
        out_ref[:, lo:hi] = kept[:] + received[:]
        lo = hi


def join_kernel(counts, *refs):
    n = 2 * sum(counts)
    at = 0
    for out_ref, count in zip(refs[n:], counts):
        add_columns(out_ref, refs[at:at + 2 * count])
        at += 2 * count


def join(groups, after):
    args = [x for group in groups for pair in group for x in pair]
    shapes = [shaped((group[0][0].shape[0], sum(kept.shape[1] for kept, _ in group))) for group in groups]
    return call(functools.partial(join_kernel, [len(group) for group in groups]), after, args,
                in_specs=[held(x.shape) for x in args], out_specs=[whole_out(s.shape) for s in shapes],
                out_shape=shapes, flops=STEP * sum(s.size for s in shapes))


def finish_kernel(n_in, n_pix, n_pos, *refs):
    (wt_ref, pos_ref, *vec_refs), full_ref = refs[n_in:-1], refs[-1]
    add_columns(full_ref, refs[:n_in])
    wt_ref[:] = full_ref[:, :n_pix]
    pos_ref[:] = full_ref[:, n_pix:n_pix + n_pos]
    pos_ref[:, :1] = full_ref[:, VEC_ROW + CLS:VEC_ROW + CLS + 1]
    rows = full_ref[:, VEC_ROW - VEC_AT:VEC_ROW - VEC_AT + LANES].T
    at = VEC_AT
    for ref in vec_refs:
        for lo in range(0, ref.shape[1], HEAD):
            ref[:, lo:lo + HEAD] = rows[at:at + 1]
            at += 1


def finish_small(pairs, n_pix, n_pos, widths, after):
    args = [x for pair in pairs for x in pair]
    shapes = [shaped((HEAD, n_pix)), shaped((HEAD, n_pos))] + [shaped((1, w)) for w in widths]
    return call(functools.partial(finish_kernel, len(args), n_pix, n_pos), after, args, in_specs=[held(x.shape) for x in args],
                out_specs=[whole_out(s.shape) for s in shapes], out_shape=shapes,
                scratch_shapes=[pltpu.VMEM((HEAD, PACK), F32)], flops=PACK)


PARAM_NAMES = ('w_patch', 'b_patch', 'pos_table', 'cls_tok', 'lnp_g', 'lnp_b', 'ln1_g', 'ln1_b', 'w_qkv', 'b_qkv', 'w_out', 'b_out', 'ln2_g', 'ln2_b', 'w_fc', 'b_fc', 'w_proj', 'b_proj')
PACKED = tuple(PARAM_NAMES[i] for i in (1, 3, 4, 5, 6, 7, 11, 12, 13, 17, 9, 15))


def solution(mesh):
    n_dev = mesh.shape[MESH_AXIS]

    def across(value, link):
        return lax.ppermute(value, MESH_AXIS, [(i, i ^ (1 << LINKS.index(link))) for i in range(n_dev)])

    def compute(patches, keep, *rest):
        shard = dict(zip(PARAM_NAMES, rest[:-1]))
        d, d_mlp = shard['w_out'].shape[1], shard['w_fc'].shape[1]
        n_pix, n_pos = shard['w_patch'].shape[0], shard['pos_table'].shape[0]
        scale = shard['w_qkv'].shape[-1] ** -0.5
        me = lax.axis_index(MESH_AXIS).reshape(1)
        by_token = lambda x: x.transpose(1, 0, 2)

        def whole(value):
            return lax.all_gather(value, MESH_AXIS, tiled=True)

        w_qkv = shard['w_qkv'].astype(BF16).reshape(HEAD, -1)
        first = whole(pack_small(w_qkv, shard['w_patch'].T, shard['pos_table'].T, [shard[name][None] for name in PACKED]))
        w_fo = whole(jnp.concatenate([shard['w_fc'].astype(BF16), shard['w_out'].astype(BF16)], axis=1))
        w_proj = whole(shard['w_proj'].astype(BF16))

        zo, g = pick_rows(keep, by_token(patches), by_token(rest[-1]))
        hat, a, stats, vecs, b_qkv, b_fc = embed(zo, first, d_mlp)
        qkv, ctx = attend(a, first, b_qkv, scale)
        m, c, act, pre = mlp_up(ctx, hat, w_fo, vecs, b_fc)

        def cut(outs, orders):
            return [(order, kept, across(sent, order[0])) for order, sent, kept in zip(orders, outs[::2], outs[1::2])]

        def halve(items, level, after):
            pairs = halves(me, items, level, after)
            return [(order, kept, across(sent, order[level])) for (order, _, _), (sent, kept) in zip(items, pairs)]

        def ends(items):
            return [(kept, received) for _, kept, received in items]

        two, one = ORDERS[:2], ORDERS[2:]
        outs = wgrad(act, g, two, (0, d // 2, d), 0, (), by_rows=True)
        proj = cut(outs, two)
        h1 = mlp_down(act, m, w_proj, vecs, (outs[1],))
        d_pre, d_mid, d_mid_b, d_ctx, sums_m, sum_fc = mlp_grad(g, pre, m, w_proj, w_fo, vecs, (h1,))
        proj = halve(proj, 1, (sum_fc,))
        outs = wgrad(c, d_pre, two, (0, d_mlp // 2, d_mlp), 1, (proj[0][1],))
        fc = cut(outs, two)
        proj = halve(proj, 2, (outs[1],))
        outs = wgrad(ctx, d_mid_b, one, (0, d), 2, (proj[0][1],))
        fc += cut(outs, one)
        d_qkv, sum_qkv = attend_grad(qkv, d_ctx, scale, (outs[1],))
        g_proj, = join([ends(proj)], (sum_qkv,))
        fc = halve(fc, 1, (g_proj,))
        outs = wgrad(a, d_qkv, ORDERS, (0, d, 2 * d, 3 * d), 3, (fc[0][1],))
        qkv = cut(outs, ORDERS)
        fc = halve(fc, 2, (outs[1],))
        d_emb, sums_e = embed_grad(d_qkv, d_mid, hat, stats, first, vecs, (fc[0][1],))
        qkv = halve(qkv, 1, (sums_e,))
        tail = vector_tail(sums_e, sums_m, sum_qkv, sum_fc)
        outs = wgrad(d_emb, zo, two, (0, PACK // 2, PACK), 4, (qkv[0][1],), tail=(tail,))
        small = cut(outs, two)
        qkv = halve(qkv, 2, (outs[1],))
        g_fc, g_out = join([ends(fc)[:2], ends(fc)[2:]], (qkv[0][1],))
        small = halve(small, 1, (g_fc,))
        g_qkv, = join([ends(qkv)], (small[0][1],))
        small = halve(small, 2, (g_qkv,))
        done = finish_small(ends(small), n_pix, n_pos, [shard[name].shape[0] for name in PACKED], (g_qkv,))

        grads = dict(w_patch=done[0].T, pos_table=done[1].T, w_qkv=g_qkv.reshape(shard['w_qkv'].shape), w_out=g_out, w_fc=g_fc, w_proj=g_proj)
        grads.update({name: value.reshape(-1) for name, value in zip(PACKED, done[2:])})
        return (by_token(h1),) + tuple(grads[name] for name in PARAM_NAMES)

    batch_spec = P(MESH_AXIS)
    param_specs = tuple(P(None, MESH_AXIS) if name in ('w_patch', 'pos_table') else batch_spec for name in PARAM_NAMES)
    return jax.shard_map(compute, mesh=mesh, in_specs=(batch_spec, batch_spec) + param_specs + (batch_spec,), out_specs=(batch_spec,) + param_specs, check_vma=False)
```

```python
import functools

import jax
import jax.numpy as jnp
from jax import lax
from jax.experimental import pallas as pl
from jax.experimental.pallas import tpu as pltpu
from jax.sharding import PartitionSpec as P


F32, BF16, I32 = jnp.float32, jnp.bfloat16, jnp.int32
LN_EPS = 1e-5
INV_SQRT2 = 0.7071067811865476
INV_SQRT_2PI = 0.3989422804014327
LOG2E = 1.4426950408889634
MASKED = -1e30
SUBLANES, LANES, HEAD = 8, 128, 64
TOK, FEW, MANY = 50, 4, 8
ROWS, GROWS = FEW * TOK, MANY * TOK
WIN = 112
STARTS = (0, ROWS - WIN)
EDGE = 96
PACK, VEC_ROW = 1024, 976
VEC_AT = VEC_ROW % LANES
N_VEC, VEC_ROWS = 10, 32
B_PATCH, CLS, LNP_G, LNP_B, LN1_G, LN1_B, B_OUT, LN2_G, LN2_B, B_PROJ = range(N_VEC)
STEP = 512
ALL_VMEM = 67043328
ANY = pl.BlockSpec(memory_space=pl.ANY)


def product(dims, left, right):
    return lax.dot_general(left, right, ((dims[:1], dims[1:]), ((), ())), preferred_element_type=F32)


dot = functools.partial(product, (1, 0))
dot_nt = functools.partial(product, (1, 1))
dot_tn = functools.partial(product, (0, 0))


def col_sum(x):
    return jnp.sum(x, axis=0, keepdims=True)


def col_max(x):
    return jnp.max(x, axis=0, keepdims=True)


def row_mean(x):
    return jnp.mean(x, axis=1, keepdims=True)


def row(ref, at):
    return ref[at:at + 1, :]


def iota(shape, axis):
    return lax.broadcasted_iota(I32, shape, axis)


def one_hot(test):
    return test.astype(F32).astype(BF16)


def origin(shape, *_):
    return (0,) * len(shape)


def held(shape):
    return pl.BlockSpec(shape, functools.partial(origin, shape), pipeline_mode=pl.Buffered(1))


def held_cols(n_rows, n_cols, at):
    return pl.BlockSpec((n_rows, n_cols), lambda *_: (0, at // n_cols), pipeline_mode=pl.Buffered(1))


def whole_out(shape):
    return pl.BlockSpec(shape, functools.partial(origin, shape))


def rows_spec(n_rows, width):
    return pl.BlockSpec((n_rows, width), lambda i, *_: (i, 0))


def this_block(n_rows, width, n):
    return pl.BlockSpec((n_rows, width), lambda i: (jnp.minimum(i, n - 1), 0))


def last_block(n_rows, width):
    return pl.BlockSpec((n_rows, width), lambda i: (jnp.maximum(i - 1, 0), 0))


def shaped(shape, dtype=F32):
    return jax.ShapeDtypeStruct(shape, dtype)


def call(kernel, after, args, *, prefetch=(), grid=(1,), in_specs, out_specs, out_shape, scratch_shapes=(), flops, n_bytes=0, partners=None):
    n_in, n_after = len(prefetch) + len(args), len(after)

    def body(*refs):
        return kernel(*refs[:n_in], *refs[n_in + n_after:])

    return pl.pallas_call(
        body,
        grid_spec=pltpu.PrefetchScalarGridSpec(
            num_scalar_prefetch=len(prefetch), grid=grid, in_specs=list(in_specs) + [ANY] * n_after,
            out_specs=out_specs, scratch_shapes=list(scratch_shapes)),
        out_shape=out_shape,
        compiler_params=pltpu.CompilerParams(
            dimension_semantics=(pltpu.ARBITRARY,) * len(grid), vmem_limit_bytes=ALL_VMEM,
            collective_id=partners, has_side_effects=partners is not None),
        cost_estimate=pl.CostEstimate(flops=int(flops), bytes_accessed=int(n_bytes), transcendentals=0),
    )(*prefetch, *args, *after)


def first_step():
    return pl.when(pl.program_id(0) == 0)


def clear(*refs):
    for ref in refs:
        ref[:] = jnp.zeros_like(ref)


def normalize(x):
    centered = x - row_mean(x)
    inv = lax.rsqrt(row_mean(centered * centered) + LN_EPS)
    return centered * inv, inv


def norm_grad(d_out, x_hat, inv, gain):
    d_hat = d_out * gain
    return inv * (d_hat - row_mean(d_hat) - x_hat * row_mean(d_hat * x_hat))


def image_of(at, n_img=FEW):
    return sum((at >= j * TOK).astype(I32) for j in range(1, n_img))


def is_class(n_rows):
    at = iota((n_rows, 1), 0)
    return at == TOK * image_of(at, n_rows // TOK)


def pack_kernel(wq_ref, wt_ref, pt_ref, *refs):
    *vec_refs, whole_ref, rows_ref, pos_ref = refs
    n_pix, n_pos, n_qkv = wt_ref.shape[1], pt_ref.shape[1], wq_ref.shape[1]
    whole_ref[:, :n_qkv] = wq_ref[:]
    out_ref = whole_ref.at[:, n_qkv:]
    out_ref[:, :n_pix] = wt_ref[:].astype(BF16)
    out_ref[:, n_pix:n_pix + LANES] = pt_ref[:, :LANES].astype(BF16)
    clear(rows_ref, pos_ref)
    pos_ref[:, :n_pos - LANES] = pt_ref[:, LANES:]
    at = VEC_AT
    for ref in vec_refs:
        for lo in range(0, ref.shape[1], HEAD):
            rows_ref[at:at + 1, :HEAD] = ref[:, lo:lo + HEAD]
            at += 1
    out_ref[:, n_pix + LANES:] = (pos_ref[:] + rows_ref[:].T[:HEAD]).astype(BF16)


def pack_small(wq, wt, pt, vecs):
    args = [wq, wt, pt] + vecs
    shape = (HEAD, wq.shape[1] + PACK)
    return call(pack_kernel, (), args, in_specs=[held(x.shape) for x in args], out_specs=whole_out(shape), out_shape=shaped(shape, BF16),
                scratch_shapes=[pltpu.VMEM((LANES, LANES), F32), pltpu.VMEM((HEAD, LANES), F32)], flops=PACK)


def pick_kernel(keep_ref, patches_ref, g_ref, zo_ref, gi_ref, pad_ref):
    n_patch, _, n_pix = patches_ref.shape
    clear(pad_ref)
    pad_ref[:, :TOK - 1] = keep_ref[:].astype(F32)
    image, lane = iota(pad_ref.shape, 0), iota(pad_ref.shape, 1)
    spread = pad_ref[:]
    for b in range(MANY):
        spread = jnp.where(image == b, pltpu.roll(pad_ref[:], TOK * b + 1, 1), spread)
    own = (lane > TOK * image) & (lane < TOK * image + TOK)
    token = col_sum(jnp.where(own, spread + 1.0, 0.0))
    source = col_sum(jnp.where(own, spread * MANY + image.astype(F32), 0.0))
    source = jnp.where(token > 0.0, source, -1.0)
    cols = jnp.where(image == 0, source, token).T[:GROWS].astype(I32)
    source, token = cols[:, :1], cols[:, 1:2]
    pick = one_hot(iota((GROWS, MANY * n_patch), 1) == source)
    zo_ref[:, :n_pix] = dot(pick, patches_ref.reshape(MANY * n_patch, n_pix)[:]).astype(BF16)
    zo_ref[:, n_pix:] = one_hot(iota((GROWS, PACK - n_pix), 1) == token)
    to, source = iota((GROWS, GROWS), 0), iota((GROWS, GROWS), 1)
    move = one_hot(to == lax.rem(source, MANY) * TOK + lax.div(source, MANY))
    gi_ref[:] = dot(move, g_ref.reshape(GROWS, g_ref.shape[2])[:]).astype(BF16)


def pick_rows(keep, patches_t, g_t):
    _, n_img, _ = patches_t.shape
    d = g_t.shape[2]
    n_tok = n_img * TOK
    by_image = lambda x: pl.BlockSpec((x.shape[0], MANY, x.shape[2]), lambda i: (0, i, 0))
    return call(pick_kernel, (), (keep, patches_t, g_t), grid=(n_img // MANY,),
                in_specs=[rows_spec(MANY, TOK - 1), by_image(patches_t), by_image(g_t)],
                out_specs=[rows_spec(GROWS, PACK), rows_spec(GROWS, d)], out_shape=[shaped((n_tok, PACK), BF16), shaped((n_tok, d), BF16)],
                scratch_shapes=[pltpu.VMEM((MANY, STEP), F32)], flops=STEP * patches_t.size)


def embed_kernel(zo_ref, wt_ref, hat_ref, a_ref, stat_ref, vec_ref, bq_ref, bf_ref, next_ref, now_ref):
    @first_step()
    def _():
        base = VEC_ROW - VEC_AT
        vec_ref[:] = wt_ref[:, base:base + LANES].astype(F32).T[VEC_AT:VEC_AT + VEC_ROWS]
        at = N_VEC
        for ref in (bq_ref, bf_ref):
            n = ref.shape[1] // vec_ref.shape[1]
            chunk = lambda q: row(vec_ref, at + q % n)[:, q // n * HEAD:(q // n + 1) * HEAD]
            for lo in range(0, ref.shape[1], LANES):
                ref[:, lo:lo + LANES] = jnp.concatenate([chunk(lo // HEAD), chunk(lo // HEAD + 1)], axis=1)
            at += n

    now_ref[:] = next_ref[:]
    next_ref[:] = dot_nt(zo_ref[:], wt_ref[:]) + jnp.where(is_class(GROWS), row(vec_ref, CLS), row(vec_ref, B_PATCH))
    hat, inv = normalize(now_ref[:])
    hat_ref[:] = hat
    h0 = hat * row(vec_ref, LNP_G) + row(vec_ref, LNP_B)
    mean1 = row_mean(h0)
    centered = h0 - mean1
    inv1 = lax.rsqrt(row_mean(centered * centered) + LN_EPS)
    a_ref[:] = (centered * inv1 * row(vec_ref, LN1_G) + row(vec_ref, LN1_B)).astype(BF16)
    lane = iota(stat_ref.shape, 1)
    stat_ref[:] = jnp.where(lane == 0, inv, jnp.where(lane == 1, inv1, mean1))


def embed(zo, first, d_mlp):
    n_tok = zo.shape[0]
    d, width = first.shape
    n = n_tok // GROWS
    outs = ((VEC_ROWS, d), (1, width - PACK), (1, d_mlp))
    return call(embed_kernel, (), (zo, first), grid=(n + 1,),
                in_specs=[this_block(GROWS, PACK, n), held_cols(d, PACK, width - PACK)],
                out_specs=[last_block(GROWS, d), last_block(GROWS, d), last_block(GROWS, LANES)] + [whole_out(s) for s in outs],
                out_shape=[shaped((n_tok, d)), shaped((n_tok, d), BF16), shaped((n_tok, LANES))] + [shaped(s) for s in outs],
                scratch_shapes=[pltpu.VMEM((GROWS, d), F32)] * 2, flops=2 * zo.size * d)


def window_mask(start):
    key, query = (iota((WIN, 2 * WIN), axis) for axis in (0, 1))
    return jnp.where(image_of(key + start) == image_of(lax.rem(query, WIN) + start), 0.0, MASKED)


def set_masks(mask_ref):
    for i, start in enumerate(STARTS):
        mask_ref[i] = window_mask(start)


def split_heads(x):
    first = iota(x.shape, 1) < HEAD
    zero = jnp.zeros_like(x)
    return jnp.concatenate([jnp.where(first, x, zero), jnp.where(first, zero, x)], axis=0)


def join_heads(x):
    return jnp.where(iota((WIN, LANES), 1) < HEAD, x[:WIN], x[WIN:])


def join_windows(lo, hi):
    at = EDGE + SUBLANES
    shift = STARTS[1]
    edge = jnp.where(iota((SUBLANES, LANES), 0) < 2 * TOK - EDGE, lo[EDGE:at], hi[EDGE - shift:at - shift])
    return jnp.concatenate([lo[:EDGE], edge, hi[at - shift:]], axis=0)


def weights_t(logits, mask, scale):
    masked = logits + mask
    e = jnp.exp2((masked - col_max(masked)) * (scale * LOG2E))
    return e * (1.0 / col_sum(e))


def lane_tile(at):
    return slice(at * LANES, (at + 1) * LANES)


def reader(ref):
    return lambda at, i: ref[STARTS[i]:STARTS[i] + WIN, lane_tile(at)]


def every_unit(n_tiles):
    return [(pair, i) for pair in range(n_tiles) for i in range(len(STARTS))]


def window_scratch():
    return pltpu.VMEM((len(STARTS), WIN, 2 * WIN), F32)


def attend_kernel(scale, a_ref, w_ref, b_ref, qkv_ref, o_ref, mask_ref):
    @first_step()
    def _():
        set_masks(mask_ref)

    n_tiles = o_ref.shape[1] // LANES
    a = a_ref[:]
    for lo in range(0, b_ref.shape[1], STEP):
        cols = slice(lo, lo + STEP)
        qkv_ref[:, cols] = (dot(a, w_ref[:, cols]) + b_ref[:, cols]).astype(BF16)
    read, units = reader(qkv_ref), every_unit(n_tiles)
    logits = [dot_nt(read(n_tiles + pair, i), split_heads(read(pair, i))) for pair, i in units]
    probs = [weights_t(x, mask_ref[i], scale).astype(BF16) for x, (_, i) in zip(logits, units)]
    outs = [join_heads(dot_tn(p, read(2 * n_tiles + pair, i))) for p, (pair, i) in zip(probs, units)]
    for lo, hi, (pair, _) in zip(outs[::2], outs[1::2], units[::2]):
        o_ref[:, lane_tile(pair)] = join_windows(lo, hi).astype(BF16)


def attend(a, first, b_qkv, scale):
    n_tok, d = a.shape
    width = b_qkv.shape[1]
    return call(functools.partial(attend_kernel, scale), (), (a, first, b_qkv), grid=(n_tok // ROWS,),
                in_specs=[rows_spec(ROWS, d), held_cols(d, width, 0), held(b_qkv.shape)],
                out_specs=[rows_spec(ROWS, width), rows_spec(ROWS, d)],
                out_shape=[shaped((n_tok, width), BF16), shaped((n_tok, d), BF16)],
                scratch_shapes=[window_scratch()], flops=4 * a.size * width)


def attend_grad_kernel(scale, qkv_ref, dctx_ref, dqkv_ref, bsum_ref, mask_ref):
    @first_step()
    def _():
        set_masks(mask_ref)
        clear(bsum_ref)

    n_tiles = dctx_ref.shape[1] // LANES
    read, read_grad, units = reader(qkv_ref), reader(dctx_ref), every_unit(n_tiles)
    q2 = [split_heads(read(pair, i)) for pair, i in units]
    do2 = [split_heads(read_grad(pair, i)) for pair, i in units]
    logits = [dot_nt(read(n_tiles + pair, i), q) for q, (pair, i) in zip(q2, units)]
    dp = [dot_nt(read(2 * n_tiles + pair, i), do) for do, (pair, i) in zip(do2, units)]
    logits = [x * scale + mask_ref[i] for x, (_, i) in zip(logits, units)]
    e = [jnp.exp2((x - col_max(x)) * LOG2E) for x in logits]
    p = [x * (1.0 / col_sum(x)) for x in e]
    dv = [dot(x.astype(BF16), do) for x, do in zip(p, do2)]
    ds = [(x * (y - col_sum(x * y)) * scale).astype(BF16) for x, y in zip(p, dp)]
    dk = [dot(x, q) for x, q in zip(ds, q2)]
    dq = [join_heads(dot_tn(x, read(n_tiles + pair, i))) for x, (pair, i) in zip(ds, units)]
    for at, (pair, _) in enumerate(units[::2]):
        for part, grads in enumerate((dq, dk, dv)):
            both = join_windows(grads[2 * at], grads[2 * at + 1])
            cols = lane_tile(part * n_tiles + pair)
            dqkv_ref[:, cols] = both.astype(BF16)
            bsum_ref[:, cols] += col_sum(both)


def attend_grad(qkv, d_ctx, scale, after):
    n_tok, width = qkv.shape
    return call(functools.partial(attend_grad_kernel, scale), after, (qkv, d_ctx), grid=(n_tok // ROWS,),
                in_specs=[rows_spec(ROWS, width), rows_spec(ROWS, d_ctx.shape[1])], out_specs=[rows_spec(ROWS, width), whole_out((1, width))],
                out_shape=[shaped((n_tok, width), BF16), shaped((1, width))],
                scratch_shapes=[window_scratch()], flops=3 * d_ctx.size * width)


def erf_cdf(u):
    return 0.5 + 0.5 * lax.erf(u * INV_SQRT2)


def mlp_up_kernel(o_ref, hat_ref, wo_ref, wf_ref, vec_ref, bf_ref, m_ref, c_ref, act_ref, pre_ref, next_ref, now_ref):
    now_ref[:] = next_ref[:]
    m = hat_ref[:] * row(vec_ref, LNP_G) + row(vec_ref, LNP_B) + dot(o_ref[:], wo_ref[:]) + row(vec_ref, B_OUT)
    m_ref[:] = m
    hat2, _ = normalize(m)
    next_c = (hat2 * row(vec_ref, LN2_G) + row(vec_ref, LN2_B)).astype(BF16)
    c_ref[:] = next_c
    c = now_ref[:]
    for lo in range(0, wf_ref.shape[1], STEP):
        cols = slice(lo, lo + STEP)
        u = dot(c, wf_ref[:, cols]) + bf_ref[:, cols]
        pre_ref[:, cols] = u
        act_ref[:, cols] = (u * erf_cdf(u)).astype(BF16)
    next_ref[:] = next_c


def mlp_up(o, hat, w_fo, vecs, b_fc):
    n_tok, d = o.shape
    f = b_fc.shape[1]
    n = n_tok // ROWS
    return call(mlp_up_kernel, (), (o, hat, w_fo, w_fo, vecs, b_fc), grid=(n + 1,),
                in_specs=[this_block(ROWS, d, n), this_block(ROWS, d, n), held_cols(d, d, f), held_cols(d, f, 0), held(vecs.shape), held(b_fc.shape)],
                out_specs=[this_block(ROWS, d, n), this_block(ROWS, d, n), last_block(ROWS, f), last_block(ROWS, f)],
                out_shape=[shaped((n_tok, d)), shaped((n_tok, d), BF16), shaped((n_tok, f), BF16), shaped((n_tok, f))],
                scratch_shapes=[pltpu.VMEM((ROWS, d), BF16)] * 2, flops=3 * o.size * f)


def mlp_down_kernel(act_ref, m_ref, w_ref, vec_ref, h1_ref):
    h1 = (m_ref[:] + dot(act_ref[:], w_ref[:]) + row(vec_ref, B_PROJ)).astype(BF16)
    to, source = iota((GROWS, GROWS), 0), iota((GROWS, GROWS), 1)
    move = one_hot(source == lax.rem(to, MANY) * TOK + lax.div(to, MANY))
    h1_ref.reshape(GROWS, h1_ref.shape[2])[:] = dot(move, h1).astype(BF16)


def mlp_down(act, m, w_proj, vecs, after):
    n_tok, f = act.shape
    d = m.shape[1]
    return call(mlp_down_kernel, after, (act, m, w_proj, vecs), grid=(n_tok // GROWS,),
                in_specs=[rows_spec(GROWS, f), rows_spec(GROWS, d), held(w_proj.shape), held(vecs.shape)],
                out_specs=pl.BlockSpec((TOK, MANY, d), lambda i: (0, i, 0)),
                out_shape=shaped((TOK, n_tok // TOK, d), BF16), flops=2 * m.size * f)


def mlp_grad_kernel(g_ref, pre_ref, m_ref, wp_ref, wf_ref, wo_ref, vec_ref, dpre_ref, dmid_ref, dmidb_ref, dctx_ref, vsum_ref, bfc_ref):
    @first_step()
    def _():
        clear(vsum_ref, bfc_ref)

    g = g_ref[:]
    step = 2 * STEP
    d_c = jnp.zeros(m_ref.shape, F32)
    cuts = [slice(lo, lo + step) for lo in range(0, wp_ref.shape[0], step)]
    acts, pres = dict(), dict()
    n = len(cuts)
    for tick in range(n + 2):
        if tick < n:
            acts[tick] = dot_nt(g, wp_ref[cuts[tick], :])
        if 0 <= tick - 1 < n:
            cols = cuts[tick - 1]
            u = pre_ref[:, cols]
            w = u * INV_SQRT2
            d_pre = acts.pop(tick - 1) * (0.5 + 0.5 * lax.erf(w) + u * (jnp.exp2((w * w) * (-LOG2E)) * INV_SQRT_2PI))
            bfc_ref[:, cols] += col_sum(d_pre)
            pres[tick - 1] = d_pre.astype(BF16)
            dpre_ref[:, cols] = pres[tick - 1]
        if tick >= 2:
            d_c = d_c + dot_nt(pres.pop(tick - 2), wf_ref[:, cuts[tick - 2]])
    hat2, inv2 = normalize(m_ref[:])
    g_f = g.astype(F32)
    d_mid = norm_grad(d_c, hat2, inv2, row(vec_ref, LN2_G)) + g_f
    dmid_ref[:] = d_mid
    d_mid_b = d_mid.astype(BF16)
    dmidb_ref[:] = d_mid_b
    dctx_ref[:] = dot_nt(d_mid_b, wo_ref[:]).astype(BF16)
    for at, part in enumerate((d_mid, d_c * hat2, d_c, g_f)):
        vsum_ref[at:at + 1, :] += col_sum(part)


def mlp_grad(g, pre, m, w_proj, w_fo, vecs, after):
    n_tok, d = g.shape
    f = pre.shape[1]
    wide, narrow = rows_spec(GROWS, f), rows_spec(GROWS, d)
    return call(mlp_grad_kernel, after, (g, pre, m, w_proj, w_fo, w_fo, vecs), grid=(n_tok // GROWS,),
                in_specs=[narrow, wide, narrow, held(w_proj.shape), held_cols(d, f, 0), held_cols(d, d, f), held(vecs.shape)],
                out_specs=[wide, narrow, narrow, narrow, whole_out((SUBLANES, d)), whole_out((1, f))],
                out_shape=[shaped((n_tok, f), BF16), shaped((n_tok, d)), shaped((n_tok, d), BF16), shaped((n_tok, d), BF16),
                           shaped((SUBLANES, d)), shaped((1, f))],
                flops=5 * g.size * f)


CUTS = (0, 104, 208, 304, GROWS)


def embed_grad_kernel(dqkv_ref, dmid_ref, hat_ref, stat_ref, w_ref, vec_ref, demb_ref, vsum_ref, next_ref, now_ref, dx_ref):
    step = pl.program_id(0)

    @first_step()
    def _():
        clear(vsum_ref)

    now_ref[:] = next_ref[:]
    width = now_ref.shape[1] // (len(CUTS) - 1)
    sums = []
    for j, (lo, hi) in enumerate(zip(CUTS, CUTS[1:])):
        cols, rows = slice(j * width, (j + 1) * width), slice(lo, hi)
        next_ref[:, cols] = dot_nt(dqkv_ref[:], w_ref[cols, :])
        d_a, hat_p = now_ref[rows, :], hat_ref[rows, :]
        inv_p, inv1, mean1 = (stat_ref[rows, k:k + 1] for k in range(3))
        hat1 = (hat_p * row(vec_ref, LNP_G) + row(vec_ref, LNP_B) - mean1) * inv1
        d_zero = norm_grad(d_a, hat1, inv1, row(vec_ref, LN1_G)) + dmid_ref[rows, :]
        d_x = norm_grad(d_zero, hat_p, inv_p, row(vec_ref, LNP_G))
        demb_ref[rows, :] = d_x.astype(BF16)
        dx_ref[rows, :] = d_x
        sums.append([col_sum(part) for part in (d_x, d_zero * hat_p, d_zero, d_a * hat1, d_a)])
    d_all, *others = (sum(parts) for parts in zip(*sums))
    d_cls = sum(row(dx_ref, at) for at in range(0, GROWS, TOK))
    for at, part in enumerate([d_all - d_cls, d_cls] + others):
        vsum_ref[at:at + 1, :] += jnp.where(step > 0, part, 0.0)


def embed_grad(dqkv, d_mid, hat, stats, first, vecs, after):
    n_tok, d = d_mid.shape
    width = dqkv.shape[1]
    n = n_tok // GROWS
    return call(embed_grad_kernel, after, (dqkv, d_mid, hat, stats, first, vecs), grid=(n + 1,),
                in_specs=[this_block(GROWS, width, n), last_block(GROWS, d), last_block(GROWS, d), last_block(GROWS, LANES),
                          held_cols(d, width, 0), held(vecs.shape)],
                out_specs=[last_block(GROWS, d), whole_out((SUBLANES, d))], out_shape=[shaped((n_tok, d), BF16), shaped((SUBLANES, d))],
                scratch_shapes=[pltpu.VMEM((GROWS, d), F32)] * 3, flops=3 * d_mid.size * width)


def tail_kernel(se_ref, sm_ref, sq_ref, sf_ref, out_ref, rows_ref):
    d = se_ref.shape[1]
    clear(rows_ref)
    at, cut = VEC_AT, VEC_AT + B_OUT
    rows_ref[at:cut, :] = se_ref[:B_OUT, :]
    at += N_VEC
    rows_ref[cut:at, :] = sm_ref[:N_VEC - B_OUT, :]
    for ref in (sq_ref, sf_ref):
        n = ref.shape[1] // d
        for r in range(n):
            chunk = lambda q: ref[:, (n * q + r) * HEAD:(n * q + r + 1) * HEAD]
            for j in range(d // LANES):
                rows_ref[at:at + 1, lane_tile(j)] = jnp.concatenate([chunk(2 * j), chunk(2 * j + 1)], axis=1)
            at += 1
    for j in range(d // LANES):
        out_ref[lane_tile(j)] = rows_ref[:, lane_tile(j)].T


def vector_tail(*args):
    d = args[0].shape[1]
    return call(tail_kernel, (), args, in_specs=[held(x.shape) for x in args], out_specs=whole_out((d, LANES)), out_shape=shaped((d, LANES)),
                scratch_shapes=[pltpu.VMEM((LANES, d), F32)], flops=d)


MESH_AXIS = 'fsdp'
LINKS = ('core', 'x', 'y', 'z')
GRID = LINKS[:0:-1]
CHIPS = 1 << len(GRID)
ORDERS = tuple(LINKS[k:] + LINKS[1:k] for k in range(1, len(LINKS)))
RING = [at ^ (at >> 1) for at in range(CHIPS)]


def bit(at, link):
    return lax.rem(lax.div(at, 1 << LINKS.index(link)), 2)


def ring_chip(at):
    half, quarter = lax.div(at, 2), lax.div(at, 4)
    return 4 * quarter + 2 * lax.rem(half + quarter, 2) + lax.rem(at + half, 2)


def wgrad_kernel(orders, edges, by_rows, has_tail, a_ref, b_ref, *refs):
    tail_ref = refs[0] if has_tail else None
    n_out = 2 * len(orders) or 1
    outs, refs = refs[has_tail:has_tail + n_out], refs[has_tail + n_out:]
    made_ref, got_ref, own_ref, send_sem, got_sem, free_sem, out_sem = refs[:7]
    step, last = pl.program_id(0), pl.num_programs(0) - 1
    slot = lax.rem(step, 2)
    me = lax.axis_index(MESH_AXIS)
    mine = bit(me, 'core')
    partner = dict(device_id=(me + 1 - 2 * mine,), device_id_type=pl.DeviceIdType.MESH)

    def part(at, core):
        return made_ref.at[at, core] if by_rows else made_ref.at[at, :, core]

    def exchange(at):
        return pltpu.make_async_remote_copy(part(at, 1 - mine), got_ref.at[at], send_sem.at[at], got_sem.at[at], **partner)

    def whole(at, tile):
        width = own_ref.shape[-1]
        out = outs[0].at[tile] if by_rows else outs[0].at[:, :, pl.ds(pl.multiple_of(tile * width, width), width)]
        return pltpu.make_async_copy(own_ref.at[at], out, out_sem.at[at, 0])

    def copies(at, tile, order_index, wanted):
        link = orders[order_index][0]
        out = outs[2 * order_index + wanted]
        sem = out_sem.at[at, order_index if by_rows else wanted]
        if by_rows:
            rest = [bit(2 * tile, other) for other in GRID if other != link]
            lo, hi = edges[order_index:order_index + 2]
            return pltpu.make_async_copy(own_ref.at[at, :, pl.ds(lo, hi - lo)], out.at[rest[0], rest[1]], sem)
        width = own_ref.shape[-1]
        cols = pl.ds(pl.multiple_of((tile - edges[order_index] // width) * width, width), width)
        side = bit(me, link) if wanted else 1 - bit(me, link)
        return pltpu.make_async_copy(own_ref.at[(at,) + (slice(None),) * GRID.index(link) + (side,)], out.at[:, :, :, cols], sem)

    def stored(at):
        if not orders:
            whole(at, 0).wait()
        elif by_rows:
            for index in range(len(orders)):
                copies(at, 0, index, 0).wait()
        else:
            for wanted in range(2):
                copies(at, 0, 0, wanted).wait()

    def finish(at, tile):
        exchange(at).wait_recv()

        @pl.when(tile >= 2)
        def _():
            stored(at)

        own_ref[at] = (part(at, mine)[:] + got_ref[at]).reshape(own_ref.shape[1:])

        @pl.when(tile + 2 <= last)
        def _():
            pl.semaphore_signal(free_sem.at[at], **partner)

        if not orders:
            whole(at, tile).start()
        for index, order in enumerate(orders):
            if by_rows:
                same = bit(2 * tile, order[0]) == bit(me, order[0])
                for wanted, test in enumerate((jnp.logical_not(same), same)):
                    pl.when(test)(copies(at, tile, index, wanted).start)
            else:
                width = own_ref.shape[-1]

                @pl.when((tile >= edges[index] // width) & (tile < edges[index + 1] // width))
                def _():
                    for wanted in range(2):
                        copies(at, tile, index, wanted).start()

    @first_step()
    def _():
        barrier = pltpu.get_barrier_semaphore()
        pl.semaphore_signal(barrier, **partner)
        if not by_rows:
            for j in range(a_ref.shape[1] // LANES):
                refs[-1][lane_tile(j if orders else RING.index(j)), :] = a_ref[:, lane_tile(j)].T
        pl.semaphore_wait(barrier, 1)

    @pl.when(step >= 2)
    def _():
        exchange(slot).wait_send()

    total = dot_tn(a_ref[:], b_ref[:]) if by_rows else dot(refs[-1][:], b_ref[:])
    made_ref[slot] = total.reshape(made_ref.shape[1:])
    if has_tail:
        @pl.when(step == last)
        def _():
            end = own_ref.shape[-1] - LANES
            made_ref[slot, :, :, :, end:] += tail_ref[:].reshape(made_ref.shape[1:4] + (LANES,))

    @pl.when(step >= 2)
    def _():
        pl.semaphore_wait(free_sem.at[slot], 1)

    exchange(slot).start()

    @pl.when(step >= 1)
    def _():
        finish(1 - slot, step - 1)

    @pl.when(step == last)
    def _():
        finish(slot, step)
        for at in range(2):
            exchange(at).wait_send()
            stored(at)


def wgrad(a, b, orders, edges, number, after, tile=STEP, by_rows=False, tail=()):
    k, m = a.shape
    n = b.shape[1]
    r = m // (2 * CHIPS)
    shapes = [shaped((2, 2, r, hi - lo)) for lo, hi in zip(edges, edges[1:]) for _ in range(2)] or [shaped((CHIPS, r, n))]
    if by_rows:
        steps, block, own = CHIPS, (2, r, n), (r, n)
        in_specs = [pl.BlockSpec((k, 2 * r), lambda j: (0, j if orders else ring_chip(j))), held(b.shape)]
        got, scratch = own, []
    else:
        steps, block, own = n // tile, (CHIPS, 2, r, tile), ((2,) * len(GRID) if orders else (CHIPS,)) + (r, tile)
        in_specs = [held(a.shape), pl.BlockSpec((k, tile), lambda j: (0, j))] + [held(x.shape) for x in tail]
        got, scratch = (CHIPS, r, tile), [pltpu.VMEM((m, k), BF16)]
    dma = pltpu.SemaphoreType.DMA
    return call(functools.partial(wgrad_kernel, orders, edges, by_rows, len(tail)), after, (a, b) + tuple(tail), grid=(steps,),
                in_specs=in_specs, out_specs=[ANY] * len(shapes), out_shape=shapes,
                scratch_shapes=[pltpu.VMEM((2,) + block, F32), pltpu.VMEM((2,) + got, F32), pltpu.VMEM((2,) + own, F32),
                                dma((2,)), dma((2,)), pltpu.SemaphoreType.REGULAR((2,)), dma((2, max(2, len(orders))))] + scratch,
                flops=2 * k * m * n, partners=number)


def add_kernel(*refs):
    _, *refs = refs
    n = len(refs) // 3
    for at in range(n):
        refs[2 * n + at][:] = refs[2 * at][:] + refs[2 * at + 1][:]


def halves(me, items, level, after):
    args, in_specs, shapes, out_specs = [], [], [], []
    for order, kept, received in items:
        links = [link for link in GRID if link not in order[:level]]
        at = links.index(order[level])
        r, n = kept.shape[-2:]
        rest = (2,) * (len(links) - 1)
        for keep in range(2):
            def index(i, s, keep=keep, at=at, count=len(links), link=order[level]):
                lead = [i] * count
                lead[at] = bit(s[0], link) if keep else 1 - bit(s[0], link)
                return (*lead, 0, 0)

            args += [kept, received]
            in_specs += [pl.BlockSpec((None,) * len(links) + (r, n), index)] * 2
            shapes.append(shaped(rest + (r, n)))
            out_specs.append(pl.BlockSpec((None,) * len(rest) + (r, n), lambda i, s, count=len(rest): (i,) * count + (0, 0)))
    outs = call(add_kernel, after, args, prefetch=(me,), grid=(len(GRID) - level,), in_specs=in_specs, out_specs=out_specs,
                out_shape=shapes, flops=STEP * sum(x.size for x in shapes))
    return list(zip(outs[::2], outs[1::2]))


def add_columns(out_ref, refs):
    lo = 0
    for kept, received in zip(refs[::2], refs[1::2]):
        hi = lo + kept.shape[1]
        out_ref[:, lo:hi] = kept[:] + received[:]
        lo = hi


def join_kernel(counts, *refs):
    n = 2 * sum(counts)
    at = 0
    for out_ref, count in zip(refs[n:], counts):
        add_columns(out_ref, refs[at:at + 2 * count])
        at += 2 * count


def join(groups, after):
    args = [x for group in groups for pair in group for x in pair]
    shapes = [shaped((group[0][0].shape[0], sum(kept.shape[1] for kept, _ in group))) for group in groups]
    return call(functools.partial(join_kernel, [len(group) for group in groups]), after, args,
                in_specs=[held(x.shape) for x in args], out_specs=[whole_out(s.shape) for s in shapes],
                out_shape=shapes, flops=STEP * sum(s.size for s in shapes))


def finish_kernel(n_in, n_pix, n_pos, *refs):
    (wt_ref, pos_ref, *vec_refs), full_ref = refs[n_in:-1], refs[-1]
    add_columns(full_ref, refs[:n_in])
    wt_ref[:] = full_ref[:, :n_pix]
    pos_ref[:] = full_ref[:, n_pix:n_pix + n_pos]
    pos_ref[:, :1] = full_ref[:, VEC_ROW + CLS:VEC_ROW + CLS + 1]
    rows = full_ref[:, VEC_ROW - VEC_AT:VEC_ROW - VEC_AT + LANES].T
    at = VEC_AT
    for ref in vec_refs:
        for lo in range(0, ref.shape[1], HEAD):
            ref[:, lo:lo + HEAD] = rows[at:at + 1]
            at += 1


def finish_small(pairs, n_pix, n_pos, widths, after):
    args = [x for pair in pairs for x in pair]
    shapes = [shaped((HEAD, n_pix)), shaped((HEAD, n_pos))] + [shaped((1, w)) for w in widths]
    return call(functools.partial(finish_kernel, len(args), n_pix, n_pos), after, args, in_specs=[held(x.shape) for x in args],
                out_specs=[whole_out(s.shape) for s in shapes], out_shape=shapes,
                scratch_shapes=[pltpu.VMEM((HEAD, PACK), F32)], flops=PACK)


PARAM_NAMES = ('w_patch', 'b_patch', 'pos_table', 'cls_tok', 'lnp_g', 'lnp_b', 'ln1_g', 'ln1_b', 'w_qkv', 'b_qkv', 'w_out', 'b_out', 'ln2_g', 'ln2_b', 'w_fc', 'b_fc', 'w_proj', 'b_proj')
PACKED = tuple(PARAM_NAMES[i] for i in (1, 3, 4, 5, 6, 7, 11, 12, 13, 17, 9, 15))


def solution(mesh):
    n_dev = mesh.shape[MESH_AXIS]

    def across(value, link):
        return lax.ppermute(value, MESH_AXIS, [(i, i ^ (1 << LINKS.index(link))) for i in range(n_dev)])

    def compute(patches, keep, *rest):
        shard = dict(zip(PARAM_NAMES, rest[:-1]))
        d, d_mlp = shard['w_out'].shape[1], shard['w_fc'].shape[1]
        n_pix, n_pos = shard['w_patch'].shape[0], shard['pos_table'].shape[0]
        scale = shard['w_qkv'].shape[-1] ** -0.5
        me = lax.axis_index(MESH_AXIS).reshape(1)
        by_token = lambda x: x.transpose(1, 0, 2)

        def whole(value):
            return lax.all_gather(value, MESH_AXIS, tiled=True)

        w_qkv = shard['w_qkv'].astype(BF16).reshape(HEAD, -1)
        first = whole(pack_small(w_qkv, shard['w_patch'].T, shard['pos_table'].T, [shard[name][None] for name in PACKED]))
        w_fo = whole(jnp.concatenate([shard['w_fc'].astype(BF16), shard['w_out'].astype(BF16)], axis=1))
        w_proj = whole(shard['w_proj'].astype(BF16))

        zo, g = pick_rows(keep, by_token(patches), by_token(rest[-1]))
        hat, a, stats, vecs, b_qkv, b_fc = embed(zo, first, d_mlp)
        qkv, ctx = attend(a, first, b_qkv, scale)
        m, c, act, pre = mlp_up(ctx, hat, w_fo, vecs, b_fc)

        def cut(outs, orders):
            return [(order, kept, across(sent, order[0])) for order, sent, kept in zip(orders, outs[::2], outs[1::2])]

        def halve(items, level, after):
            pairs = halves(me, items, level, after)
            return [(order, kept, across(sent, order[level])) for (order, _, _), (sent, kept) in zip(items, pairs)]

        def over_chips(made):
            rings = [[2 * chip + core for chip in RING] for core in range(2)]
            return lax.psum_scatter(made[0].reshape(-1, made[0].shape[-1]), MESH_AXIS, axis_index_groups=rings, tiled=True)

        def ends(items):
            return [(kept, received) for _, kept, received in items]

        two = ORDERS[:2]
        made = wgrad(act, g, (), (), 0, (), by_rows=True)
        g_proj = over_chips(made)
        h1 = mlp_down(act, m, w_proj, vecs, made)
        d_pre, d_mid, d_mid_b, d_ctx, sums_m, sum_fc = mlp_grad(g, pre, m, w_proj, w_fo, vecs, (h1,))
        made = wgrad(c, d_pre, (), (), 1, ())
        g_fc = over_chips(made)
        made = wgrad(ctx, d_mid_b, (), (), 2, made)
        g_out = over_chips(made)
        d_qkv, sum_qkv = attend_grad(qkv, d_ctx, scale, made)
        outs = wgrad(a, d_qkv, ORDERS, (0, d, 2 * d, 3 * d), 3, ())
        qkv = cut(outs, ORDERS)
        d_emb, sums_e = embed_grad(d_qkv, d_mid, hat, stats, first, vecs, (outs[1],))
        qkv = halve(qkv, 1, (sums_e,))
        tail = vector_tail(sums_e, sums_m, sum_qkv, sum_fc)
        outs = wgrad(d_emb, zo, two, (0, PACK // 2, PACK), 4, (qkv[0][1],), tail=(tail,))
        small = cut(outs, two)
        qkv = halve(qkv, 2, (outs[1],))
        small = halve(small, 1, (qkv[0][1],))
        g_qkv, = join([ends(qkv)], (small[0][1],))
        small = halve(small, 2, (g_qkv,))
        done = finish_small(ends(small), n_pix, n_pos, [shard[name].shape[0] for name in PACKED], (g_qkv,))

        grads = dict(w_patch=done[0].T, pos_table=done[1].T, w_qkv=g_qkv.reshape(shard['w_qkv'].shape), w_out=g_out, w_fc=g_fc, w_proj=g_proj)
        grads.update({name: value.reshape(-1) for name, value in zip(PACKED, done[2:])})
        return (by_token(h1),) + tuple(grads[name] for name in PARAM_NAMES)

    batch_spec = P(MESH_AXIS)
    param_specs = tuple(P(None, MESH_AXIS) if name in ('w_patch', 'pos_table') else batch_spec for name in PARAM_NAMES)
    return jax.shard_map(compute, mesh=mesh, in_specs=(batch_spec, batch_spec) + param_specs + (batch_spec,), out_specs=(batch_spec,) + param_specs, check_vma=False)
```

```python
import functools

import jax
import jax.numpy as jnp
from jax import lax
from jax.experimental import pallas as pl
from jax.experimental.pallas import tpu as pltpu
from jax.sharding import PartitionSpec as P


F32, BF16, I32 = jnp.float32, jnp.bfloat16, jnp.int32
LN_EPS = 1e-5
INV_SQRT2 = 0.7071067811865476
INV_SQRT_2PI = 0.3989422804014327
LOG2E = 1.4426950408889634
MASKED = -1e30
SUBLANES, LANES, HEAD = 8, 128, 64
TOK, FEW, MANY = 50, 4, 8
ROWS, GROWS = FEW * TOK, MANY * TOK
WIN = 112
STARTS = (0, ROWS - WIN)
EDGE = 96
PACK, VEC_ROW = 1024, 976
VEC_AT = VEC_ROW % LANES
N_VEC, VEC_ROWS = 10, 32
B_PATCH, CLS, LNP_G, LNP_B, LN1_G, LN1_B, B_OUT, LN2_G, LN2_B, B_PROJ = range(N_VEC)
STEP = 512
ALL_VMEM = 67043328
ANY = pl.BlockSpec(memory_space=pl.ANY)


def product(dims, left, right):
    return lax.dot_general(left, right, ((dims[:1], dims[1:]), ((), ())), preferred_element_type=F32)


dot = functools.partial(product, (1, 0))
dot_nt = functools.partial(product, (1, 1))
dot_tn = functools.partial(product, (0, 0))


def col_sum(x):
    return jnp.sum(x, axis=0, keepdims=True)


def col_max(x):
    return jnp.max(x, axis=0, keepdims=True)


def row_mean(x):
    return jnp.mean(x, axis=1, keepdims=True)


def row(ref, at):
    return ref[at:at + 1, :]


def iota(shape, axis):
    return lax.broadcasted_iota(I32, shape, axis)


def one_hot(test):
    return test.astype(F32).astype(BF16)


def origin(shape, *_):
    return (0,) * len(shape)


def held(shape):
    return pl.BlockSpec(shape, functools.partial(origin, shape), pipeline_mode=pl.Buffered(1))


def held_cols(n_rows, n_cols, at):
    return pl.BlockSpec((n_rows, n_cols), lambda *_: (0, at // n_cols), pipeline_mode=pl.Buffered(1))


def whole_out(shape):
    return pl.BlockSpec(shape, functools.partial(origin, shape))


def rows_spec(n_rows, width):
    return pl.BlockSpec((n_rows, width), lambda i, *_: (i, 0))


def this_block(n_rows, width, n):
    return pl.BlockSpec((n_rows, width), lambda i: (jnp.minimum(i, n - 1), 0))


def last_block(n_rows, width):
    return pl.BlockSpec((n_rows, width), lambda i: (jnp.maximum(i - 1, 0), 0))


def shaped(shape, dtype=F32):
    return jax.ShapeDtypeStruct(shape, dtype)


def call(kernel, after, args, *, prefetch=(), grid=(1,), in_specs, out_specs, out_shape, scratch_shapes=(), flops, n_bytes=0, partners=None):
    n_in, n_after = len(prefetch) + len(args), len(after)

    def body(*refs):
        return kernel(*refs[:n_in], *refs[n_in + n_after:])

    return pl.pallas_call(
        body,
        grid_spec=pltpu.PrefetchScalarGridSpec(
            num_scalar_prefetch=len(prefetch), grid=grid, in_specs=list(in_specs) + [ANY] * n_after,
            out_specs=out_specs, scratch_shapes=list(scratch_shapes)),
        out_shape=out_shape,
        compiler_params=pltpu.CompilerParams(
            dimension_semantics=(pltpu.ARBITRARY,) * len(grid), vmem_limit_bytes=ALL_VMEM,
            collective_id=partners, has_side_effects=partners is not None),
        cost_estimate=pl.CostEstimate(flops=int(flops), bytes_accessed=int(n_bytes), transcendentals=0),
    )(*prefetch, *args, *after)


def first_step():
    return pl.when(pl.program_id(0) == 0)


def clear(*refs):
    for ref in refs:
        ref[:] = jnp.zeros_like(ref)


def normalize(x):
    centered = x - row_mean(x)
    inv = lax.rsqrt(row_mean(centered * centered) + LN_EPS)
    return centered * inv, inv


def norm_grad(d_out, x_hat, inv, gain):
    d_hat = d_out * gain
    return inv * (d_hat - row_mean(d_hat) - x_hat * row_mean(d_hat * x_hat))


def image_of(at, n_img=FEW):
    return sum((at >= j * TOK).astype(I32) for j in range(1, n_img))


def is_class(n_rows):
    at = iota((n_rows, 1), 0)
    return at == TOK * image_of(at, n_rows // TOK)


def pack_kernel(wq_ref, wt_ref, pt_ref, *refs):
    *vec_refs, whole_ref, rows_ref, pos_ref = refs
    n_pix, n_pos, n_qkv = wt_ref.shape[1], pt_ref.shape[1], wq_ref.shape[1]
    whole_ref[:, :n_qkv] = wq_ref[:]
    out_ref = whole_ref.at[:, n_qkv:]
    out_ref[:, :n_pix] = wt_ref[:].astype(BF16)
    out_ref[:, n_pix:n_pix + LANES] = pt_ref[:, :LANES].astype(BF16)
    clear(rows_ref, pos_ref)
    pos_ref[:, :n_pos - LANES] = pt_ref[:, LANES:]
    at = VEC_AT
    for ref in vec_refs:
        for lo in range(0, ref.shape[1], HEAD):
            rows_ref[at:at + 1, :HEAD] = ref[:, lo:lo + HEAD]
            at += 1
    out_ref[:, n_pix + LANES:] = (pos_ref[:] + rows_ref[:].T[:HEAD]).astype(BF16)


def pack_small(wq, wt, pt, vecs):
    args = [wq, wt, pt] + vecs
    shape = (HEAD, wq.shape[1] + PACK)
    return call(pack_kernel, (), args, in_specs=[held(x.shape) for x in args], out_specs=whole_out(shape), out_shape=shaped(shape, BF16),
                scratch_shapes=[pltpu.VMEM((LANES, LANES), F32), pltpu.VMEM((HEAD, LANES), F32)], flops=PACK)


def pick_kernel(keep_ref, patches_ref, g_ref, zo_ref, gi_ref, pad_ref):
    n_patch, _, n_pix = patches_ref.shape
    clear(pad_ref)
    pad_ref[:, :TOK - 1] = keep_ref[:].astype(F32)
    image, lane = iota(pad_ref.shape, 0), iota(pad_ref.shape, 1)
    spread = pad_ref[:]
    for b in range(MANY):
        spread = jnp.where(image == b, pltpu.roll(pad_ref[:], TOK * b + 1, 1), spread)
    own = (lane > TOK * image) & (lane < TOK * image + TOK)
    token = col_sum(jnp.where(own, spread + 1.0, 0.0))
    source = col_sum(jnp.where(own, spread * MANY + image.astype(F32), 0.0))
    source = jnp.where(token > 0.0, source, -1.0)
    cols = jnp.where(image == 0, source, token).T[:GROWS].astype(I32)
    source, token = cols[:, :1], cols[:, 1:2]
    pick = one_hot(iota((GROWS, MANY * n_patch), 1) == source)
    zo_ref[:, :n_pix] = dot(pick, patches_ref.reshape(MANY * n_patch, n_pix)[:]).astype(BF16)
    zo_ref[:, n_pix:] = one_hot(iota((GROWS, PACK - n_pix), 1) == token)
    to, source = iota((GROWS, GROWS), 0), iota((GROWS, GROWS), 1)
    move = one_hot(to == lax.rem(source, MANY) * TOK + lax.div(source, MANY))
    gi_ref[:] = dot(move, g_ref.reshape(GROWS, g_ref.shape[2])[:]).astype(BF16)


def pick_rows(keep, patches_t, g_t):
    _, n_img, _ = patches_t.shape
    d = g_t.shape[2]
    n_tok = n_img * TOK
    by_image = lambda x: pl.BlockSpec((x.shape[0], MANY, x.shape[2]), lambda i: (0, i, 0))
    return call(pick_kernel, (), (keep, patches_t, g_t), grid=(n_img // MANY,),
                in_specs=[rows_spec(MANY, TOK - 1), by_image(patches_t), by_image(g_t)],
                out_specs=[rows_spec(GROWS, PACK), rows_spec(GROWS, d)], out_shape=[shaped((n_tok, PACK), BF16), shaped((n_tok, d), BF16)],
                scratch_shapes=[pltpu.VMEM((MANY, STEP), F32)], flops=STEP * patches_t.size)


def embed_kernel(zo_ref, wt_ref, hat_ref, a_ref, stat_ref, vec_ref, bq_ref, bf_ref, next_ref, now_ref):
    @first_step()
    def _():
        base = VEC_ROW - VEC_AT
        vec_ref[:] = wt_ref[:, base:base + LANES].astype(F32).T[VEC_AT:VEC_AT + VEC_ROWS]
        at = N_VEC
        for ref in (bq_ref, bf_ref):
            n = ref.shape[1] // vec_ref.shape[1]
            chunk = lambda q: row(vec_ref, at + q % n)[:, q // n * HEAD:(q // n + 1) * HEAD]
            for lo in range(0, ref.shape[1], LANES):
                ref[:, lo:lo + LANES] = jnp.concatenate([chunk(lo // HEAD), chunk(lo // HEAD + 1)], axis=1)
            at += n

    now_ref[:] = next_ref[:]
    next_ref[:] = dot_nt(zo_ref[:], wt_ref[:]) + jnp.where(is_class(GROWS), row(vec_ref, CLS), row(vec_ref, B_PATCH))
    hat, inv = normalize(now_ref[:])
    hat_ref[:] = hat
    h0 = hat * row(vec_ref, LNP_G) + row(vec_ref, LNP_B)
    mean1 = row_mean(h0)
    centered = h0 - mean1
    inv1 = lax.rsqrt(row_mean(centered * centered) + LN_EPS)
    a_ref[:] = (centered * inv1 * row(vec_ref, LN1_G) + row(vec_ref, LN1_B)).astype(BF16)
    lane = iota(stat_ref.shape, 1)
    stat_ref[:] = jnp.where(lane == 0, inv, jnp.where(lane == 1, inv1, mean1))


def embed(zo, first, d_mlp):
    n_tok = zo.shape[0]
    d, width = first.shape
    n = n_tok // GROWS
    outs = ((VEC_ROWS, d), (1, width - PACK), (1, d_mlp))
    return call(embed_kernel, (), (zo, first), grid=(n + 1,),
                in_specs=[this_block(GROWS, PACK, n), held_cols(d, PACK, width - PACK)],
                out_specs=[last_block(GROWS, d), last_block(GROWS, d), last_block(GROWS, LANES)] + [whole_out(s) for s in outs],
                out_shape=[shaped((n_tok, d)), shaped((n_tok, d), BF16), shaped((n_tok, LANES))] + [shaped(s) for s in outs],
                scratch_shapes=[pltpu.VMEM((GROWS, d), F32)] * 2, flops=2 * zo.size * d)


def window_mask(start):
    key, query = (iota((WIN, 2 * WIN), axis) for axis in (0, 1))
    return jnp.where(image_of(key + start) == image_of(lax.rem(query, WIN) + start), 0.0, MASKED)


def set_masks(mask_ref):
    for i, start in enumerate(STARTS):
        mask_ref[i] = window_mask(start)


def split_heads(x):
    first = iota(x.shape, 1) < HEAD
    zero = jnp.zeros_like(x)
    return jnp.concatenate([jnp.where(first, x, zero), jnp.where(first, zero, x)], axis=0)


def join_heads(x):
    return jnp.where(iota((WIN, LANES), 1) < HEAD, x[:WIN], x[WIN:])


def join_windows(lo, hi):
    at = EDGE + SUBLANES
    shift = STARTS[1]
    edge = jnp.where(iota((SUBLANES, LANES), 0) < 2 * TOK - EDGE, lo[EDGE:at], hi[EDGE - shift:at - shift])
    return jnp.concatenate([lo[:EDGE], edge, hi[at - shift:]], axis=0)


def weights_t(logits, mask, scale):
    masked = logits + mask
    e = jnp.exp2((masked - col_max(masked)) * (scale * LOG2E))
    return e * (1.0 / col_sum(e))


def lane_tile(at):
    return slice(at * LANES, (at + 1) * LANES)


def reader(ref):
    return lambda at, i: ref[STARTS[i]:STARTS[i] + WIN, lane_tile(at)]


def every_unit(n_tiles):
    return [(pair, i) for pair in range(n_tiles) for i in range(len(STARTS))]


def window_scratch():
    return pltpu.VMEM((len(STARTS), WIN, 2 * WIN), F32)


def attend_kernel(scale, a_ref, w_ref, b_ref, qkv_ref, o_ref, mask_ref):
    @first_step()
    def _():
        set_masks(mask_ref)

    n_tiles = o_ref.shape[1] // LANES
    a = a_ref[:]
    for lo in range(0, b_ref.shape[1], STEP):
        cols = slice(lo, lo + STEP)
        qkv_ref[:, cols] = (dot(a, w_ref[:, cols]) + b_ref[:, cols]).astype(BF16)
    read, units = reader(qkv_ref), every_unit(n_tiles)
    logits = [dot_nt(read(n_tiles + pair, i), split_heads(read(pair, i))) for pair, i in units]
    probs = [weights_t(x, mask_ref[i], scale).astype(BF16) for x, (_, i) in zip(logits, units)]
    outs = [join_heads(dot_tn(p, read(2 * n_tiles + pair, i))) for p, (pair, i) in zip(probs, units)]
    for lo, hi, (pair, _) in zip(outs[::2], outs[1::2], units[::2]):
        o_ref[:, lane_tile(pair)] = join_windows(lo, hi).astype(BF16)


def attend(a, first, b_qkv, scale):
    n_tok, d = a.shape
    width = b_qkv.shape[1]
    return call(functools.partial(attend_kernel, scale), (), (a, first, b_qkv), grid=(n_tok // ROWS,),
                in_specs=[rows_spec(ROWS, d), held_cols(d, width, 0), held(b_qkv.shape)],
                out_specs=[rows_spec(ROWS, width), rows_spec(ROWS, d)],
                out_shape=[shaped((n_tok, width), BF16), shaped((n_tok, d), BF16)],
                scratch_shapes=[window_scratch()], flops=4 * a.size * width)


def attend_grad_kernel(scale, qkv_ref, dctx_ref, dqkv_ref, bsum_ref, mask_ref):
    @first_step()
    def _():
        set_masks(mask_ref)
        clear(bsum_ref)

    n_tiles = dctx_ref.shape[1] // LANES
    read, read_grad, units = reader(qkv_ref), reader(dctx_ref), every_unit(n_tiles)
    q2 = [split_heads(read(pair, i)) for pair, i in units]
    do2 = [split_heads(read_grad(pair, i)) for pair, i in units]
    logits = [dot_nt(read(n_tiles + pair, i), q) for q, (pair, i) in zip(q2, units)]
    dp = [dot_nt(read(2 * n_tiles + pair, i), do) for do, (pair, i) in zip(do2, units)]
    logits = [x * scale + mask_ref[i] for x, (_, i) in zip(logits, units)]
    e = [jnp.exp2((x - col_max(x)) * LOG2E) for x in logits]
    p = [x * (1.0 / col_sum(x)) for x in e]
    dv = [dot(x.astype(BF16), do) for x, do in zip(p, do2)]
    ds = [(x * (y - col_sum(x * y)) * scale).astype(BF16) for x, y in zip(p, dp)]
    dk = [dot(x, q) for x, q in zip(ds, q2)]
    dq = [join_heads(dot_tn(x, read(n_tiles + pair, i))) for x, (pair, i) in zip(ds, units)]
    for at, (pair, _) in enumerate(units[::2]):
        for part, grads in enumerate((dq, dk, dv)):
            both = join_windows(grads[2 * at], grads[2 * at + 1])
            cols = lane_tile(part * n_tiles + pair)
            dqkv_ref[:, cols] = both.astype(BF16)
            bsum_ref[:, cols] += col_sum(both)


def attend_grad(qkv, d_ctx, scale, after):
    n_tok, width = qkv.shape
    return call(functools.partial(attend_grad_kernel, scale), after, (qkv, d_ctx), grid=(n_tok // ROWS,),
                in_specs=[rows_spec(ROWS, width), rows_spec(ROWS, d_ctx.shape[1])], out_specs=[rows_spec(ROWS, width), whole_out((1, width))],
                out_shape=[shaped((n_tok, width), BF16), shaped((1, width))],
                scratch_shapes=[window_scratch()], flops=3 * d_ctx.size * width)


def erf_cdf(u):
    return 0.5 + 0.5 * lax.erf(u * INV_SQRT2)


def mlp_up_kernel(o_ref, hat_ref, wo_ref, wf_ref, vec_ref, bf_ref, m_ref, c_ref, act_ref, pre_ref, next_ref, now_ref):
    now_ref[:] = next_ref[:]
    m = hat_ref[:] * row(vec_ref, LNP_G) + row(vec_ref, LNP_B) + dot(o_ref[:], wo_ref[:]) + row(vec_ref, B_OUT)
    m_ref[:] = m
    hat2, _ = normalize(m)
    next_c = (hat2 * row(vec_ref, LN2_G) + row(vec_ref, LN2_B)).astype(BF16)
    c_ref[:] = next_c
    c = now_ref[:]
    for lo in range(0, wf_ref.shape[1], STEP):
        cols = slice(lo, lo + STEP)
        u = dot(c, wf_ref[:, cols]) + bf_ref[:, cols]
        pre_ref[:, cols] = u
        act_ref[:, cols] = (u * erf_cdf(u)).astype(BF16)
    next_ref[:] = next_c


def mlp_up(o, hat, w_fo, vecs, b_fc):
    n_tok, d = o.shape
    f = b_fc.shape[1]
    n = n_tok // ROWS
    return call(mlp_up_kernel, (), (o, hat, w_fo, w_fo, vecs, b_fc), grid=(n + 1,),
                in_specs=[this_block(ROWS, d, n), this_block(ROWS, d, n), held_cols(d, d, f), held_cols(d, f, 0), held(vecs.shape), held(b_fc.shape)],
                out_specs=[this_block(ROWS, d, n), this_block(ROWS, d, n), last_block(ROWS, f), last_block(ROWS, f)],
                out_shape=[shaped((n_tok, d)), shaped((n_tok, d), BF16), shaped((n_tok, f), BF16), shaped((n_tok, f))],
                scratch_shapes=[pltpu.VMEM((ROWS, d), BF16)] * 2, flops=3 * o.size * f)


def mlp_down_kernel(act_ref, m_ref, w_ref, vec_ref, h1_ref):
    h1 = (m_ref[:] + dot(act_ref[:], w_ref[:]) + row(vec_ref, B_PROJ)).astype(BF16)
    to, source = iota((GROWS, GROWS), 0), iota((GROWS, GROWS), 1)
    move = one_hot(source == lax.rem(to, MANY) * TOK + lax.div(to, MANY))
    h1_ref.reshape(GROWS, h1_ref.shape[2])[:] = dot(move, h1).astype(BF16)


def mlp_down(act, m, w_proj, vecs, after):
    n_tok, f = act.shape
    d = m.shape[1]
    return call(mlp_down_kernel, after, (act, m, w_proj, vecs), grid=(n_tok // GROWS,),
                in_specs=[rows_spec(GROWS, f), rows_spec(GROWS, d), held(w_proj.shape), held(vecs.shape)],
                out_specs=pl.BlockSpec((TOK, MANY, d), lambda i: (0, i, 0)),
                out_shape=shaped((TOK, n_tok // TOK, d), BF16), flops=2 * m.size * f)


def mlp_grad_kernel(g_ref, pre_ref, m_ref, wp_ref, wf_ref, wo_ref, vec_ref, dpre_ref, dmid_ref, dmidb_ref, dctx_ref, vsum_ref, bfc_ref):
    @first_step()
    def _():
        clear(vsum_ref, bfc_ref)

    g = g_ref[:]
    step = 2 * STEP
    d_c = jnp.zeros(m_ref.shape, F32)
    cuts = [slice(lo, lo + step) for lo in range(0, wp_ref.shape[0], step)]
    acts, pres = dict(), dict()
    n = len(cuts)
    for tick in range(n + 2):
        if tick < n:
            acts[tick] = dot_nt(g, wp_ref[cuts[tick], :])
        if 0 <= tick - 1 < n:
            cols = cuts[tick - 1]
            u = pre_ref[:, cols]
            w = u * INV_SQRT2
            d_pre = acts.pop(tick - 1) * (0.5 + 0.5 * lax.erf(w) + u * (jnp.exp2((w * w) * (-LOG2E)) * INV_SQRT_2PI))
            bfc_ref[:, cols] += col_sum(d_pre)
            pres[tick - 1] = d_pre.astype(BF16)
            dpre_ref[:, cols] = pres[tick - 1]
        if tick >= 2:
            d_c = d_c + dot_nt(pres.pop(tick - 2), wf_ref[:, cuts[tick - 2]])
    hat2, inv2 = normalize(m_ref[:])
    g_f = g.astype(F32)
    d_mid = norm_grad(d_c, hat2, inv2, row(vec_ref, LN2_G)) + g_f
    dmid_ref[:] = d_mid
    d_mid_b = d_mid.astype(BF16)
    dmidb_ref[:] = d_mid_b
    dctx_ref[:] = dot_nt(d_mid_b, wo_ref[:]).astype(BF16)
    for at, part in enumerate((d_mid, d_c * hat2, d_c, g_f)):
        vsum_ref[at:at + 1, :] += col_sum(part)


def mlp_grad(g, pre, m, w_proj, w_fo, vecs, after):
    n_tok, d = g.shape
    f = pre.shape[1]
    wide, narrow = rows_spec(GROWS, f), rows_spec(GROWS, d)
    return call(mlp_grad_kernel, after, (g, pre, m, w_proj, w_fo, w_fo, vecs), grid=(n_tok // GROWS,),
                in_specs=[narrow, wide, narrow, held(w_proj.shape), held_cols(d, f, 0), held_cols(d, d, f), held(vecs.shape)],
                out_specs=[wide, narrow, narrow, narrow, whole_out((SUBLANES, d)), whole_out((1, f))],
                out_shape=[shaped((n_tok, f), BF16), shaped((n_tok, d)), shaped((n_tok, d), BF16), shaped((n_tok, d), BF16),
                           shaped((SUBLANES, d)), shaped((1, f))],
                flops=5 * g.size * f)


CUTS = (0, 104, 208, 304, GROWS)


def embed_grad_kernel(dqkv_ref, dmid_ref, hat_ref, stat_ref, w_ref, vec_ref, demb_ref, vsum_ref, next_ref, now_ref, dx_ref):
    step = pl.program_id(0)

    @first_step()
    def _():
        clear(vsum_ref)

    now_ref[:] = next_ref[:]
    width = now_ref.shape[1] // (len(CUTS) - 1)
    sums = []
    for j, (lo, hi) in enumerate(zip(CUTS, CUTS[1:])):
        cols, rows = slice(j * width, (j + 1) * width), slice(lo, hi)
        next_ref[:, cols] = dot_nt(dqkv_ref[:], w_ref[cols, :])
        d_a, hat_p = now_ref[rows, :], hat_ref[rows, :]
        inv_p, inv1, mean1 = (stat_ref[rows, k:k + 1] for k in range(3))
        hat1 = (hat_p * row(vec_ref, LNP_G) + row(vec_ref, LNP_B) - mean1) * inv1
        d_zero = norm_grad(d_a, hat1, inv1, row(vec_ref, LN1_G)) + dmid_ref[rows, :]
        d_x = norm_grad(d_zero, hat_p, inv_p, row(vec_ref, LNP_G))
        demb_ref[rows, :] = d_x.astype(BF16)
        dx_ref[rows, :] = d_x
        sums.append([col_sum(part) for part in (d_x, d_zero * hat_p, d_zero, d_a * hat1, d_a)])
    d_all, *others = (sum(parts) for parts in zip(*sums))
    d_cls = sum(row(dx_ref, at) for at in range(0, GROWS, TOK))
    for at, part in enumerate([d_all - d_cls, d_cls] + others):
        vsum_ref[at:at + 1, :] += jnp.where(step > 0, part, 0.0)


def embed_grad(dqkv, d_mid, hat, stats, first, vecs, after):
    n_tok, d = d_mid.shape
    width = dqkv.shape[1]
    n = n_tok // GROWS
    return call(embed_grad_kernel, after, (dqkv, d_mid, hat, stats, first, vecs), grid=(n + 1,),
                in_specs=[this_block(GROWS, width, n), last_block(GROWS, d), last_block(GROWS, d), last_block(GROWS, LANES),
                          held_cols(d, width, 0), held(vecs.shape)],
                out_specs=[last_block(GROWS, d), whole_out((SUBLANES, d))], out_shape=[shaped((n_tok, d), BF16), shaped((SUBLANES, d))],
                scratch_shapes=[pltpu.VMEM((GROWS, d), F32)] * 3, flops=3 * d_mid.size * width)


def tail_kernel(se_ref, sm_ref, sq_ref, sf_ref, out_ref, rows_ref):
    d = se_ref.shape[1]
    clear(rows_ref)
    at, cut = VEC_AT, VEC_AT + B_OUT
    rows_ref[at:cut, :] = se_ref[:B_OUT, :]
    at += N_VEC
    rows_ref[cut:at, :] = sm_ref[:N_VEC - B_OUT, :]
    for ref in (sq_ref, sf_ref):
        n = ref.shape[1] // d
        for r in range(n):
            chunk = lambda q: ref[:, (n * q + r) * HEAD:(n * q + r + 1) * HEAD]
            for j in range(d // LANES):
                rows_ref[at:at + 1, lane_tile(j)] = jnp.concatenate([chunk(2 * j), chunk(2 * j + 1)], axis=1)
            at += 1
    for j in range(d // LANES):
        out_ref[lane_tile(j)] = rows_ref[:, lane_tile(j)].T


def vector_tail(*args):
    d = args[0].shape[1]
    return call(tail_kernel, (), args, in_specs=[held(x.shape) for x in args], out_specs=whole_out((d, LANES)), out_shape=shaped((d, LANES)),
                scratch_shapes=[pltpu.VMEM((LANES, d), F32)], flops=d)


MESH_AXIS = 'fsdp'
LINKS = ('core', 'x', 'y', 'z')
GRID = LINKS[:0:-1]
CHIPS = 1 << len(GRID)
ORDERS = tuple(LINKS[k:] + LINKS[1:k] for k in range(1, len(LINKS)))
RING = [at ^ (at >> 1) for at in range(CHIPS)]


def bit(at, link):
    return lax.rem(lax.div(at, 1 << LINKS.index(link)), 2)


def device(at):
    return dict(device_id=(at,), device_id_type=pl.DeviceIdType.MESH)


def ring_chip(at):
    half, quarter = lax.div(at, 2), lax.div(at, 4)
    return 4 * quarter + 2 * lax.rem(half + quarter, 2) + lax.rem(at + half, 2)


def wgrad_kernel(orders, edges, by_rows, a_ref, b_ref, *refs):
    n_out = 2 * len(orders) or 1
    outs, refs = refs[:n_out], refs[n_out:]
    made_ref, got_ref, own_ref, send_sem, got_sem, free_sem, out_sem = refs[:7]
    step, last = pl.program_id(0), pl.num_programs(0) - 1
    slot = lax.rem(step, 2)
    me = lax.axis_index(MESH_AXIS)
    mine = bit(me, LINKS[0])
    partner = device(me + 1 - 2 * mine)

    def part(at, core):
        return made_ref.at[at, core] if by_rows else made_ref.at[at, :, core]

    def exchange(at):
        return pltpu.make_async_remote_copy(part(at, 1 - mine), got_ref.at[at], send_sem.at[at], got_sem.at[at], **partner)

    def whole(at, tile):
        width = own_ref.shape[-1]
        out = outs[0].at[tile] if by_rows else outs[0].at[:, :, pl.ds(pl.multiple_of(tile * width, width), width)]
        return pltpu.make_async_copy(own_ref.at[at], out, out_sem.at[at, 0])

    def copies(at, tile, order_index, wanted):
        link = orders[order_index][0]
        out = outs[2 * order_index + wanted]
        sem = out_sem.at[at, order_index if by_rows else wanted]
        if by_rows:
            rest = [bit(2 * tile, other) for other in GRID if other != link]
            lo, hi = edges[order_index:order_index + 2]
            return pltpu.make_async_copy(own_ref.at[at, :, pl.ds(lo, hi - lo)], out.at[rest[0], rest[1]], sem)
        width = own_ref.shape[-1]
        cols = pl.ds(pl.multiple_of((tile - edges[order_index] // width) * width, width), width)
        side = bit(me, link) if wanted else 1 - bit(me, link)
        return pltpu.make_async_copy(own_ref.at[(at,) + (slice(None),) * GRID.index(link) + (side,)], out.at[:, :, :, cols], sem)

    def stored(at):
        if not orders:
            whole(at, 0).wait()
        elif by_rows:
            for index in range(len(orders)):
                copies(at, 0, index, 0).wait()
        else:
            for wanted in range(2):
                copies(at, 0, 0, wanted).wait()

    def finish(at, tile):
        exchange(at).wait_recv()

        @pl.when(tile >= 2)
        def _():
            stored(at)

        own_ref[at] = (part(at, mine)[:] + got_ref[at]).reshape(own_ref.shape[1:])

        @pl.when(tile + 2 <= last)
        def _():
            pl.semaphore_signal(free_sem.at[at], **partner)

        if not orders:
            whole(at, tile).start()
        for index, order in enumerate(orders):
            if by_rows:
                same = bit(2 * tile, order[0]) == bit(me, order[0])
                for wanted, test in enumerate((jnp.logical_not(same), same)):
                    pl.when(test)(copies(at, tile, index, wanted).start)
            else:
                width = own_ref.shape[-1]

                @pl.when((tile >= edges[index] // width) & (tile < edges[index + 1] // width))
                def _():
                    for wanted in range(2):
                        copies(at, tile, index, wanted).start()

    @first_step()
    def _():
        barrier = pltpu.get_barrier_semaphore()
        pl.semaphore_signal(barrier, **partner)
        if not by_rows:
            for j in range(a_ref.shape[1] // LANES):
                refs[-1][lane_tile(j if orders else RING.index(j)), :] = a_ref[:, lane_tile(j)].T
        pl.semaphore_wait(barrier, 1)

    @pl.when(step >= 2)
    def _():
        exchange(slot).wait_send()

    total = dot_tn(a_ref[:], b_ref[:]) if by_rows else dot(refs[-1][:], b_ref[:])
    made_ref[slot] = total.reshape(made_ref.shape[1:])

    @pl.when(step >= 2)
    def _():
        pl.semaphore_wait(free_sem.at[slot], 1)

    exchange(slot).start()

    @pl.when(step >= 1)
    def _():
        finish(1 - slot, step - 1)

    @pl.when(step == last)
    def _():
        finish(slot, step)
        for at in range(2):
            exchange(at).wait_send()
            stored(at)


def wgrad(a, b, orders, edges, number, after, tile=STEP, by_rows=False):
    k, m = a.shape
    n = b.shape[1]
    r = m // (2 * CHIPS)
    shapes = [shaped((2, 2, r, hi - lo)) for lo, hi in zip(edges, edges[1:]) for _ in range(2)] or [shaped((CHIPS, r, n))]
    if by_rows:
        steps, block, own = CHIPS, (2, r, n), (r, n)
        in_specs = [pl.BlockSpec((k, 2 * r), lambda j: (0, j if orders else ring_chip(j))), held(b.shape)]
        got, scratch = own, []
    else:
        steps, block, own = n // tile, (CHIPS, 2, r, tile), ((2,) * len(GRID) if orders else (CHIPS,)) + (r, tile)
        in_specs = [held(a.shape), pl.BlockSpec((k, tile), lambda j: (0, j))]
        got, scratch = (CHIPS, r, tile), [pltpu.VMEM((m, k), BF16)]
    dma = pltpu.SemaphoreType.DMA
    return call(functools.partial(wgrad_kernel, orders, edges, by_rows), after, (a, b), grid=(steps,),
                in_specs=in_specs, out_specs=[ANY] * len(shapes), out_shape=shapes,
                scratch_shapes=[pltpu.VMEM((2,) + block, F32), pltpu.VMEM((2,) + got, F32), pltpu.VMEM((2,) + own, F32),
                                dma((2,)), dma((2,)), pltpu.SemaphoreType.REGULAR((2,)), dma((2, max(2, len(orders))))] + scratch,
                flops=2 * k * m * n, partners=number)


def add_kernel(*refs):
    _, *refs = refs
    n = len(refs) // 3
    for at in range(n):
        refs[2 * n + at][:] = refs[2 * at][:] + refs[2 * at + 1][:]


def halves(me, items, level, after):
    args, in_specs, shapes, out_specs = [], [], [], []
    for order, kept, received in items:
        links = [link for link in GRID if link not in order[:level]]
        at = links.index(order[level])
        r, n = kept.shape[-2:]
        rest = (2,) * (len(links) - 1)
        for keep in range(2):
            def index(i, s, keep=keep, at=at, count=len(links), link=order[level]):
                lead = [i] * count
                lead[at] = bit(s[0], link) if keep else 1 - bit(s[0], link)
                return (*lead, 0, 0)

            args += [kept, received]
            in_specs += [pl.BlockSpec((None,) * len(links) + (r, n), index)] * 2
            shapes.append(shaped(rest + (r, n)))
            out_specs.append(pl.BlockSpec((None,) * len(rest) + (r, n), lambda i, s, count=len(rest): (i,) * count + (0, 0)))
    outs = call(add_kernel, after, args, prefetch=(me,), grid=(len(GRID) - level,), in_specs=in_specs, out_specs=out_specs,
                out_shape=shapes, flops=STEP * sum(x.size for x in shapes))
    return list(zip(outs[::2], outs[1::2]))


LAST_TILE = 2 * LANES


def last_kernel(a_ref, b_ref, tail_ref, full_ref, at_ref, made_ref, got_ref, own_ref, all_ref, swap_sem, spread_sem):
    step, n_steps = pl.program_id(0), made_ref.shape[0]
    me = lax.axis_index(MESH_AXIS)
    mine, chip = bit(me, LINKS[0]), lax.div(me, 2)
    partner = device(me + 1 - 2 * mine)
    others = [lax.rem(chip + k, CHIPS) for k in range(1, CHIPS)]

    def swap(tile):
        return pltpu.make_async_remote_copy(made_ref.at[tile, :, 1 - mine], got_ref.at[tile], swap_sem.at[0, tile], swap_sem.at[1, tile], **partner)

    def sends(tile):
        return [pltpu.make_async_remote_copy(own_ref.at[tile, other], all_ref.at[tile, chip], spread_sem.at[0, tile, k], spread_sem.at[1, tile, k],
                                             **device(2 * other + mine)) for k, other in enumerate(others)]

    def spread(tile):
        swap(tile).wait_recv()
        own_ref[tile] = made_ref[tile, :, mine] + got_ref[tile]
        for copy in sends(tile):
            copy.start()
        all_ref[tile, chip] = own_ref[tile, chip]

    @first_step()
    def _():
        barrier = pltpu.get_barrier_semaphore()
        pl.semaphore_signal(barrier, **partner)
        for other in others:
            pl.semaphore_signal(barrier, **device(2 * other + mine))
        for j in range(CHIPS):
            at_ref[lane_tile(j), :] = a_ref[:, lane_tile(j)].T
        pl.semaphore_wait(barrier, CHIPS)

    made_ref[step] = dot(at_ref[:], b_ref[:]).reshape(made_ref.shape[1:])

    @pl.when(step == n_steps - 1)
    def _():
        made_ref[step, :, :, :, LANES:] += tail_ref[:].reshape(made_ref.shape[1:4] + (LANES,))

    swap(step).start()

    @pl.when(step > 0)
    def _():
        spread(step - 1)

    @pl.when(step == n_steps - 1)
    def _():
        spread(step)
        for tile in range(n_steps):
            swap(tile).wait_send()
            for copy in sends(tile):
                copy.wait_send()
                copy.wait_recv()
            full_ref[:, tile * LAST_TILE:(tile + 1) * LAST_TILE] = sum(all_ref[tile, source] for source in range(CHIPS))


def last_grads(a, b, tail, number):
    k, m = a.shape
    n_steps = PACK // LAST_TILE
    shape, block = (HEAD, PACK), (n_steps, CHIPS, HEAD, LAST_TILE)
    dma = pltpu.SemaphoreType.DMA
    return call(last_kernel, (), (a, b, tail), grid=(n_steps,),
                in_specs=[held(a.shape), pl.BlockSpec((k, LAST_TILE), lambda j: (0, j)), held(tail.shape)],
                out_specs=whole_out(shape), out_shape=shaped(shape),
                scratch_shapes=[pltpu.VMEM((m, k), BF16), pltpu.VMEM((n_steps, CHIPS, 2, HEAD, LAST_TILE), F32)] + [pltpu.VMEM(block, F32)] * 3
                + [dma((2, n_steps)), dma((2, n_steps, CHIPS - 1))], flops=2 * k * m * PACK, partners=number)


def end_kernel(full_ref, kept_ref, received_ref, sum_ref, wt_ref, pos_ref, *vec_refs):
    n_pix, n_pos = wt_ref.shape[1], pos_ref.shape[1]
    sum_ref[:] = kept_ref[:] + received_ref[:]
    wt_ref[:] = full_ref[:, :n_pix]
    pos_ref[:] = full_ref[:, n_pix:n_pix + n_pos]
    pos_ref[:, :1] = full_ref[:, VEC_ROW + CLS:VEC_ROW + CLS + 1]
    rows = full_ref[:, VEC_ROW - VEC_AT:VEC_ROW - VEC_AT + LANES].T
    at = VEC_AT
    for ref in vec_refs:
        for lo in range(0, ref.shape[1], HEAD):
            ref[:, lo:lo + HEAD] = rows[at:at + 1]
            at += 1


def end_grads(full, kept, received, widths):
    args = (full, kept, received)
    shapes = [kept.shape] + [(HEAD, w) for w in widths[:2]] + [(1, w) for w in widths[2:]]
    return call(end_kernel, (), args, in_specs=[held(x.shape) for x in args], out_specs=[whole_out(s) for s in shapes],
                out_shape=[shaped(s) for s in shapes], flops=PACK)


PARAM_NAMES = ('w_patch', 'b_patch', 'pos_table', 'cls_tok', 'lnp_g', 'lnp_b', 'ln1_g', 'ln1_b', 'w_qkv', 'b_qkv', 'w_out', 'b_out', 'ln2_g', 'ln2_b', 'w_fc', 'b_fc', 'w_proj', 'b_proj')
PACKED = tuple(PARAM_NAMES[i] for i in (1, 3, 4, 5, 6, 7, 11, 12, 13, 17, 9, 15))


def solution(mesh):
    n_dev = mesh.shape[MESH_AXIS]

    def across(value, link):
        return lax.ppermute(value, MESH_AXIS, [(i, i ^ (1 << LINKS.index(link))) for i in range(n_dev)])

    def compute(patches, keep, *rest):
        shard = dict(zip(PARAM_NAMES, rest[:-1]))
        d, d_mlp = shard['w_out'].shape[1], shard['w_fc'].shape[1]
        n_pix, n_pos = shard['w_patch'].shape[0], shard['pos_table'].shape[0]
        scale = shard['w_qkv'].shape[-1] ** -0.5
        me = lax.axis_index(MESH_AXIS).reshape(1)
        by_token = lambda x: x.transpose(1, 0, 2)

        def whole(value):
            return lax.all_gather(value, MESH_AXIS, tiled=True)

        w_qkv = shard['w_qkv'].astype(BF16).reshape(HEAD, -1)
        first = whole(pack_small(w_qkv, shard['w_patch'].T, shard['pos_table'].T, [shard[name][None] for name in PACKED]))
        w_fo = whole(jnp.concatenate([shard['w_fc'].astype(BF16), shard['w_out'].astype(BF16)], axis=1))
        w_proj = whole(shard['w_proj'].astype(BF16))

        zo, g = pick_rows(keep, by_token(patches), by_token(rest[-1]))
        hat, a, stats, vecs, b_qkv, b_fc = embed(zo, first, d_mlp)
        qkv, ctx = attend(a, first, b_qkv, scale)
        m, c, act, pre = mlp_up(ctx, hat, w_fo, vecs, b_fc)

        def cut(outs, orders):
            return [(order, kept, across(sent, order[0])) for order, sent, kept in zip(orders, outs[::2], outs[1::2])]

        def halve(items, level, after):
            pairs = halves(me, items, level, after)
            return [(order, kept, across(sent, order[level])) for (order, _, _), (sent, kept) in zip(items, pairs)]

        def over_chips(made):
            rings = [[2 * chip + core for chip in RING] for core in range(2)]
            return lax.psum_scatter(made[0].reshape(-1, made[0].shape[-1]), MESH_AXIS, axis_index_groups=rings, tiled=True)

        made = wgrad(act, g, (), (), 0, (), by_rows=True)
        g_proj = over_chips(made)
        h1 = mlp_down(act, m, w_proj, vecs, made)
        d_pre, d_mid, d_mid_b, d_ctx, sums_m, sum_fc = mlp_grad(g, pre, m, w_proj, w_fo, vecs, (h1,))
        made = wgrad(c, d_pre, (), (), 1, ())
        g_fc = over_chips(made)
        one = ORDERS[2:]
        outs = wgrad(ctx, d_mid_b, one, (0, d), 2, made)
        out = cut(outs, one)
        d_qkv, sum_qkv = attend_grad(qkv, d_ctx, scale, (outs[1],))
        out = halve(out, 1, (sum_qkv,))
        made = wgrad(a, d_qkv, (), (), 3, (out[0][1],))
        g_qkv = over_chips(made)
        out = halve(out, 2, made)
        d_emb, sums_e = embed_grad(d_qkv, d_mid, hat, stats, first, vecs, (out[0][1],))
        _, kept, received = out[0]
        tail = vector_tail(sums_e, sums_m, sum_qkv, sum_fc)
        full = last_grads(d_emb, zo, tail, 4)
        widths = [n_pix, n_pos] + [shard[name].shape[0] for name in PACKED]
        g_out, *done = end_grads(full, kept, received, widths)

        grads = dict(w_patch=done[0].T, pos_table=done[1].T, w_qkv=g_qkv.reshape(shard['w_qkv'].shape), w_out=g_out, w_fc=g_fc, w_proj=g_proj)
        grads.update({name: value.reshape(-1) for name, value in zip(PACKED, done[2:])})
        return (by_token(h1),) + tuple(grads[name] for name in PARAM_NAMES)

    batch_spec = P(MESH_AXIS)
    param_specs = tuple(P(None, MESH_AXIS) if name in ('w_patch', 'pos_table') else batch_spec for name in PARAM_NAMES)
    return jax.shard_map(compute, mesh=mesh, in_specs=(batch_spec, batch_spec) + param_specs + (batch_spec,), out_specs=(batch_spec,) + param_specs, check_vma=False)
```

```python
import functools

import jax
import jax.numpy as jnp
from jax import lax
from jax.experimental import pallas as pl
from jax.experimental.pallas import tpu as pltpu
from jax.sharding import PartitionSpec as P


F32, BF16, I32 = jnp.float32, jnp.bfloat16, jnp.int32
LN_EPS = 1e-5
INV_SQRT2 = 0.7071067811865476
INV_SQRT_2PI = 0.3989422804014327
LOG2E = 1.4426950408889634
MASKED = -1e30
SUBLANES, LANES, HEAD = 8, 128, 64
TOK, FEW, MANY = 50, 4, 8
ROWS, GROWS = FEW * TOK, MANY * TOK
WIN = 112
STARTS = (0, ROWS - WIN)
EDGE = 96
PACK, VEC_ROW = 1024, 976
VEC_AT = VEC_ROW % LANES
N_VEC, VEC_ROWS = 10, 32
B_PATCH, CLS, LNP_G, LNP_B, LN1_G, LN1_B, B_OUT, LN2_G, LN2_B, B_PROJ = range(N_VEC)
STEP = 512
ALL_VMEM = 67043328
ANY = pl.BlockSpec(memory_space=pl.ANY)


def product(dims, left, right):
    return lax.dot_general(left, right, ((dims[:1], dims[1:]), ((), ())), preferred_element_type=F32)


dot = functools.partial(product, (1, 0))
dot_nt = functools.partial(product, (1, 1))
dot_tn = functools.partial(product, (0, 0))


def col_sum(x):
    return jnp.sum(x, axis=0, keepdims=True)


def col_max(x):
    return jnp.max(x, axis=0, keepdims=True)


def row_mean(x):
    return jnp.mean(x, axis=1, keepdims=True)


def row(ref, at):
    return ref[at:at + 1, :]


def iota(shape, axis):
    return lax.broadcasted_iota(I32, shape, axis)


def one_hot(test):
    return test.astype(F32).astype(BF16)


def origin(shape, *_):
    return (0,) * len(shape)


def held(shape):
    return pl.BlockSpec(shape, functools.partial(origin, shape), pipeline_mode=pl.Buffered(1))


def held_cols(n_rows, n_cols, at):
    return pl.BlockSpec((n_rows, n_cols), lambda *_: (0, at // n_cols), pipeline_mode=pl.Buffered(1))


def whole_out(shape):
    return pl.BlockSpec(shape, functools.partial(origin, shape))


def rows_spec(n_rows, width):
    return pl.BlockSpec((n_rows, width), lambda i, *_: (i, 0))


def this_block(n_rows, width, n):
    return pl.BlockSpec((n_rows, width), lambda i: (jnp.minimum(i, n - 1), 0))


def last_block(n_rows, width):
    return pl.BlockSpec((n_rows, width), lambda i: (jnp.maximum(i - 1, 0), 0))


def shaped(shape, dtype=F32):
    return jax.ShapeDtypeStruct(shape, dtype)


def call(kernel, after, args, *, prefetch=(), grid=(1,), in_specs, out_specs, out_shape, scratch_shapes=(), flops, n_bytes=0, partners=None, aliases=()):
    n_in, n_after = len(prefetch) + len(args), len(after)

    def body(*refs):
        return kernel(*refs[:n_in], *refs[n_in + n_after:])

    return pl.pallas_call(
        body,
        grid_spec=pltpu.PrefetchScalarGridSpec(
            num_scalar_prefetch=len(prefetch), grid=grid, in_specs=list(in_specs) + [ANY] * n_after,
            out_specs=out_specs, scratch_shapes=list(scratch_shapes)),
        out_shape=out_shape, input_output_aliases=dict(aliases),
        compiler_params=pltpu.CompilerParams(
            dimension_semantics=(pltpu.ARBITRARY,) * len(grid), vmem_limit_bytes=ALL_VMEM,
            collective_id=partners, has_side_effects=partners is not None),
        cost_estimate=pl.CostEstimate(flops=int(flops), bytes_accessed=int(n_bytes), transcendentals=0),
    )(*prefetch, *args, *after)


MESH_AXIS = 'fsdp'
CHIPS = 8


def device(at):
    return dict(device_id=(at,), device_id_type=pl.DeviceIdType.MESH)


def place():
    me = lax.axis_index(MESH_AXIS)
    core, chip = lax.rem(me, 2), lax.div(me, 2)
    return me, chip, core, me + 1 - 2 * core, [lax.rem(chip + k, CHIPS) for k in range(1, CHIPS)]


def meet(partners):
    barrier = pltpu.get_barrier_semaphore()
    for partner in partners:
        pl.semaphore_signal(barrier, **device(partner))
    pl.semaphore_wait(barrier, len(partners))


def first_step():
    return pl.when(pl.program_id(0) == 0)


def final_step():
    return pl.when(pl.program_id(0) == pl.num_programs(0) - 1)


def staggered(body, refs):
    step, last = pl.program_id(0), pl.num_programs(0) - 1
    pl.when(step == 0)(lambda: body(False, True, *refs))
    pl.when((step > 0) & (step < last))(lambda: body(True, True, *refs))
    pl.when(step == last)(lambda: body(True, False, *refs))


def gather_sems():
    dma = pltpu.SemaphoreType.DMA
    return [dma(()), dma((2 * CHIPS - 1,)), dma((2 * CHIPS - 1,))]


def hosted_gather(own_ref, all_ref, own_sem, send_sem, got_sem):
    me, chip, core, partner, others = place()
    sources = [lax.rem(chip + CHIPS - k, CHIPS) for k in range(1, CHIPS)]

    def rows(owner):
        return all_ref.at[pl.ds(pl.multiple_of(owner * HEAD, HEAD), HEAD)]

    def send(source, owner, to, at):
        return pltpu.make_async_remote_copy(source, rows(owner), send_sem.at[at], got_sem.at[at], **device(to))

    local = pltpu.make_async_copy(own_ref, rows(me), own_sem)
    sent = [send(own_ref, me, partner, 0)] + [send(own_ref, me, 2 * other + core, k + 1) for k, other in enumerate(others)]
    passed = [send(rows(2 * source + core), 2 * source + core, partner, CHIPS + k) for k, source in enumerate(sources)]

    @first_step()
    def _():
        meet([partner] + [2 * other + core for other in others])
        local.start()
        for copy in sent:
            copy.start()

    def finish():
        @final_step()
        def _():
            for arrived, copy in zip(sent[1:], passed):
                arrived.wait_recv()
                copy.start()
            local.wait()
            sent[0].wait_recv()
            for copy in passed:
                copy.wait_recv()
            for copy in sent + passed:
                copy.wait_send()

    return finish


def clear(*refs):
    for ref in refs:
        ref[:] = jnp.zeros_like(ref)


def normalize(x):
    centered = x - row_mean(x)
    inv = lax.rsqrt(row_mean(centered * centered) + LN_EPS)
    return centered * inv, inv


def norm_grad(d_out, x_hat, inv, gain):
    d_hat = d_out * gain
    return inv * (d_hat - row_mean(d_hat) - x_hat * row_mean(d_hat * x_hat))


def image_of(at, n_img=FEW):
    return sum((at >= j * TOK).astype(I32) for j in range(1, n_img))


def is_class(n_rows):
    at = iota((n_rows, 1), 0)
    return at == TOK * image_of(at, n_rows // TOK)


def pack_kernel(wt_ref, pt_ref, *refs):
    *vec_refs, out_ref, rows_ref, pos_ref = refs
    n_pix, n_pos = wt_ref.shape[1], pt_ref.shape[1]
    out_ref[:, :n_pix] = wt_ref[:].astype(BF16)
    out_ref[:, n_pix:n_pix + LANES] = pt_ref[:, :LANES].astype(BF16)
    clear(rows_ref, pos_ref)
    pos_ref[:, :n_pos - LANES] = pt_ref[:, LANES:]
    at = VEC_AT
    for ref in vec_refs:
        for lo in range(0, ref.shape[1], HEAD):
            rows_ref[at:at + 1, :HEAD] = ref[:, lo:lo + HEAD]
            at += 1
    out_ref[:, n_pix + LANES:] = (pos_ref[:] + rows_ref[:].T[:HEAD]).astype(BF16)


def pack_small(wt, pt, vecs):
    args = [wt, pt] + vecs
    shape = (HEAD, PACK)
    return call(pack_kernel, (), args, in_specs=[held(x.shape) for x in args], out_specs=whole_out(shape), out_shape=shaped(shape, BF16),
                scratch_shapes=[pltpu.VMEM((LANES, LANES), F32), pltpu.VMEM((HEAD, LANES), F32)], flops=PACK)


def pick_kernel(keep_ref, patches_ref, g_ref, small_ref, zo_ref, gi_ref, all_ref, pad_ref, move_ref, *sems):
    finish = hosted_gather(small_ref, all_ref, *sems)

    @first_step()
    def _():
        to, source = iota((GROWS, GROWS), 0), iota((GROWS, GROWS), 1)
        move_ref[:] = one_hot(to == lax.rem(source, MANY) * TOK + lax.div(source, MANY))

    n_patch, _, n_pix = patches_ref.shape
    clear(pad_ref)
    pad_ref[:, :TOK - 1] = keep_ref[:].astype(F32)
    image, lane = iota(pad_ref.shape, 0), iota(pad_ref.shape, 1)
    spread = pad_ref[:]
    for b in range(MANY):
        spread = jnp.where(image == b, pltpu.roll(pad_ref[:], TOK * b + 1, 1), spread)
    own = (lane > TOK * image) & (lane < TOK * image + TOK)
    token = col_sum(jnp.where(own, spread + 1.0, 0.0))
    source = col_sum(jnp.where(own, spread * MANY + image.astype(F32), 0.0))
    source = jnp.where(token > 0.0, source, -1.0)
    cols = jnp.where(image == 0, source, token).T[:GROWS].astype(I32)
    source, token = cols[:, :1], cols[:, 1:2]
    pick = one_hot(iota((GROWS, MANY * n_patch), 1) == source)
    zo_ref[:, :n_pix] = dot(pick, patches_ref[:].reshape(MANY * n_patch, n_pix)).astype(BF16)
    zo_ref[:, n_pix:] = one_hot(iota((GROWS, PACK - n_pix), 1) == token)
    gi_ref[:] = dot(move_ref[:], g_ref[:].reshape(GROWS, g_ref.shape[2])).astype(BF16)

    finish()


def pick_rows(keep, patches_t, g_t, small):
    _, n_img, _ = patches_t.shape
    d = g_t.shape[2]
    n_tok = n_img * TOK
    by_image = lambda x: pl.BlockSpec((x.shape[0], MANY, x.shape[2]), lambda i: (0, i, 0))
    return call(pick_kernel, (), (keep, patches_t, g_t, small), grid=(n_img // MANY,),
                in_specs=[rows_spec(MANY, TOK - 1), by_image(patches_t), by_image(g_t), ANY],
                out_specs=[rows_spec(GROWS, PACK), rows_spec(GROWS, d), ANY],
                out_shape=[shaped((n_tok, PACK), BF16), shaped((n_tok, d), BF16), shaped((2 * CHIPS * HEAD, PACK), BF16)],
                scratch_shapes=[pltpu.VMEM((MANY, STEP), F32), pltpu.VMEM((GROWS, GROWS), BF16)] + gather_sems(),
                flops=STEP * patches_t.size, partners=0)


def embed_kernel(zo_ref, wt_ref, hat_ref, a_ref, stat_ref, vec_ref, bq_ref, bf_ref, next_ref, now_ref):
    @first_step()
    def _():
        base = VEC_ROW - VEC_AT
        vec_ref[:] = wt_ref[:, base:base + LANES].astype(F32).T[VEC_AT:VEC_AT + VEC_ROWS]
        at = N_VEC
        for ref in (bq_ref, bf_ref):
            n = ref.shape[1] // vec_ref.shape[1]
            chunk = lambda q: row(vec_ref, at + q % n)[:, q // n * HEAD:(q // n + 1) * HEAD]
            for lo in range(0, ref.shape[1], LANES):
                ref[:, lo:lo + LANES] = jnp.concatenate([chunk(lo // HEAD), chunk(lo // HEAD + 1)], axis=1)
            at += n

    now_ref[:] = next_ref[:]
    next_ref[:] = dot_nt(zo_ref[:], wt_ref[:]) + jnp.where(is_class(GROWS), row(vec_ref, CLS), row(vec_ref, B_PATCH))
    hat, inv = normalize(now_ref[:])
    hat_ref[:] = hat
    h0 = hat * row(vec_ref, LNP_G) + row(vec_ref, LNP_B)
    mean1 = row_mean(h0)
    centered = h0 - mean1
    inv1 = lax.rsqrt(row_mean(centered * centered) + LN_EPS)
    a_ref[:] = (centered * inv1 * row(vec_ref, LN1_G) + row(vec_ref, LN1_B)).astype(BF16)
    lane = iota(stat_ref.shape, 1)
    stat_ref[:] = jnp.where(lane == 0, inv, jnp.where(lane == 1, inv1, mean1))


def embed(zo, small, d_qkv, d_mlp):
    n_tok = zo.shape[0]
    d = small.shape[0]
    n = n_tok // GROWS
    outs = ((VEC_ROWS, d), (1, d_qkv), (1, d_mlp))
    return call(embed_kernel, (), (zo, small), grid=(n + 1,),
                in_specs=[this_block(GROWS, PACK, n), held(small.shape)],
                out_specs=[last_block(GROWS, d), last_block(GROWS, d), last_block(GROWS, LANES)] + [whole_out(s) for s in outs],
                out_shape=[shaped((n_tok, d)), shaped((n_tok, d), BF16), shaped((n_tok, LANES))] + [shaped(s) for s in outs],
                scratch_shapes=[pltpu.VMEM((GROWS, d), F32)] * 2, flops=2 * zo.size * d)


def window_mask(start):
    key, query = (iota((WIN, 2 * WIN), axis) for axis in (0, 1))
    return jnp.where(image_of(key + start) == image_of(lax.rem(query, WIN) + start), 0.0, MASKED)


def set_masks(mask_ref):
    for i, start in enumerate(STARTS):
        mask_ref[i] = window_mask(start)


def split_heads(x):
    first = iota(x.shape, 1) < HEAD
    zero = jnp.zeros_like(x)
    return jnp.concatenate([jnp.where(first, x, zero), jnp.where(first, zero, x)], axis=0)


def join_heads(x):
    return jnp.where(iota((WIN, LANES), 1) < HEAD, x[:WIN], x[WIN:])


def join_windows(lo, hi):
    at = EDGE + SUBLANES
    shift = STARTS[1]
    edge = jnp.where(iota((SUBLANES, LANES), 0) < 2 * TOK - EDGE, lo[EDGE:at], hi[EDGE - shift:at - shift])
    return jnp.concatenate([lo[:EDGE], edge, hi[at - shift:]], axis=0)


def weights_t(logits, mask, scale):
    masked = logits + mask
    e = jnp.exp2((masked - col_max(masked)) * (scale * LOG2E))
    return e * (1.0 / col_sum(e))


def lane_tile(at):
    return slice(at * LANES, (at + 1) * LANES)


def reader(ref):
    return lambda at, i: ref[STARTS[i]:STARTS[i] + WIN, lane_tile(at)]


def every_unit(n_tiles):
    return [(pair, i) for pair in range(n_tiles) for i in range(len(STARTS))]


def window_scratch():
    return pltpu.VMEM((len(STARTS), WIN, 2 * WIN), F32)


def attend_kernel(scale, a_ref, w_ref, b_ref, qkv_ref, o_ref, mask_ref):
    @first_step()
    def _():
        set_masks(mask_ref)

    n_tiles = o_ref.shape[1] // LANES
    a = a_ref[:]
    for lo in range(0, b_ref.shape[1], STEP):
        cols = slice(lo, lo + STEP)
        qkv_ref[:, cols] = (dot(a, w_ref[:, cols]) + b_ref[:, cols]).astype(BF16)
    read, units = reader(qkv_ref), every_unit(n_tiles)
    logits = [dot_nt(read(n_tiles + pair, i), split_heads(read(pair, i))) for pair, i in units]
    probs = [weights_t(x, mask_ref[i], scale).astype(BF16) for x, (_, i) in zip(logits, units)]
    outs = [join_heads(dot_tn(p, read(2 * n_tiles + pair, i))) for p, (pair, i) in zip(probs, units)]
    for lo, hi, (pair, _) in zip(outs[::2], outs[1::2], units[::2]):
        o_ref[:, lane_tile(pair)] = join_windows(lo, hi).astype(BF16)


def attend(a, first, b_qkv, scale):
    n_tok, d = a.shape
    width = b_qkv.shape[1]
    return call(functools.partial(attend_kernel, scale), (), (a, first, b_qkv), grid=(n_tok // ROWS,),
                in_specs=[rows_spec(ROWS, d), held_cols(d, width, 0), held(b_qkv.shape)],
                out_specs=[rows_spec(ROWS, width), rows_spec(ROWS, d)],
                out_shape=[shaped((n_tok, width), BF16), shaped((n_tok, d), BF16)],
                scratch_shapes=[window_scratch()], flops=4 * a.size * width)


def attend_grad_kernel(scale, qkv_ref, dctx_ref, dqkv_ref, bsum_ref, mask_ref):
    @first_step()
    def _():
        set_masks(mask_ref)
        clear(bsum_ref)

    n_tiles = dctx_ref.shape[1] // LANES
    read, read_grad, units = reader(qkv_ref), reader(dctx_ref), every_unit(n_tiles)
    q2 = [split_heads(read(pair, i)) for pair, i in units]
    do2 = [split_heads(read_grad(pair, i)) for pair, i in units]
    logits = [dot_nt(read(n_tiles + pair, i), q) for q, (pair, i) in zip(q2, units)]
    dp = [dot_nt(read(2 * n_tiles + pair, i), do) for do, (pair, i) in zip(do2, units)]
    logits = [x * scale + mask_ref[i] for x, (_, i) in zip(logits, units)]
    e = [jnp.exp2((x - col_max(x)) * LOG2E) for x in logits]
    p = [x * (1.0 / col_sum(x)) for x in e]
    dv = [dot(x.astype(BF16), do) for x, do in zip(p, do2)]
    ds = [(x * (y - col_sum(x * y)) * scale).astype(BF16) for x, y in zip(p, dp)]
    dk = [dot(x, q) for x, q in zip(ds, q2)]
    dq = [join_heads(dot_tn(x, read(n_tiles + pair, i))) for x, (pair, i) in zip(ds, units)]
    for at, (pair, _) in enumerate(units[::2]):
        for part, grads in enumerate((dq, dk, dv)):
            both = join_windows(grads[2 * at], grads[2 * at + 1])
            cols = lane_tile(part * n_tiles + pair)
            dqkv_ref[:, cols] = both.astype(BF16)
            bsum_ref[:, cols] += col_sum(both)


def attend_grad(qkv, d_ctx, scale, after):
    n_tok, width = qkv.shape
    return call(functools.partial(attend_grad_kernel, scale), after, (qkv, d_ctx), grid=(n_tok // ROWS,),
                in_specs=[rows_spec(ROWS, width), rows_spec(ROWS, d_ctx.shape[1])], out_specs=[rows_spec(ROWS, width), whole_out((1, width))],
                out_shape=[shaped((n_tok, width), BF16), shaped((1, width))],
                scratch_shapes=[window_scratch()], flops=3 * d_ctx.size * width)


def erf_cdf(u):
    return 0.5 + 0.5 * lax.erf(u * INV_SQRT2)


def mlp_up_kernel(*refs):
    staggered(mlp_up_step, refs)


def mlp_up_step(with_now, with_next, o_ref, hat_ref, wo_ref, wf_ref, vec_ref, bf_ref, m_ref, c_ref, act_ref, pre_ref, next_ref, now_ref):
    if with_now:
        now_ref[:] = next_ref[:]
        c = now_ref[:]
    if with_next:
        m = hat_ref[:] * row(vec_ref, LNP_G) + row(vec_ref, LNP_B) + dot(o_ref[:], wo_ref[:]) + row(vec_ref, B_OUT)
        m_ref[:] = m
        hat2, _ = normalize(m)
        next_c = (hat2 * row(vec_ref, LN2_G) + row(vec_ref, LN2_B)).astype(BF16)
        c_ref[:] = next_c
    if with_now:
        for lo in range(0, wf_ref.shape[1], STEP):
            cols = slice(lo, lo + STEP)
            u = dot(c, wf_ref[:, cols]) + bf_ref[:, cols]
            pre_ref[:, cols] = u
            act_ref[:, cols] = (u * erf_cdf(u)).astype(BF16)
    if with_next:
        next_ref[:] = next_c


def mlp_up(o, hat, w_fo, vecs, b_fc):
    n_tok, d = o.shape
    f = b_fc.shape[1]
    n = n_tok // GROWS
    return call(mlp_up_kernel, (), (o, hat, w_fo, w_fo, vecs, b_fc), grid=(n + 1,),
                in_specs=[this_block(GROWS, d, n), this_block(GROWS, d, n), held_cols(d, d, f), held_cols(d, f, 0), held(vecs.shape), held(b_fc.shape)],
                out_specs=[this_block(GROWS, d, n), this_block(GROWS, d, n), last_block(GROWS, f), last_block(GROWS, f)],
                out_shape=[shaped((n_tok, d)), shaped((n_tok, d), BF16), shaped((n_tok, f), BF16), shaped((n_tok, f))],
                scratch_shapes=[pltpu.VMEM((GROWS, d), BF16)] * 2, flops=3 * o.size * f)


def mlp_down_kernel(act_ref, m_ref, w_ref, vec_ref, own_ref, h1_ref, all_ref, send_sem, got_sem):
    _, chip, core, _, others = place()
    copies = [pltpu.make_async_remote_copy(own_ref.at[other], all_ref.at[chip], send_sem.at[k], got_sem.at[k], **device(2 * other + core))
              for k, other in enumerate(others)]

    @first_step()
    def _():
        meet([2 * other + core for other in others])
        for copy in copies:
            copy.start()

    h1_ref[:] = (m_ref[:] + dot(act_ref[:], w_ref[:]) + row(vec_ref, B_PROJ)).astype(BF16)

    @final_step()
    def _():
        for copy in copies:
            copy.wait()


def mlp_down(act, m, w_proj, vecs, own, number):
    n_tok, f = act.shape
    d = m.shape[1]
    dma = pltpu.SemaphoreType.DMA((CHIPS - 1,))
    return call(mlp_down_kernel, (), (act, m, w_proj, vecs, own), grid=(n_tok // GROWS,),
                in_specs=[rows_spec(GROWS, f), rows_spec(GROWS, d), held(w_proj.shape), held(vecs.shape), ANY],
                out_specs=[rows_spec(GROWS, d), ANY], out_shape=[shaped((n_tok, d), BF16), shaped(own.shape)], scratch_shapes=[dma, dma],
                flops=2 * m.size * f, partners=number)


def mlp_grad_kernel(g_ref, pre_ref, m_ref, wp_ref, wf_ref, wo_ref, vec_ref, dpre_ref, dmid_ref, dmidb_ref, dctx_ref, vsum_ref, bfc_ref):
    @first_step()
    def _():
        clear(vsum_ref, bfc_ref)

    g = g_ref[:]
    step = 2 * STEP
    d_c = jnp.zeros(m_ref.shape, F32)
    cuts = [slice(lo, lo + step) for lo in range(0, wp_ref.shape[0], step)]
    acts, pres = dict(), dict()
    n = len(cuts)
    for tick in range(n + 2):
        if tick < n:
            acts[tick] = dot_nt(g, wp_ref[cuts[tick], :])
        if 0 <= tick - 1 < n:
            cols = cuts[tick - 1]
            u = pre_ref[:, cols]
            w = u * INV_SQRT2
            d_pre = acts.pop(tick - 1) * (0.5 + 0.5 * lax.erf(w) + u * (jnp.exp2((w * w) * (-LOG2E)) * INV_SQRT_2PI))
            bfc_ref[:, cols] += col_sum(d_pre)
            pres[tick - 1] = d_pre.astype(BF16)
            dpre_ref[:, cols] = pres[tick - 1]
        if tick >= 2:
            d_c = d_c + dot_nt(pres.pop(tick - 2), wf_ref[:, cuts[tick - 2]])
    hat2, inv2 = normalize(m_ref[:])
    g_f = g.astype(F32)
    d_mid = norm_grad(d_c, hat2, inv2, row(vec_ref, LN2_G)) + g_f
    dmid_ref[:] = d_mid
    d_mid_b = d_mid.astype(BF16)
    dmidb_ref[:] = d_mid_b
    dctx_ref[:] = dot_nt(d_mid_b, wo_ref[:]).astype(BF16)
    for at, part in enumerate((d_mid, d_c * hat2, d_c, g_f)):
        vsum_ref[at:at + 1, :] += col_sum(part)


def mlp_grad(g, pre, m, w_proj, w_fo, vecs, after):
    n_tok, d = g.shape
    f = pre.shape[1]
    wide, narrow = rows_spec(GROWS, f), rows_spec(GROWS, d)
    return call(mlp_grad_kernel, after, (g, pre, m, w_proj, w_fo, w_fo, vecs), grid=(n_tok // GROWS,),
                in_specs=[narrow, wide, narrow, held(w_proj.shape), held_cols(d, f, 0), held_cols(d, d, f), held(vecs.shape)],
                out_specs=[wide, narrow, narrow, narrow, whole_out((SUBLANES, d)), whole_out((1, f))],
                out_shape=[shaped((n_tok, f), BF16), shaped((n_tok, d)), shaped((n_tok, d), BF16), shaped((n_tok, d), BF16),
                           shaped((SUBLANES, d)), shaped((1, f))],
                flops=5 * g.size * f)


CUTS = (0, 104, 208, 304, GROWS)


def embed_grad_kernel(*refs):
    @first_step()
    def _():
        clear(refs[7])

    staggered(embed_grad_step, refs)


def embed_grad_step(with_now, with_next, dqkv_ref, dmid_ref, hat_ref, stat_ref, w_ref, vec_ref, demb_ref, vsum_ref, next_ref, now_ref, dx_ref):
    if with_now:
        now_ref[:] = next_ref[:]
    width = now_ref.shape[1] // (len(CUTS) - 1)
    sums = []
    for j, (lo, hi) in enumerate(zip(CUTS, CUTS[1:])):
        cols, rows = slice(j * width, (j + 1) * width), slice(lo, hi)
        if with_next:
            next_ref[:, cols] = dot_nt(dqkv_ref[:], w_ref[cols, :])
        if not with_now:
            continue
        d_a, hat_p = now_ref[rows, :], hat_ref[rows, :]
        inv_p, inv1, mean1 = (stat_ref[rows, k:k + 1] for k in range(3))
        hat1 = (hat_p * row(vec_ref, LNP_G) + row(vec_ref, LNP_B) - mean1) * inv1
        d_zero = norm_grad(d_a, hat1, inv1, row(vec_ref, LN1_G)) + dmid_ref[rows, :]
        d_x = norm_grad(d_zero, hat_p, inv_p, row(vec_ref, LNP_G))
        demb_ref[rows, :] = d_x.astype(BF16)
        dx_ref[rows, :] = d_x
        sums.append([col_sum(part) for part in (d_x, d_zero * hat_p, d_zero, d_a * hat1, d_a)])
    if with_now:
        d_all, *others = (sum(parts) for parts in zip(*sums))
        d_cls = sum(row(dx_ref, at) for at in range(0, GROWS, TOK))
        for at, part in enumerate([d_all - d_cls, d_cls] + others):
            vsum_ref[at:at + 1, :] += part


def embed_grad(dqkv, d_mid, hat, stats, first, vecs, after):
    n_tok, d = d_mid.shape
    width = dqkv.shape[1]
    n = n_tok // GROWS
    return call(embed_grad_kernel, after, (dqkv, d_mid, hat, stats, first, vecs), grid=(n + 1,),
                in_specs=[this_block(GROWS, width, n), last_block(GROWS, d), last_block(GROWS, d), last_block(GROWS, LANES),
                          held_cols(d, width, 0), held(vecs.shape)],
                out_specs=[last_block(GROWS, d), whole_out((SUBLANES, d))], out_shape=[shaped((n_tok, d), BF16), shaped((SUBLANES, d))],
                scratch_shapes=[pltpu.VMEM((GROWS, d), F32)] * 3, flops=3 * d_mid.size * width)


def tail_kernel(se_ref, sm_ref, sq_ref, sf_ref, out_ref, rows_ref):
    d = se_ref.shape[1]
    clear(rows_ref)
    at, cut = VEC_AT, VEC_AT + B_OUT
    rows_ref[at:cut, :] = se_ref[:B_OUT, :]
    at += N_VEC
    rows_ref[cut:at, :] = sm_ref[:N_VEC - B_OUT, :]
    for ref in (sq_ref, sf_ref):
        n = ref.shape[1] // d
        for r in range(n):
            chunk = lambda q: ref[:, (n * q + r) * HEAD:(n * q + r + 1) * HEAD]
            for j in range(d // LANES):
                rows_ref[at:at + 1, lane_tile(j)] = jnp.concatenate([chunk(2 * j), chunk(2 * j + 1)], axis=1)
            at += 1
    for j in range(d // LANES):
        out_ref[lane_tile(j)] = rows_ref[:, lane_tile(j)].T


def vector_tail(*args):
    d = args[0].shape[1]
    return call(tail_kernel, (), args, in_specs=[held(x.shape) for x in args], out_specs=whole_out((d, LANES)), out_shape=shaped((d, LANES)),
                scratch_shapes=[pltpu.VMEM((LANES, d), F32)], flops=d)


RING = [at ^ (at >> 1) for at in range(CHIPS)]


def ring_chip(at):
    half, quarter = lax.div(at, 2), lax.div(at, 4)
    return 4 * quarter + 2 * lax.rem(half + quarter, 2) + lax.rem(at + half, 2)


def wgrad_kernel(by_rows, first_tile, n_in, a_ref, b_ref, *refs):
    out_ref, made_ref, got_ref, own_ref, send_sem, got_sem, free_sem, out_sem, *at_ref = refs[n_in:]
    step, last = pl.program_id(0), pl.num_programs(0) - 1
    slot = lax.rem(step, 2)
    _, _, mine, partner, _ = place()
    partner = device(partner)

    def part(at, core):
        return made_ref.at[at, core] if by_rows else made_ref.at[at, :, core]

    def exchange(at):
        return pltpu.make_async_remote_copy(part(at, 1 - mine), got_ref.at[at], send_sem.at[at], got_sem.at[at], **partner)

    def store(at, tile):
        width = own_ref.shape[-1]
        out = out_ref.at[tile] if by_rows else out_ref.at[:, :, pl.ds(pl.multiple_of((tile + first_tile) * width, width), width)]
        return pltpu.make_async_copy(own_ref.at[at], out, out_sem.at[at])

    def finish(at, tile):
        exchange(at).wait_recv()

        @pl.when(tile >= 2)
        def _():
            store(at, 0).wait()

        own_ref[at] = part(at, mine)[:] + got_ref[at]

        @pl.when(tile + 2 <= last)
        def _():
            pl.semaphore_signal(free_sem.at[at], **partner)

        store(at, tile).start()

    @first_step()
    def _():
        if not by_rows:
            for j in range(CHIPS):
                at_ref[0][lane_tile(RING.index(j)), :] = a_ref[:, lane_tile(j)].T
        meet([partner['device_id'][0]])

    @pl.when(step >= 2)
    def _():
        exchange(slot).wait_send()

    total = dot_tn(a_ref[:], b_ref[:]) if by_rows else dot(at_ref[0][:], b_ref[:])
    made_ref[slot] = total.reshape(made_ref.shape[1:])

    @pl.when(step >= 2)
    def _():
        pl.semaphore_wait(free_sem.at[slot], 1)

    exchange(slot).start()

    @pl.when(step >= 1)
    def _():
        finish(1 - slot, step - 1)

    @pl.when(step == last)
    def _():
        finish(slot, step)
        for at in range(2):
            exchange(at).wait_send()
            store(at, 0).wait()


def wgrad(a, b, number, after, by_rows=False, into=(), spare=0):
    k, m = a.shape
    n = b.shape[1]
    r = m // (2 * CHIPS)
    width = into[0].shape[-1] if into else n + spare
    if by_rows:
        steps, made, own = CHIPS, (2, r, n), (r, n)
        in_specs, scratch = [pl.BlockSpec((k, 2 * r), lambda j: (0, ring_chip(j))), held(b.shape)], []
    else:
        steps, made, own = n // STEP, (CHIPS, 2, r, STEP), (CHIPS, r, STEP)
        in_specs, scratch = [held(a.shape), pl.BlockSpec((k, STEP), lambda j: (0, j))], [pltpu.VMEM((m, k), BF16)]
    slots = lambda shape: pltpu.VMEM((2,) + shape, F32)
    dma = pltpu.SemaphoreType.DMA((2,))
    return call(functools.partial(wgrad_kernel, by_rows, (width - n - spare) // STEP, len(into)), after, (a, b) + tuple(into), grid=(steps,),
                in_specs=in_specs + [ANY] * len(into), out_specs=ANY, out_shape=shaped((CHIPS, r, width)), aliases=[(2, 0)] * len(into),
                scratch_shapes=[slots(made), slots(own), slots(own), dma, dma, pltpu.SemaphoreType.REGULAR((2,)), dma] + scratch,
                flops=2 * k * m * n, partners=number)


def last_kernel(a_ref, b_ref, tail_ref, out_ref, at_ref, made_ref, got_ref, own_ref, swap_sem, out_sem):
    step, n_steps = pl.program_id(0), made_ref.shape[0]
    _, _, core, partner, _ = place()
    width = made_ref.shape[-1]

    def swap(tile):
        return pltpu.make_async_remote_copy(made_ref.at[tile, :, 1 - core], got_ref.at[tile], swap_sem.at[0, tile], swap_sem.at[1, tile], **device(partner))

    def store(tile):
        return pltpu.make_async_copy(own_ref.at[tile], out_ref.at[:, :, pl.ds(pl.multiple_of(tile * width, width), width)], out_sem.at[tile])

    def finish(tile):
        swap(tile).wait_recv()
        own_ref[tile] = made_ref[tile, :, core] + got_ref[tile]
        store(tile).start()

    @first_step()
    def _():
        for j in range(CHIPS):
            at_ref[lane_tile(j), :] = a_ref[:, lane_tile(j)].T
        meet([partner])

    made_ref[step] = dot(at_ref[:], b_ref[:]).reshape(made_ref.shape[1:])

    @final_step()
    def _():
        made_ref[step, :, :, :, width - LANES:] += tail_ref[:].reshape(made_ref.shape[1:4] + (LANES,))

    swap(step).start()

    @pl.when(step > 0)
    def _():
        finish(step - 1)

    @final_step()
    def _():
        finish(step)
        for tile in range(n_steps):
            swap(tile).wait_send()
            store(tile).wait()


def last_grads(a, b, tail, number):
    k, m = a.shape
    n_steps = PACK // STEP
    slots = lambda *shape: pltpu.VMEM((n_steps, CHIPS) + shape + (HEAD, STEP), F32)
    dma = pltpu.SemaphoreType.DMA
    return call(last_kernel, (), (a, b, tail), grid=(n_steps,),
                in_specs=[held(a.shape), pl.BlockSpec((k, STEP), lambda j: (0, j)), held(tail.shape)],
                out_specs=ANY, out_shape=shaped((CHIPS, HEAD, PACK)),
                scratch_shapes=[pltpu.VMEM((m, k), BF16), slots(2), slots(), slots(), dma((2, n_steps)), dma((n_steps,))],
                flops=2 * k * m * PACK, partners=number)


def end_kernel(h1_ref, own_ref, all_ref, token_ref, wt_ref, pos_ref, *refs):
    *vec_refs, full_ref, move_ref = refs

    @first_step()
    def _():
        to, source = iota((GROWS, GROWS), 0), iota((GROWS, GROWS), 1)
        move_ref[:] = one_hot(source == lax.rem(to, MANY) * TOK + lax.div(to, MANY))
        _, chip, _, _, others = place()
        full_ref[:] = own_ref[chip] + sum(all_ref[other] for other in others)
        n_pix, n_pos = wt_ref.shape[1], pos_ref.shape[1]
        wt_ref[:] = full_ref[:, :n_pix]
        pos_ref[:] = full_ref[:, n_pix:n_pix + n_pos]
        pos_ref[:, :1] = full_ref[:, VEC_ROW + CLS:VEC_ROW + CLS + 1]
        rows = full_ref[:, VEC_ROW - VEC_AT:VEC_ROW - VEC_AT + LANES].T
        at = VEC_AT
        for ref in vec_refs:
            for lo in range(0, ref.shape[1], HEAD):
                ref[:, lo:lo + HEAD] = rows[at:at + 1]
                at += 1

    token_ref[:] = dot(move_ref[:], h1_ref[:]).astype(BF16).reshape(token_ref.shape)


def end_grads(h1, own, received, widths):
    n_tok, d = h1.shape
    shapes = [(HEAD, w) for w in widths[:2]] + [(1, w) for w in widths[2:]]
    return call(end_kernel, (), (h1, own, received), grid=(n_tok // GROWS,),
                in_specs=[rows_spec(GROWS, d), held(own.shape), held(received.shape)],
                out_specs=[pl.BlockSpec((TOK, MANY, d), lambda i: (0, i, 0))] + [whole_out(s) for s in shapes],
                out_shape=[shaped((TOK, n_tok // TOK, d), BF16)] + [shaped(s) for s in shapes],
                scratch_shapes=[pltpu.VMEM((HEAD, PACK), F32), pltpu.VMEM((GROWS, GROWS), BF16)], flops=PACK)


PARAM_NAMES = ('w_patch', 'b_patch', 'pos_table', 'cls_tok', 'lnp_g', 'lnp_b', 'ln1_g', 'ln1_b', 'w_qkv', 'b_qkv', 'w_out', 'b_out', 'ln2_g', 'ln2_b', 'w_fc', 'b_fc', 'w_proj', 'b_proj')
PACKED = tuple(PARAM_NAMES[i] for i in (1, 3, 4, 5, 6, 7, 11, 12, 13, 17, 9, 15))


def solution(mesh):
    def compute(patches, keep, *rest):
        shard = dict(zip(PARAM_NAMES, rest[:-1]))
        d, d_mlp = shard['w_out'].shape[1], shard['w_fc'].shape[1]
        n_pix, n_pos = shard['w_patch'].shape[0], shard['pos_table'].shape[0]
        scale = shard['w_qkv'].shape[-1] ** -0.5
        by_token = lambda x: x.transpose(1, 0, 2)

        def whole(value):
            return lax.all_gather(value, MESH_AXIS, tiled=True)

        w_qkv = whole(shard['w_qkv'].astype(BF16).reshape(HEAD, -1))
        small = pack_small(shard['w_patch'].T, shard['pos_table'].T, [shard[name][None] for name in PACKED])
        w_fo = whole(jnp.concatenate([shard['w_fc'].astype(BF16), shard['w_out'].astype(BF16)], axis=1))
        w_proj = whole(shard['w_proj'].astype(BF16))

        zo, g, small = pick_rows(keep, by_token(patches), by_token(rest[-1]), small)
        hat, a, stats, vecs, b_qkv, b_fc = embed(zo, small, w_qkv.shape[1], d_mlp)
        qkv, ctx = attend(a, w_qkv, b_qkv, scale)
        m, c, act, pre = mlp_up(ctx, hat, w_fo, vecs, b_fc)

        def over_chips(made):
            rings = [[2 * chip + core for chip in RING] for core in range(2)]
            return lax.psum_scatter(made.reshape(-1, made.shape[-1]), MESH_AXIS, axis_index_groups=rings, tiled=True)

        made = wgrad(act, g, 2, (), by_rows=True)
        g_proj = over_chips(made)
        d_pre, d_mid, d_mid_b, d_ctx, sums_m, sum_fc = mlp_grad(g, pre, m, w_proj, w_fo, vecs, (made,))
        made = wgrad(c, d_pre, 1, ())
        g_fc = over_chips(made)
        d_qkv, sum_qkv = attend_grad(qkv, d_ctx, scale, (made,))
        made = wgrad(a, d_qkv, 3, (), spare=d)
        made = wgrad(ctx, d_mid_b, 4, (), into=(made,))
        g_qkv_out = over_chips(made)
        d_emb, sums_e = embed_grad(d_qkv, d_mid, hat, stats, w_qkv, vecs, (made,))
        own = last_grads(d_emb, zo, vector_tail(sums_e, sums_m, sum_qkv, sum_fc), 6)
        h1, received = mlp_down(act, m, w_proj, vecs, own, 7)
        widths = [n_pix, n_pos] + [shard[name].shape[0] for name in PACKED]
        h1, *done = end_grads(h1, own, received, widths)

        grads = dict(w_patch=done[0].T, pos_table=done[1].T, w_qkv=g_qkv_out[:, :-d].reshape(shard['w_qkv'].shape), w_out=g_qkv_out[:, -d:], w_fc=g_fc, w_proj=g_proj)
        grads.update({name: value.reshape(-1) for name, value in zip(PACKED, done[2:])})
        return (by_token(h1),) + tuple(grads[name] for name in PARAM_NAMES)

    batch_spec = P(MESH_AXIS)
    param_specs = tuple(P(None, MESH_AXIS) if name in ('w_patch', 'pos_table') else batch_spec for name in PARAM_NAMES)
    return jax.shard_map(compute, mesh=mesh, in_specs=(batch_spec, batch_spec) + param_specs + (batch_spec,), out_specs=(batch_spec,) + param_specs, check_vma=False)
```

```python
import functools

import jax
import jax.numpy as jnp
from jax import lax
from jax.experimental import pallas as pl
from jax.experimental.pallas import tpu as pltpu
from jax.sharding import PartitionSpec as P


F32, BF16, I32 = jnp.float32, jnp.bfloat16, jnp.int32
LN_EPS = 1e-5
INV_SQRT2 = 0.7071067811865476
INV_SQRT_2PI = 0.3989422804014327
LOG2E = 1.4426950408889634
MASKED = -1e30
SUBLANES, LANES, HEAD = 8, 128, 64
TOK, FEW, MANY = 50, 4, 8
ROWS, GROWS = FEW * TOK, MANY * TOK
WIN = 112
STARTS = (0, ROWS - WIN)
EDGE = 96
PACK, VEC_ROW = 1024, 976
VEC_AT = VEC_ROW % LANES
N_VEC, VEC_ROWS = 10, 32
B_PATCH, CLS, LNP_G, LNP_B, LN1_G, LN1_B, B_OUT, LN2_G, LN2_B, B_PROJ = range(N_VEC)
STEP = 512
ALL_VMEM = 67043328
ANY = pl.BlockSpec(memory_space=pl.ANY)


def product(dims, left, right):
    return lax.dot_general(left, right, ((dims[:1], dims[1:]), ((), ())), preferred_element_type=F32)


dot = functools.partial(product, (1, 0))
dot_nt = functools.partial(product, (1, 1))
dot_tn = functools.partial(product, (0, 0))


def col_sum(x):
    return jnp.sum(x, axis=0, keepdims=True)


def col_max(x):
    return jnp.max(x, axis=0, keepdims=True)


def row_mean(x):
    return jnp.mean(x, axis=1, keepdims=True)


def row(ref, at):
    return ref[at:at + 1, :]


def iota(shape, axis):
    return lax.broadcasted_iota(I32, shape, axis)


def one_hot(test):
    return test.astype(F32).astype(BF16)


def origin(shape, *_):
    return (0,) * len(shape)


def held(shape):
    return pl.BlockSpec(shape, functools.partial(origin, shape), pipeline_mode=pl.Buffered(1))


def held_cols(n_rows, n_cols, at):
    return pl.BlockSpec((n_rows, n_cols), lambda *_: (0, at // n_cols), pipeline_mode=pl.Buffered(1))


def whole_out(shape):
    return pl.BlockSpec(shape, functools.partial(origin, shape))


def rows_spec(n_rows, width):
    return pl.BlockSpec((n_rows, width), lambda i, *_: (i, 0))


def this_block(n_rows, width, n):
    return pl.BlockSpec((n_rows, width), lambda i: (jnp.minimum(i, n - 1), 0))


def last_block(n_rows, width):
    return pl.BlockSpec((n_rows, width), lambda i: (jnp.maximum(i - 1, 0), 0))


def shaped(shape, dtype=F32):
    return jax.ShapeDtypeStruct(shape, dtype)


def call(kernel, after, args, *, prefetch=(), grid=(1,), in_specs, out_specs, out_shape, scratch_shapes=(), flops, n_bytes=0, partners=None, aliases=()):
    n_in, n_after = len(prefetch) + len(args), len(after)

    def body(*refs):
        return kernel(*refs[:n_in], *refs[n_in + n_after:])

    return pl.pallas_call(
        body,
        grid_spec=pltpu.PrefetchScalarGridSpec(
            num_scalar_prefetch=len(prefetch), grid=grid, in_specs=list(in_specs) + [ANY] * n_after,
            out_specs=out_specs, scratch_shapes=list(scratch_shapes)),
        out_shape=out_shape, input_output_aliases=dict(aliases),
        compiler_params=pltpu.CompilerParams(
            dimension_semantics=(pltpu.ARBITRARY,) * len(grid), vmem_limit_bytes=ALL_VMEM,
            collective_id=partners, has_side_effects=partners is not None),
        cost_estimate=pl.CostEstimate(flops=int(flops), bytes_accessed=int(n_bytes), transcendentals=0),
    )(*prefetch, *args, *after)


MESH_AXIS = 'fsdp'
CHIPS = 8


def device(at):
    return dict(device_id=(at,), device_id_type=pl.DeviceIdType.MESH)


def place():
    me = lax.axis_index(MESH_AXIS)
    core, chip = lax.rem(me, 2), lax.div(me, 2)
    return me, chip, core, me + 1 - 2 * core, [lax.rem(chip + k, CHIPS) for k in range(1, CHIPS)]


def meet(partners):
    barrier = pltpu.get_barrier_semaphore()
    for partner in partners:
        pl.semaphore_signal(barrier, **device(partner))
    pl.semaphore_wait(barrier, len(partners))


def first_step():
    return pl.when(pl.program_id(0) == 0)


def final_step():
    return pl.when(pl.program_id(0) == pl.num_programs(0) - 1)


def staggered(body, refs):
    step, last = pl.program_id(0), pl.num_programs(0) - 1
    pl.when(step == 0)(lambda: body(False, True, *refs))
    pl.when((step > 0) & (step < last))(lambda: body(True, True, *refs))
    pl.when(step == last)(lambda: body(True, False, *refs))


def gather_sems():
    dma = pltpu.SemaphoreType.DMA
    return [dma(()), dma((2 * CHIPS - 1,)), dma((2 * CHIPS - 1,))]


def hosted_gather(own_ref, all_ref, own_sem, send_sem, got_sem):
    me, chip, core, partner, others = place()
    sources = [lax.rem(chip + CHIPS - k, CHIPS) for k in range(1, CHIPS)]

    def rows(owner):
        return all_ref.at[pl.ds(pl.multiple_of(owner * HEAD, HEAD), HEAD)]

    def send(source, owner, to, at):
        return pltpu.make_async_remote_copy(source, rows(owner), send_sem.at[at], got_sem.at[at], **device(to))

    local = pltpu.make_async_copy(own_ref, rows(me), own_sem)
    sent = [send(own_ref, me, partner, 0)] + [send(own_ref, me, 2 * other + core, k + 1) for k, other in enumerate(others)]
    passed = [send(rows(2 * source + core), 2 * source + core, partner, CHIPS + k) for k, source in enumerate(sources)]

    @first_step()
    def _():
        meet([partner] + [2 * other + core for other in others])
        local.start()
        for copy in sent:
            copy.start()

    def finish():
        @final_step()
        def _():
            for arrived, copy in zip(sent[1:], passed):
                arrived.wait_recv()
                copy.start()
            local.wait()
            sent[0].wait_recv()
            for copy in passed:
                copy.wait_recv()
            for copy in sent + passed:
                copy.wait_send()

    return finish


def clear(*refs):
    for ref in refs:
        ref[:] = jnp.zeros_like(ref)


def normalize(x):
    centered = x - row_mean(x)
    inv = lax.rsqrt(row_mean(centered * centered) + LN_EPS)
    return centered * inv, inv


def norm_grad(d_out, x_hat, inv, gain):
    d_hat = d_out * gain
    return inv * (d_hat - row_mean(d_hat) - x_hat * row_mean(d_hat * x_hat))


def image_of(at, n_img=FEW):
    return sum((at >= j * TOK).astype(I32) for j in range(1, n_img))


def is_class(n_rows):
    at = iota((n_rows, 1), 0)
    return at == TOK * image_of(at, n_rows // TOK)


def pack_kernel(wt_ref, pt_ref, *refs):
    *vec_refs, out_ref, rows_ref, pos_ref = refs
    n_pix, n_pos = wt_ref.shape[1], pt_ref.shape[1]
    out_ref[:, :n_pix] = wt_ref[:].astype(BF16)
    out_ref[:, n_pix:n_pix + LANES] = pt_ref[:, :LANES].astype(BF16)
    clear(rows_ref, pos_ref)
    pos_ref[:, :n_pos - LANES] = pt_ref[:, LANES:]
    at = VEC_AT
    for ref in vec_refs:
        for lo in range(0, ref.shape[1], HEAD):
            rows_ref[at:at + 1, :HEAD] = ref[:, lo:lo + HEAD]
            at += 1
    out_ref[:, n_pix + LANES:] = (pos_ref[:] + rows_ref[:].T[:HEAD]).astype(BF16)


def pack_small(wt, pt, vecs):
    args = [wt, pt] + vecs
    shape = (HEAD, PACK)
    return call(pack_kernel, (), args, in_specs=[held(x.shape) for x in args], out_specs=whole_out(shape), out_shape=shaped(shape, BF16),
                scratch_shapes=[pltpu.VMEM((LANES, LANES), F32), pltpu.VMEM((HEAD, LANES), F32)], flops=PACK)


def pick_kernel(keep_ref, patches_ref, g_ref, small_ref, zo_ref, gi_ref, all_ref, pad_ref, move_ref, *sems):
    finish = hosted_gather(small_ref, all_ref, *sems)

    @first_step()
    def _():
        to, source = iota((GROWS, GROWS), 0), iota((GROWS, GROWS), 1)
        move_ref[:] = one_hot(to == lax.rem(source, MANY) * TOK + lax.div(source, MANY))

    n_patch, _, n_pix = patches_ref.shape
    clear(pad_ref)
    pad_ref[:, :TOK - 1] = keep_ref[:].astype(F32)
    image, lane = iota(pad_ref.shape, 0), iota(pad_ref.shape, 1)
    spread = pad_ref[:]
    for b in range(MANY):
        spread = jnp.where(image == b, pltpu.roll(pad_ref[:], TOK * b + 1, 1), spread)
    own = (lane > TOK * image) & (lane < TOK * image + TOK)
    token = col_sum(jnp.where(own, spread + 1.0, 0.0))
    source = col_sum(jnp.where(own, spread * MANY + image.astype(F32), 0.0))
    source = jnp.where(token > 0.0, source, -1.0)
    cols = jnp.where(image == 0, source, token).T[:GROWS].astype(I32)
    source, token = cols[:, :1], cols[:, 1:2]
    pick = one_hot(iota((GROWS, MANY * n_patch), 1) == source)
    zo_ref[:, :n_pix] = dot(pick, patches_ref[:].reshape(MANY * n_patch, n_pix)).astype(BF16)
    zo_ref[:, n_pix:] = one_hot(iota((GROWS, PACK - n_pix), 1) == token)
    gi_ref[:] = dot(move_ref[:], g_ref[:].reshape(GROWS, g_ref.shape[2])).astype(BF16)

    finish()


def pick_rows(keep, patches_t, g_t, small):
    _, n_img, _ = patches_t.shape
    d = g_t.shape[2]
    n_tok = n_img * TOK
    by_image = lambda x: pl.BlockSpec((x.shape[0], MANY, x.shape[2]), lambda i: (0, i, 0))
    return call(pick_kernel, (), (keep, patches_t, g_t, small), grid=(n_img // MANY,),
                in_specs=[rows_spec(MANY, TOK - 1), by_image(patches_t), by_image(g_t), ANY],
                out_specs=[rows_spec(GROWS, PACK), rows_spec(GROWS, d), ANY],
                out_shape=[shaped((n_tok, PACK), BF16), shaped((n_tok, d), BF16), shaped((2 * CHIPS * HEAD, PACK), BF16)],
                scratch_shapes=[pltpu.VMEM((MANY, STEP), F32), pltpu.VMEM((GROWS, GROWS), BF16)] + gather_sems(),
                flops=STEP * patches_t.size, partners=0)


def embed_kernel(zo_ref, wt_ref, hat_ref, a_ref, stat_ref, vec_ref, bq_ref, bf_ref, next_ref, now_ref):
    @first_step()
    def _():
        base = VEC_ROW - VEC_AT
        vec_ref[:] = wt_ref[:, base:base + LANES].astype(F32).T[VEC_AT:VEC_AT + VEC_ROWS]
        at = N_VEC
        for ref in (bq_ref, bf_ref):
            n = ref.shape[1] // vec_ref.shape[1]
            chunk = lambda q: row(vec_ref, at + q % n)[:, q // n * HEAD:(q // n + 1) * HEAD]
            for lo in range(0, ref.shape[1], LANES):
                ref[:, lo:lo + LANES] = jnp.concatenate([chunk(lo // HEAD), chunk(lo // HEAD + 1)], axis=1)
            at += n

    now_ref[:] = next_ref[:]
    next_ref[:] = dot_nt(zo_ref[:], wt_ref[:]) + jnp.where(is_class(GROWS), row(vec_ref, CLS), row(vec_ref, B_PATCH))
    hat, inv = normalize(now_ref[:])
    hat_ref[:] = hat
    h0 = hat * row(vec_ref, LNP_G) + row(vec_ref, LNP_B)
    mean1 = row_mean(h0)
    centered = h0 - mean1
    inv1 = lax.rsqrt(row_mean(centered * centered) + LN_EPS)
    a_ref[:] = (centered * inv1 * row(vec_ref, LN1_G) + row(vec_ref, LN1_B)).astype(BF16)
    lane = iota(stat_ref.shape, 1)
    stat_ref[:] = jnp.where(lane == 0, inv, jnp.where(lane == 1, inv1, mean1))


def embed(zo, small, d_qkv, d_mlp):
    n_tok = zo.shape[0]
    d = small.shape[0]
    n = n_tok // GROWS
    outs = ((VEC_ROWS, d), (1, d_qkv), (1, d_mlp))
    return call(embed_kernel, (), (zo, small), grid=(n + 1,),
                in_specs=[this_block(GROWS, PACK, n), held(small.shape)],
                out_specs=[last_block(GROWS, d), last_block(GROWS, d), last_block(GROWS, LANES)] + [whole_out(s) for s in outs],
                out_shape=[shaped((n_tok, d)), shaped((n_tok, d), BF16), shaped((n_tok, LANES))] + [shaped(s) for s in outs],
                scratch_shapes=[pltpu.VMEM((GROWS, d), F32)] * 2, flops=2 * zo.size * d)


def window_mask(start):
    key, query = (iota((WIN, 2 * WIN), axis) for axis in (0, 1))
    return jnp.where(image_of(key + start) == image_of(lax.rem(query, WIN) + start), 0.0, MASKED)


def set_masks(mask_ref):
    for i, start in enumerate(STARTS):
        mask_ref[i] = window_mask(start)


def split_heads(x):
    first = iota(x.shape, 1) < HEAD
    zero = jnp.zeros_like(x)
    return jnp.concatenate([jnp.where(first, x, zero), jnp.where(first, zero, x)], axis=0)


def join_heads(x):
    return jnp.where(iota((WIN, LANES), 1) < HEAD, x[:WIN], x[WIN:])


def join_windows(lo, hi):
    at = EDGE + SUBLANES
    shift = STARTS[1]
    edge = jnp.where(iota((SUBLANES, LANES), 0) < 2 * TOK - EDGE, lo[EDGE:at], hi[EDGE - shift:at - shift])
    return jnp.concatenate([lo[:EDGE], edge, hi[at - shift:]], axis=0)


def weights_t(logits, mask, scale):
    masked = logits + mask
    e = jnp.exp2((masked - col_max(masked)) * (scale * LOG2E))
    return e * (1.0 / col_sum(e))


def lane_tile(at):
    return slice(at * LANES, (at + 1) * LANES)


def reader(ref):
    return lambda at, i: ref[STARTS[i]:STARTS[i] + WIN, lane_tile(at)]


def every_unit(n_tiles):
    return [(pair, i) for pair in range(n_tiles) for i in range(len(STARTS))]


def window_scratch():
    return pltpu.VMEM((len(STARTS), WIN, 2 * WIN), F32)


def attend_kernel(scale, a_ref, w_ref, b_ref, qkv_ref, o_ref, mask_ref):
    @first_step()
    def _():
        set_masks(mask_ref)

    n_tiles = o_ref.shape[1] // LANES
    a = a_ref[:]
    for lo in range(0, b_ref.shape[1], STEP):
        cols = slice(lo, lo + STEP)
        qkv_ref[:, cols] = (dot(a, w_ref[:, cols]) + b_ref[:, cols]).astype(BF16)
    read, units = reader(qkv_ref), every_unit(n_tiles)
    logits = [dot_nt(read(n_tiles + pair, i), split_heads(read(pair, i))) for pair, i in units]
    probs = [weights_t(x, mask_ref[i], scale).astype(BF16) for x, (_, i) in zip(logits, units)]
    outs = [join_heads(dot_tn(p, read(2 * n_tiles + pair, i))) for p, (pair, i) in zip(probs, units)]
    for lo, hi, (pair, _) in zip(outs[::2], outs[1::2], units[::2]):
        o_ref[:, lane_tile(pair)] = join_windows(lo, hi).astype(BF16)


def attend(a, first, b_qkv, scale):
    n_tok, d = a.shape
    width = b_qkv.shape[1]
    return call(functools.partial(attend_kernel, scale), (), (a, first, b_qkv), grid=(n_tok // ROWS,),
                in_specs=[rows_spec(ROWS, d), held_cols(d, width, 0), held(b_qkv.shape)],
                out_specs=[rows_spec(ROWS, width), rows_spec(ROWS, d)],
                out_shape=[shaped((n_tok, width), BF16), shaped((n_tok, d), BF16)],
                scratch_shapes=[window_scratch()], flops=4 * a.size * width)


def attend_grad_kernel(scale, qkv_ref, dctx_ref, dqkv_ref, bsum_ref, mask_ref):
    @first_step()
    def _():
        set_masks(mask_ref)
        clear(bsum_ref)

    n_tiles = dctx_ref.shape[1] // LANES
    read, read_grad, units = reader(qkv_ref), reader(dctx_ref), every_unit(n_tiles)
    q2 = [split_heads(read(pair, i)) for pair, i in units]
    do2 = [split_heads(read_grad(pair, i)) for pair, i in units]
    logits = [dot_nt(read(n_tiles + pair, i), q) for q, (pair, i) in zip(q2, units)]
    dp = [dot_nt(read(2 * n_tiles + pair, i), do) for do, (pair, i) in zip(do2, units)]
    logits = [x * scale + mask_ref[i] for x, (_, i) in zip(logits, units)]
    e = [jnp.exp2((x - col_max(x)) * LOG2E) for x in logits]
    p = [x * (1.0 / col_sum(x)) for x in e]
    dv = [dot(x.astype(BF16), do) for x, do in zip(p, do2)]
    ds = [(x * (y - col_sum(x * y)) * scale).astype(BF16) for x, y in zip(p, dp)]
    dk = [dot(x, q) for x, q in zip(ds, q2)]
    dq = [join_heads(dot_tn(x, read(n_tiles + pair, i))) for x, (pair, i) in zip(ds, units)]
    for at, (pair, _) in enumerate(units[::2]):
        for part, grads in enumerate((dq, dk, dv)):
            both = join_windows(grads[2 * at], grads[2 * at + 1])
            cols = lane_tile(part * n_tiles + pair)
            dqkv_ref[:, cols] = both.astype(BF16)
            bsum_ref[:, cols] += col_sum(both)


def attend_grad(qkv, d_ctx, scale, after):
    n_tok, width = qkv.shape
    return call(functools.partial(attend_grad_kernel, scale), after, (qkv, d_ctx), grid=(n_tok // ROWS,),
                in_specs=[rows_spec(ROWS, width), rows_spec(ROWS, d_ctx.shape[1])], out_specs=[rows_spec(ROWS, width), whole_out((1, width))],
                out_shape=[shaped((n_tok, width), BF16), shaped((1, width))],
                scratch_shapes=[window_scratch()], flops=3 * d_ctx.size * width)


def erf_cdf(u):
    return 0.5 + 0.5 * lax.erf(u * INV_SQRT2)


def mlp_up_kernel(*refs):
    staggered(mlp_up_step, refs)


def mlp_up_step(with_now, with_next, o_ref, hat_ref, wo_ref, wf_ref, vec_ref, bf_ref, m_ref, c_ref, act_ref, pre_ref, next_ref, now_ref):
    if with_now:
        now_ref[:] = next_ref[:]
        c = now_ref[:]
    if with_next:
        m = hat_ref[:] * row(vec_ref, LNP_G) + row(vec_ref, LNP_B) + dot(o_ref[:], wo_ref[:]) + row(vec_ref, B_OUT)
        m_ref[:] = m
        hat2, _ = normalize(m)
        next_c = (hat2 * row(vec_ref, LN2_G) + row(vec_ref, LN2_B)).astype(BF16)
        c_ref[:] = next_c
    if with_now:
        for lo in range(0, wf_ref.shape[1], STEP):
            cols = slice(lo, lo + STEP)
            u = dot(c, wf_ref[:, cols]) + bf_ref[:, cols]
            pre_ref[:, cols] = u
            act_ref[:, cols] = (u * erf_cdf(u)).astype(BF16)
    if with_next:
        next_ref[:] = next_c


def mlp_up(o, hat, w_fo, vecs, b_fc):
    n_tok, d = o.shape
    f = b_fc.shape[1]
    n = n_tok // GROWS
    return call(mlp_up_kernel, (), (o, hat, w_fo, w_fo, vecs, b_fc), grid=(n + 1,),
                in_specs=[this_block(GROWS, d, n), this_block(GROWS, d, n), held_cols(d, d, f), held_cols(d, f, 0), held(vecs.shape), held(b_fc.shape)],
                out_specs=[this_block(GROWS, d, n), this_block(GROWS, d, n), last_block(GROWS, f), last_block(GROWS, f)],
                out_shape=[shaped((n_tok, d)), shaped((n_tok, d), BF16), shaped((n_tok, f), BF16), shaped((n_tok, f))],
                scratch_shapes=[pltpu.VMEM((GROWS, d), BF16)] * 2, flops=3 * o.size * f)


def mlp_down_kernel(act_ref, m_ref, w_ref, vec_ref, own_ref, h1_ref, all_ref, move_ref, send_sem, got_sem):
    _, chip, core, _, others = place()
    copies = [pltpu.make_async_remote_copy(own_ref.at[other], all_ref.at[chip], send_sem.at[k], got_sem.at[k], **device(2 * other + core))
              for k, other in enumerate(others)]

    @first_step()
    def _():
        meet([2 * other + core for other in others])
        for copy in copies:
            copy.start()
        to, source = iota((GROWS, GROWS), 0), iota((GROWS, GROWS), 1)
        move_ref[:] = one_hot(source == lax.rem(to, MANY) * TOK + lax.div(to, MANY))

    h1 = (m_ref[:] + dot(act_ref[:], w_ref[:]) + row(vec_ref, B_PROJ)).astype(BF16)
    h1_ref[:] = dot(move_ref[:], h1).astype(BF16).reshape(h1_ref.shape)

    @final_step()
    def _():
        for copy in copies:
            copy.wait()


def mlp_down(act, m, w_proj, vecs, own, number):
    n_tok, f = act.shape
    d = m.shape[1]
    dma = pltpu.SemaphoreType.DMA((CHIPS - 1,))
    return call(mlp_down_kernel, (), (act, m, w_proj, vecs, own), grid=(n_tok // GROWS,),
                in_specs=[rows_spec(GROWS, f), rows_spec(GROWS, d), held(w_proj.shape), held(vecs.shape), ANY],
                out_specs=[pl.BlockSpec((TOK, MANY, d), lambda i: (0, i, 0)), ANY],
                out_shape=[shaped((TOK, n_tok // TOK, d), BF16), shaped(own.shape)],
                scratch_shapes=[pltpu.VMEM((GROWS, GROWS), BF16), dma, dma],
                flops=2 * m.size * f, partners=number)


def mlp_grad_kernel(g_ref, pre_ref, m_ref, wp_ref, wf_ref, wo_ref, vec_ref, dpre_ref, dmid_ref, dmidb_ref, dctx_ref, vsum_ref, bfc_ref):
    @first_step()
    def _():
        clear(vsum_ref, bfc_ref)

    g = g_ref[:]
    step = 2 * STEP
    d_c = jnp.zeros(m_ref.shape, F32)
    cuts = [slice(lo, lo + step) for lo in range(0, wp_ref.shape[0], step)]
    acts, pres = dict(), dict()
    n = len(cuts)
    for tick in range(n + 2):
        if tick < n:
            acts[tick] = dot_nt(g, wp_ref[cuts[tick], :])
        if 0 <= tick - 1 < n:
            cols = cuts[tick - 1]
            u = pre_ref[:, cols]
            w = u * INV_SQRT2
            d_pre = acts.pop(tick - 1) * (0.5 + 0.5 * lax.erf(w) + u * (jnp.exp2((w * w) * (-LOG2E)) * INV_SQRT_2PI))
            bfc_ref[:, cols] += col_sum(d_pre)
            pres[tick - 1] = d_pre.astype(BF16)
            dpre_ref[:, cols] = pres[tick - 1]
        if tick >= 2:
            d_c = d_c + dot_nt(pres.pop(tick - 2), wf_ref[:, cuts[tick - 2]])
    hat2, inv2 = normalize(m_ref[:])
    g_f = g.astype(F32)
    d_mid = norm_grad(d_c, hat2, inv2, row(vec_ref, LN2_G)) + g_f
    dmid_ref[:] = d_mid
    d_mid_b = d_mid.astype(BF16)
    dmidb_ref[:] = d_mid_b
    dctx_ref[:] = dot_nt(d_mid_b, wo_ref[:]).astype(BF16)
    for at, part in enumerate((d_mid, d_c * hat2, d_c, g_f)):
        vsum_ref[at:at + 1, :] += col_sum(part)


def mlp_grad(g, pre, m, w_proj, w_fo, vecs, after):
    n_tok, d = g.shape
    f = pre.shape[1]
    wide, narrow = rows_spec(GROWS, f), rows_spec(GROWS, d)
    return call(mlp_grad_kernel, after, (g, pre, m, w_proj, w_fo, w_fo, vecs), grid=(n_tok // GROWS,),
                in_specs=[narrow, wide, narrow, held(w_proj.shape), held_cols(d, f, 0), held_cols(d, d, f), held(vecs.shape)],
                out_specs=[wide, narrow, narrow, narrow, whole_out((SUBLANES, d)), whole_out((1, f))],
                out_shape=[shaped((n_tok, f), BF16), shaped((n_tok, d)), shaped((n_tok, d), BF16), shaped((n_tok, d), BF16),
                           shaped((SUBLANES, d)), shaped((1, f))],
                flops=5 * g.size * f)


CUTS = (0, 104, 208, 304, GROWS)


def embed_grad_kernel(*refs):
    @first_step()
    def _():
        clear(refs[7])

    staggered(embed_grad_step, refs)


def embed_grad_step(with_now, with_next, dqkv_ref, dmid_ref, hat_ref, stat_ref, w_ref, vec_ref, demb_ref, vsum_ref, next_ref, now_ref, dx_ref):
    if with_now:
        now_ref[:] = next_ref[:]
    width = now_ref.shape[1] // (len(CUTS) - 1)
    sums = []
    for j, (lo, hi) in enumerate(zip(CUTS, CUTS[1:])):
        cols, rows = slice(j * width, (j + 1) * width), slice(lo, hi)
        if with_next:
            next_ref[:, cols] = dot_nt(dqkv_ref[:], w_ref[cols, :])
        if not with_now:
            continue
        d_a, hat_p = now_ref[rows, :], hat_ref[rows, :]
        inv_p, inv1, mean1 = (stat_ref[rows, k:k + 1] for k in range(3))
        hat1 = (hat_p * row(vec_ref, LNP_G) + row(vec_ref, LNP_B) - mean1) * inv1
        d_zero = norm_grad(d_a, hat1, inv1, row(vec_ref, LN1_G)) + dmid_ref[rows, :]
        d_x = norm_grad(d_zero, hat_p, inv_p, row(vec_ref, LNP_G))
        demb_ref[rows, :] = d_x.astype(BF16)
        dx_ref[rows, :] = d_x
        sums.append([col_sum(part) for part in (d_x, d_zero * hat_p, d_zero, d_a * hat1, d_a)])
    if with_now:
        d_all, *others = (sum(parts) for parts in zip(*sums))
        d_cls = sum(row(dx_ref, at) for at in range(0, GROWS, TOK))
        for at, part in enumerate([d_all - d_cls, d_cls] + others):
            vsum_ref[at:at + 1, :] += part


def embed_grad(dqkv, d_mid, hat, stats, first, vecs, after):
    n_tok, d = d_mid.shape
    width = dqkv.shape[1]
    n = n_tok // GROWS
    return call(embed_grad_kernel, after, (dqkv, d_mid, hat, stats, first, vecs), grid=(n + 1,),
                in_specs=[this_block(GROWS, width, n), last_block(GROWS, d), last_block(GROWS, d), last_block(GROWS, LANES),
                          held_cols(d, width, 0), held(vecs.shape)],
                out_specs=[last_block(GROWS, d), whole_out((SUBLANES, d))], out_shape=[shaped((n_tok, d), BF16), shaped((SUBLANES, d))],
                scratch_shapes=[pltpu.VMEM((GROWS, d), F32)] * 3, flops=3 * d_mid.size * width)


def tail_kernel(se_ref, sm_ref, sq_ref, sf_ref, out_ref, rows_ref):
    d = se_ref.shape[1]
    clear(rows_ref)
    at, cut = VEC_AT, VEC_AT + B_OUT
    rows_ref[at:cut, :] = se_ref[:B_OUT, :]
    at += N_VEC
    rows_ref[cut:at, :] = sm_ref[:N_VEC - B_OUT, :]
    for ref in (sq_ref, sf_ref):
        n = ref.shape[1] // d
        for r in range(n):
            chunk = lambda q: ref[:, (n * q + r) * HEAD:(n * q + r + 1) * HEAD]
            for j in range(d // LANES):
                rows_ref[at:at + 1, lane_tile(j)] = jnp.concatenate([chunk(2 * j), chunk(2 * j + 1)], axis=1)
            at += 1
    for j in range(d // LANES):
        out_ref[lane_tile(j)] = rows_ref[:, lane_tile(j)].T


def vector_tail(*args):
    d = args[0].shape[1]
    return call(tail_kernel, (), args, in_specs=[held(x.shape) for x in args], out_specs=whole_out((d, LANES)), out_shape=shaped((d, LANES)),
                scratch_shapes=[pltpu.VMEM((LANES, d), F32)], flops=d)


RING = [at ^ (at >> 1) for at in range(CHIPS)]


def ring_chip(at):
    half, quarter = lax.div(at, 2), lax.div(at, 4)
    return 4 * quarter + 2 * lax.rem(half + quarter, 2) + lax.rem(at + half, 2)


def wgrad_kernel(by_rows, first_tile, n_in, a_ref, b_ref, *refs):
    out_ref, made_ref, got_ref, own_ref, send_sem, got_sem, free_sem, out_sem, *at_ref = refs[n_in:]
    step, last = pl.program_id(0), pl.num_programs(0) - 1
    slot = lax.rem(step, 2)
    _, _, mine, partner, _ = place()
    partner = device(partner)

    def part(at, core):
        return made_ref.at[at, core] if by_rows else made_ref.at[at, :, core]

    def exchange(at):
        return pltpu.make_async_remote_copy(part(at, 1 - mine), got_ref.at[at], send_sem.at[at], got_sem.at[at], **partner)

    def store(at, tile):
        width = own_ref.shape[-1]
        out = out_ref.at[tile] if by_rows else out_ref.at[:, :, pl.ds(pl.multiple_of((tile + first_tile) * width, width), width)]
        return pltpu.make_async_copy(own_ref.at[at], out, out_sem.at[at])

    def finish(at, tile):
        exchange(at).wait_recv()

        @pl.when(tile >= 2)
        def _():
            store(at, 0).wait()

        own_ref[at] = part(at, mine)[:] + got_ref[at]

        @pl.when(tile + 2 <= last)
        def _():
            pl.semaphore_signal(free_sem.at[at], **partner)

        store(at, tile).start()

    @first_step()
    def _():
        if not by_rows:
            for j in range(CHIPS):
                at_ref[0][lane_tile(RING.index(j)), :] = a_ref[:, lane_tile(j)].T
        meet([partner['device_id'][0]])

    @pl.when(step >= 2)
    def _():
        exchange(slot).wait_send()

    total = dot_tn(a_ref[:], b_ref[:]) if by_rows else dot(at_ref[0][:], b_ref[:])
    made_ref[slot] = total.reshape(made_ref.shape[1:])

    @pl.when(step >= 2)
    def _():
        pl.semaphore_wait(free_sem.at[slot], 1)

    exchange(slot).start()

    @pl.when(step >= 1)
    def _():
        finish(1 - slot, step - 1)

    @pl.when(step == last)
    def _():
        finish(slot, step)
        for at in range(2):
            exchange(at).wait_send()
            store(at, 0).wait()


def wgrad(a, b, number, after, by_rows=False, into=(), spare=0):
    k, m = a.shape
    n = b.shape[1]
    r = m // (2 * CHIPS)
    width = into[0].shape[-1] if into else n + spare
    if by_rows:
        steps, made, own = CHIPS, (2, r, n), (r, n)
        in_specs, scratch = [pl.BlockSpec((k, 2 * r), lambda j: (0, ring_chip(j))), held(b.shape)], []
    else:
        steps, made, own = n // STEP, (CHIPS, 2, r, STEP), (CHIPS, r, STEP)
        in_specs, scratch = [held(a.shape), pl.BlockSpec((k, STEP), lambda j: (0, j))], [pltpu.VMEM((m, k), BF16)]
    slots = lambda shape: pltpu.VMEM((2,) + shape, F32)
    dma = pltpu.SemaphoreType.DMA((2,))
    return call(functools.partial(wgrad_kernel, by_rows, (width - n - spare) // STEP, len(into)), after, (a, b) + tuple(into), grid=(steps,),
                in_specs=in_specs + [ANY] * len(into), out_specs=ANY, out_shape=shaped((CHIPS, r, width)), aliases=[(2, 0)] * len(into),
                scratch_shapes=[slots(made), slots(own), slots(own), dma, dma, pltpu.SemaphoreType.REGULAR((2,)), dma] + scratch,
                flops=2 * k * m * n, partners=number)


def last_kernel(a_ref, b_ref, tail_ref, out_ref, at_ref, made_ref, got_ref, own_ref, swap_sem, out_sem):
    step, n_steps = pl.program_id(0), made_ref.shape[0]
    _, _, core, partner, _ = place()
    width = made_ref.shape[-1]

    def swap(tile):
        return pltpu.make_async_remote_copy(made_ref.at[tile, :, 1 - core], got_ref.at[tile], swap_sem.at[0, tile], swap_sem.at[1, tile], **device(partner))

    def store(tile):
        return pltpu.make_async_copy(own_ref.at[tile], out_ref.at[:, :, pl.ds(pl.multiple_of(tile * width, width), width)], out_sem.at[tile])

    def finish(tile):
        swap(tile).wait_recv()
        own_ref[tile] = made_ref[tile, :, core] + got_ref[tile]
        store(tile).start()

    @first_step()
    def _():
        for j in range(CHIPS):
            at_ref[lane_tile(j), :] = a_ref[:, lane_tile(j)].T
        meet([partner])

    made_ref[step] = dot(at_ref[:], b_ref[:]).reshape(made_ref.shape[1:])

    @final_step()
    def _():
        made_ref[step, :, :, :, width - LANES:] += tail_ref[:].reshape(made_ref.shape[1:4] + (LANES,))

    swap(step).start()

    @pl.when(step > 0)
    def _():
        finish(step - 1)

    @final_step()
    def _():
        finish(step)
        for tile in range(n_steps):
            swap(tile).wait_send()
            store(tile).wait()


def last_grads(a, b, tail, number):
    k, m = a.shape
    n_steps = PACK // STEP
    slots = lambda *shape: pltpu.VMEM((n_steps, CHIPS) + shape + (HEAD, STEP), F32)
    dma = pltpu.SemaphoreType.DMA
    return call(last_kernel, (), (a, b, tail), grid=(n_steps,),
                in_specs=[held(a.shape), pl.BlockSpec((k, STEP), lambda j: (0, j)), held(tail.shape)],
                out_specs=ANY, out_shape=shaped((CHIPS, HEAD, PACK)),
                scratch_shapes=[pltpu.VMEM((m, k), BF16), slots(2), slots(), slots(), dma((2, n_steps)), dma((n_steps,))],
                flops=2 * k * m * PACK, partners=number)


def end_kernel(h1_ref, own_ref, all_ref, token_ref, wt_ref, pos_ref, *refs):
    *vec_refs, full_ref = refs
    token_ref[:] = h1_ref[:]

    @first_step()
    def _():
        _, chip, _, _, others = place()
        full_ref[:] = own_ref[chip] + sum(all_ref[other] for other in others)
        n_pix, n_pos = wt_ref.shape[1], pos_ref.shape[1]
        wt_ref[:] = full_ref[:, :n_pix]
        pos_ref[:] = full_ref[:, n_pix:n_pix + n_pos]
        pos_ref[:, :1] = full_ref[:, VEC_ROW + CLS:VEC_ROW + CLS + 1]
        rows = full_ref[:, VEC_ROW - VEC_AT:VEC_ROW - VEC_AT + LANES].T
        at = VEC_AT
        for ref in vec_refs:
            for lo in range(0, ref.shape[1], HEAD):
                ref[:, lo:lo + HEAD] = rows[at:at + 1]
                at += 1


def end_grads(h1, own, received, widths):
    n_tok, d = h1.shape
    shapes = [(HEAD, w) for w in widths[:2]] + [(1, w) for w in widths[2:]]
    return call(end_kernel, (), (h1, own, received), grid=(n_tok // GROWS,),
                in_specs=[rows_spec(GROWS, d), held(own.shape), held(received.shape)],
                out_specs=[rows_spec(GROWS, d)] + [whole_out(s) for s in shapes],
                out_shape=[shaped((n_tok, d), BF16)] + [shaped(s) for s in shapes],
                scratch_shapes=[pltpu.VMEM((HEAD, PACK), F32)], flops=PACK)


PARAM_NAMES = ('w_patch', 'b_patch', 'pos_table', 'cls_tok', 'lnp_g', 'lnp_b', 'ln1_g', 'ln1_b', 'w_qkv', 'b_qkv', 'w_out', 'b_out', 'ln2_g', 'ln2_b', 'w_fc', 'b_fc', 'w_proj', 'b_proj')
PACKED = tuple(PARAM_NAMES[i] for i in (1, 3, 4, 5, 6, 7, 11, 12, 13, 17, 9, 15))


def solution(mesh):
    def compute(patches, keep, *rest):
        shard = dict(zip(PARAM_NAMES, rest[:-1]))
        d, d_mlp = shard['w_out'].shape[1], shard['w_fc'].shape[1]
        n_pix, n_pos = shard['w_patch'].shape[0], shard['pos_table'].shape[0]
        scale = shard['w_qkv'].shape[-1] ** -0.5
        by_token = lambda x: x.transpose(1, 0, 2)

        def whole(value):
            return lax.all_gather(value, MESH_AXIS, tiled=True)

        w_qkv = whole(shard['w_qkv'].astype(BF16).reshape(HEAD, -1))
        small = pack_small(shard['w_patch'].T, shard['pos_table'].T, [shard[name][None] for name in PACKED])
        w_fo = whole(jnp.concatenate([shard['w_fc'].astype(BF16), shard['w_out'].astype(BF16)], axis=1))
        w_proj = whole(shard['w_proj'].astype(BF16))

        zo, g, small = pick_rows(keep, by_token(patches), by_token(rest[-1]), small)
        hat, a, stats, vecs, b_qkv, b_fc = embed(zo, small, w_qkv.shape[1], d_mlp)
        qkv, ctx = attend(a, w_qkv, b_qkv, scale)
        m, c, act, pre = mlp_up(ctx, hat, w_fo, vecs, b_fc)

        def over_chips(made):
            rings = [[2 * chip + core for chip in RING] for core in range(2)]
            return lax.psum_scatter(made.reshape(-1, made.shape[-1]), MESH_AXIS, axis_index_groups=rings, tiled=True)

        made = wgrad(act, g, 2, (), by_rows=True)
        g_proj = over_chips(made)
        d_pre, d_mid, d_mid_b, d_ctx, sums_m, sum_fc = mlp_grad(g, pre, m, w_proj, w_fo, vecs, (made,))
        made = wgrad(c, d_pre, 1, ())
        g_fc = over_chips(made)
        d_qkv, sum_qkv = attend_grad(qkv, d_ctx, scale, (made,))
        made = wgrad(a, d_qkv, 3, (), spare=d)
        made = wgrad(ctx, d_mid_b, 4, (), into=(made,))
        g_qkv_out = over_chips(made)
        d_emb, sums_e = embed_grad(d_qkv, d_mid, hat, stats, w_qkv, vecs, (made,))
        own = last_grads(d_emb, zo, vector_tail(sums_e, sums_m, sum_qkv, sum_fc), 6)
        h1, received = mlp_down(act, m, w_proj, vecs, own, 7)
        widths = [n_pix, n_pos] + [shard[name].shape[0] for name in PACKED]
        by_rows, *done = end_grads(h1.reshape(-1, d), own, received, widths)

        grads = dict(w_patch=done[0].T, pos_table=done[1].T, w_qkv=g_qkv_out[:, :-d].reshape(shard['w_qkv'].shape), w_out=g_qkv_out[:, -d:], w_fc=g_fc, w_proj=g_proj)
        grads.update({name: value.reshape(-1) for name, value in zip(PACKED, done[2:])})
        return (by_token(by_rows.reshape(h1.shape)),) + tuple(grads[name] for name in PARAM_NAMES)

    batch_spec = P(MESH_AXIS)
    param_specs = tuple(P(None, MESH_AXIS) if name in ('w_patch', 'pos_table') else batch_spec for name in PARAM_NAMES)
    return jax.shard_map(compute, mesh=mesh, in_specs=(batch_spec, batch_spec) + param_specs + (batch_spec,), out_specs=(batch_spec,) + param_specs, check_vma=False)
```
